16 devices in a mesh: dp: 2 (over y, z), x: 8 (over x, core).
Axes of the slice: x: 4, y: 2, z: 1, core: 2. Of those that a mesh axis runs over, the one named last changes fastest.
The devices are a block of a 4x4x8 slice.
Arguments:
- c_raw: bfloat16 [96, 6144, 512], P('dp', 'x'), parts along dimension 0
- k_raw: bfloat16 [96, 6144, 64], P('dp', 'x'), parts along dimension 0
- norm_gain: bfloat16 [512], replicated
- rope_cos: float32 [6144, 32], P('x')
- rope_sin: float32 [6144, 32], P('x')
- seq_lens: int32 [96], P('dp'), parts along dimension 0
- q_lat: bfloat16 [96, 128, 512], P(('dp', 'x')), parts along dimension 0
- q_rope: bfloat16 [96, 128, 64], P(('dp', 'x')), parts along dimension 0
Outputs:
- output 1: bfloat16 [96, 6144, 512], P(('dp', 'x')), parts along dimension 0
- output 2: bfloat16 [96, 6144, 64], P(('dp', 'x')), parts along dimension 0
- output 3: bfloat16 [96, 128, 512], P(('dp', 'x')), parts along dimension 0
There are 2 independent parts. The reference program is written for one: setup_inputs(seed, part) draws one part's arguments, and reference() takes and returns one part's arrays. A program takes and returns all parts, laid end to end along the dimension named above; an argument that names none is the same for every part.
All inputs are finite; a program needn't handle non-finite values.
Results may differ from the reference program's by a relative error of at most 0.00558648.
Values are sent between devices in bfloat16 or wider.
A program may use at most 768 MiB of HBM per device.

```python
import jax
import jax.numpy as jnp
from jax import lax

REQUESTS = 48
SEQ_LEN = 6144
KV_RANK = 512
ROPE_DIM = 64
NUM_HEADS = 128

NORM_EPS = 1e-6
ATTN_SCALE = (KV_RANK + ROPE_DIM) ** -0.5


def setup_inputs(seed: int = 0, part: int = 0) -> dict:
    part_key = jax.random.fold_in(jax.random.key(seed), part)
    keys = jax.random.split(part_key, 8)
    shared = jax.random.split(jax.random.key(seed + 1), 2)
    row_scale = jnp.exp(0.5 * jax.random.normal(keys[0], (REQUESTS, SEQ_LEN, 1), jnp.float32))
    c_raw = (jax.random.normal(keys[1], (REQUESTS, SEQ_LEN, KV_RANK), jnp.float32) * row_scale).astype(jnp.bfloat16)
    k_raw = jax.random.normal(keys[2], (REQUESTS, SEQ_LEN, ROPE_DIM), jnp.float32).astype(jnp.bfloat16)
    norm_gain = (1.0 + 0.3 * jax.random.normal(shared[0], (KV_RANK,), jnp.float32)).astype(jnp.bfloat16)
    half_dim = ROPE_DIM // 2
    log_base = jax.random.uniform(shared[1], (), jnp.float32, 9.0, 14.0)
    inv_freq = jnp.exp(-log_base * (2.0 * jnp.arange(half_dim, dtype=jnp.float32) / ROPE_DIM))
    angles = jnp.arange(SEQ_LEN, dtype=jnp.float32)[:, None] * inv_freq[None, :]
    seq_lens = jax.random.randint(keys[3], (REQUESTS,), SEQ_LEN // 8, SEQ_LEN + 1)
    full_index = jax.random.randint(keys[4], (), 0, REQUESTS)
    short_offset = jax.random.randint(keys[5], (), 1, REQUESTS)
    seq_lens = seq_lens.at[full_index].set(SEQ_LEN)
    seq_lens = seq_lens.at[(full_index + short_offset) % REQUESTS].set(SEQ_LEN // 8)
    q_lat = (1.3 * jax.random.normal(keys[6], (REQUESTS, NUM_HEADS, KV_RANK), jnp.float32)).astype(jnp.bfloat16)
    q_rope = (3.0 * jax.random.normal(keys[7], (REQUESTS, NUM_HEADS, ROPE_DIM), jnp.float32)).astype(jnp.bfloat16)
    return {"c_raw": c_raw, "k_raw": k_raw, "norm_gain": norm_gain, "rope_cos": jnp.cos(angles), "rope_sin": jnp.sin(angles), "seq_lens": seq_lens.astype(jnp.int32), "q_lat": q_lat, "q_rope": q_rope}


def reference(c_raw, k_raw, norm_gain, rope_cos, rope_sin, seq_lens, q_lat, q_rope):
    positions = jnp.arange(SEQ_LEN)
    half_dim = ROPE_DIM // 2
    gain = norm_gain.astype(jnp.float32)

    def one_request(operands):
        c_row, k_row, length, lat_row, rope_row = operands
        valid = positions < length
        lat_f32 = c_row.astype(jnp.float32)
        inv_rms = lax.rsqrt(jnp.mean(lat_f32 * lat_f32, axis=-1, keepdims=True) + NORM_EPS)
        c_norm = jnp.where(valid[:, None], lat_f32 * inv_rms * gain, 0.0).astype(jnp.bfloat16)
        key_f32 = k_row.astype(jnp.float32)
        key_lo = key_f32[:, :half_dim]
        key_hi = key_f32[:, half_dim:]
        rotated = jnp.concatenate([key_lo * rope_cos - key_hi * rope_sin, key_hi * rope_cos + key_lo * rope_sin], axis=-1)
        k_rope = jnp.where(valid[:, None], rotated, 0.0).astype(jnp.bfloat16)
        scores = jnp.dot(lat_row, c_norm.T, preferred_element_type=jnp.float32) + jnp.dot(rope_row, k_rope.T, preferred_element_type=jnp.float32)
        scores = jnp.where(valid[None, :], scores * ATTN_SCALE, -1e30)
        weights = jnp.exp(scores - jnp.max(scores, axis=-1, keepdims=True))
        out_row = jnp.dot(weights, c_norm.astype(jnp.float32)) / jnp.sum(weights, axis=-1, keepdims=True)
        return c_norm, k_rope, out_row.astype(jnp.bfloat16)

    c_cache, kr_cache, o_lat = lax.map(one_request, (c_raw, k_raw, seq_lens, q_lat, q_rope))
    return (c_cache, kr_cache, o_lat)
```

```python
import functools

import jax
import jax.numpy as jnp
from jax import lax
from jax.experimental import pallas as pl
from jax.experimental.pallas import tpu as pltpu
from jax.sharding import PartitionSpec as P

NORM_EPS = 1e-6
CHUNKS = (1, 2, 2, 1)
VMEM_BYTES = 60 * 1024 * 1024


def pack_kernel(first, req_local, lens_ref, c_ref, k_ref, gain_ref, cos_ref, sin_ref, out_ref):
    rows, rank = c_ref.shape[1:]
    length = lens_ref[pl.program_id(0) * req_local + first + pl.program_id(1)]
    left = length - lax.axis_index("x") * rows

    @pl.when(left <= 0)
    def _():
        out_ref[...] = jnp.zeros_like(out_ref)

    @pl.when(left > 0)
    def _():
        lat = c_ref[0].astype(jnp.float32)
        inv = lax.rsqrt(jnp.mean(lat * lat, axis=-1, keepdims=True) + NORM_EPS)
        normed = lat * inv * gain_ref[...].astype(jnp.float32)
        valid = lax.broadcasted_iota(jnp.int32, (rows, 1), 0) < left
        out_ref[0, 0, :rows, :] = jnp.where(valid, normed, 0.0).astype(jnp.bfloat16)
        key = k_ref[0].astype(jnp.float32)
        half = key.shape[0] // 2
        lo, hi = key[:half], key[half:]
        cos, sin = cos_ref[...], sin_ref[...]
        valid = lax.broadcasted_iota(jnp.int32, (1, rows), 1) < left
        store_rope(out_ref, 0, jnp.where(valid, lo * cos - hi * sin, 0.0).astype(jnp.bfloat16), rows, rank)
        store_rope(out_ref, half, jnp.where(valid, hi * cos + lo * sin, 0.0).astype(jnp.bfloat16), rows, rank)


def store_rope(out_ref, at, keys, rows, rank):
    half = keys.shape[0]
    rest = rows - rank
    side = (at // half) * rest
    out_ref[0, 0, rows + at : rows + at + half, :] = keys[:, :rank]
    out_ref[0, 0, rows + 2 * half : rows + 3 * half, side : side + rest] = keys[:, rank:]


def load_rope(land_ref, kr_ref, rows, rank):
    half = kr_ref.shape[1] // 2
    rest = rows - rank
    kr_ref[0, :, :rank] = land_ref[0, 0, rows : rows + 2 * half, :]
    for at in (0, 1):
        kr_ref[0, at * half : (at + 1) * half, rank:] = land_ref[0, 0, rows + 2 * half : rows + 3 * half, at * rest : (at + 1) * rest]


def pack(lens, c_raw, k_raw, gain, cos, sin, n, req_local, first, count):
    requests, rows, rank = c_raw.shape
    width = k_raw.shape[1]
    total = rows + rows * width // rank
    req = lambda d, m, *_: (d * req_local + first + m, 0, 0)
    fixed = lambda d, m, *_: (0, 0)
    return pl.pallas_call(
        functools.partial(pack_kernel, first, req_local),
        grid_spec=pltpu.PrefetchScalarGridSpec(
            num_scalar_prefetch=1,
            grid=(n, count),
            in_specs=[
                pl.BlockSpec((1, rows, rank), req),
                pl.BlockSpec((1, width, rows), req),
                pl.BlockSpec((1, rank), fixed),
                pl.BlockSpec((width // 2, rows), fixed),
                pl.BlockSpec((width // 2, rows), fixed),
            ],
            out_specs=pl.BlockSpec((1, 1, total, rank), lambda d, m, *_: (d, m, 0, 0)),
        ),
        out_shape=jax.ShapeDtypeStruct((n, count, total, rank), jnp.bfloat16),
        compiler_params=pltpu.CompilerParams(vmem_limit_bytes=VMEM_BYTES),
        cost_estimate=pl.CostEstimate(flops=n * count * rows * rank * 100, bytes_accessed=n * count * total * rank * 4, transcendentals=0),
        name=f"pack_{first}",
    )(lens, c_raw, k_raw, gain, cos, sin)


def attend_kernel(n, scale, lens_ref, land_ref, qa_ref, qr_ref, *rest):
    c_out, kr_out, o_out, m_scr, l_scr, acc_scr = rest[-6:]
    slot, blk = pl.program_id(0), pl.program_id(1)
    rows, rank = c_out.shape[1:]
    length = lens_ref[slot]

    @pl.when(blk == 0)
    def _():
        m_scr[...] = jnp.full_like(m_scr, -1e30)
        l_scr[...] = jnp.zeros_like(l_scr)
        acc_scr[...] = jnp.zeros_like(acc_scr)

    @pl.when(blk * rows >= length)
    def _():
        c_out[...] = jnp.zeros_like(c_out)
        kr_out[...] = jnp.zeros_like(kr_out)

    @pl.when(blk * rows < length)
    def _():
        lat = land_ref[0, 0, :rows, :]
        c_out[0] = lat
        load_rope(land_ref, kr_out, rows, rank)
        contract = (((1,), (1,)), ((), ()))
        s = lax.dot_general(qa_ref[0], lat, contract, preferred_element_type=jnp.float32)
        s = s + jnp.dot(qr_ref[0], kr_out[0], preferred_element_type=jnp.float32)
        pos = blk * rows + lax.broadcasted_iota(jnp.int32, (1, rows), 1)
        s = jnp.where(pos < length, s * scale, -1e30)
        m_old = m_scr[...]
        m_new = jnp.maximum(m_old, jnp.max(s, axis=-1, keepdims=True))
        alpha = jnp.exp(m_old - m_new)
        p = jnp.exp(s - m_new)
        l_scr[...] = l_scr[...] * alpha + jnp.sum(p, axis=-1, keepdims=True)
        m_scr[...] = m_new
        acc_scr[...] = acc_scr[...] * alpha + lax.dot_general(
            p.astype(jnp.bfloat16), lat, (((1,), (0,)), ((), ())), preferred_element_type=jnp.float32)

    @pl.when(blk == n - 1)
    def _():
        o_out[0] = (acc_scr[...] / l_scr[...]).astype(jnp.bfloat16)


def attend(own_lens, landed, q_lat, q_rope, prev, n, rows, first, count):
    req_local, heads, rank = q_lat.shape
    width = q_rope.shape[2]
    total = landed.shape[2]
    scale = (rank + width) ** -0.5
    outs = [
        jax.ShapeDtypeStruct((req_local, n * rows, rank), jnp.bfloat16),
        jax.ShapeDtypeStruct((req_local, width, n * rows), jnp.bfloat16),
        jax.ShapeDtypeStruct((req_local, heads, rank), jnp.bfloat16),
    ]
    land = lambda m, i, lens: (jnp.minimum(i, (lens[m] - 1) // rows), m, 0, 0)
    slot = lambda m, i, lens: (first + m, 0, 0)
    any_spec = pl.BlockSpec(memory_space=pl.ANY)
    prev = list(prev) if prev is not None else []
    return pl.pallas_call(
        functools.partial(attend_kernel, n, scale),
        grid_spec=pltpu.PrefetchScalarGridSpec(
            num_scalar_prefetch=1,
            grid=(count, n),
            in_specs=[
                pl.BlockSpec((1, 1, total, rank), land),
                pl.BlockSpec((1, heads, rank), slot),
                pl.BlockSpec((1, heads, width), slot),
            ] + [any_spec] * len(prev),
            out_specs=[
                pl.BlockSpec((1, rows, rank), lambda m, i, lens: (first + m, i, 0)),
                pl.BlockSpec((1, width, rows), lambda m, i, lens: (first + m, 0, i)),
                pl.BlockSpec((1, heads, rank), slot),
            ],
            scratch_shapes=[
                pltpu.VMEM((heads, 1), jnp.float32),
                pltpu.VMEM((heads, 1), jnp.float32),
                pltpu.VMEM((heads, rank), jnp.float32),
            ],
        ),
        out_shape=outs,
        input_output_aliases={4 + k: k for k in range(len(prev))},
        compiler_params=pltpu.CompilerParams(vmem_limit_bytes=VMEM_BYTES),
        cost_estimate=pl.CostEstimate(flops=count * n * rows * heads * (2 * rank + width) * 2, bytes_accessed=count * n * rows * rank * 4, transcendentals=0),
        name=f"attend_{first}",
    )(own_lens[first : first + count], landed, q_lat, q_rope, *prev)


def solution(mesh):
    seq_spec = P("dp", "x", None)
    req_spec = P(("dp", "x"), None, None)
    n = mesh.shape["x"]

    def local_step(c_raw, k_raw, norm_gain, rope_cos, rope_sin, seq_lens, q_lat, q_rope):
        rows = c_raw.shape[1]
        req_local = q_lat.shape[0]
        own_lens = lax.dynamic_slice_in_dim(seq_lens, lax.axis_index("x") * req_local, req_local)
        k_raw = jnp.swapaxes(k_raw, 1, 2)
        tables = (norm_gain[None, :], rope_cos.T, rope_sin.T)
        landed, first = [], 0
        for count in CHUNKS:
            packed = pack(seq_lens, c_raw, k_raw, *tables, n, req_local, first, count)
            landed.append((first, count, lax.all_to_all(packed, "x", 0, 0, tiled=True)))
            first += count
        outs = None
        for first, count, block in landed:
            outs = attend(own_lens, block, q_lat, q_rope, outs, n, rows, first, count)
        return outs[0], jnp.swapaxes(outs[1], 1, 2), outs[2]

    return jax.shard_map(local_step, mesh=mesh, in_specs=(seq_spec, seq_spec, P(None), P("x", None), P("x", None), P("dp"), req_spec, req_spec), out_specs=(req_spec, req_spec, req_spec), check_vma=False)
```

```python
import functools

import jax
import jax.numpy as jnp
from jax import lax
from jax.experimental import pallas as pl
from jax.experimental.pallas import tpu as pltpu
from jax.sharding import PartitionSpec as P

NORM_EPS = 1e-6
TAIL = 1
DEPTH = 3
STRIPE = 128
VMEM_BYTES = 60 * 1024 * 1024


def peer(j, n):
    me = lax.axis_index("x")
    chip, core = me // 2, me % 2
    far = j % 3
    hop = (1 - j // (n - 2)) * (1 + 2 * far - 3 * (far // 2))
    other = (j // 3) % 2 * (1 - j // (n - 2)) + (j // (n - 2)) * (1 - j % (n - 2))
    chips = n // 2
    return (chip + hop) % chips * 2 + (core + other) % 2


def send_kernel(n, req_local, tail, lens_ref, c_hbm, k_hbm, gain_ref, cos_ref, sin_ref, land_ref, rest_ref,
                c_buf, k_buf, out_buf, c_sem, k_sem, send_sem, recv_sem):
    me = lax.axis_index("x")
    early = req_local - tail
    steps = req_local * n
    depth = out_buf.shape[0]
    rows, rank = c_buf.shape[1:]

    def load(t):
        req = peer(t % n, n) * req_local + t // n
        slot = t % 2
        return (pltpu.make_async_copy(c_hbm.at[req], c_buf.at[slot], c_sem.at[slot]),
                pltpu.make_async_copy(k_hbm.at[req], k_buf.at[slot], k_sem.at[slot]))

    def remote(t):
        dst, m, slot = peer(t % n, n), t // n, t % depth
        return pltpu.make_async_remote_copy(
            src_ref=out_buf.at[slot], dst_ref=land_ref.at[m, me], send_sem=send_sem.at[slot],
            recv_sem=recv_sem.at[m * n + me], device_id={"x": dst}, device_id_type=pl.DeviceIdType.MESH)

    def own(t):
        slot = t % depth
        return pltpu.make_async_copy(out_buf.at[slot], land_ref.at[t // n, me], send_sem.at[slot])

    def keep(t):
        dst, m, slot = peer(t % n, n), t // n, t % depth
        return pltpu.make_async_copy(out_buf.at[slot], rest_ref.at[dst, m - early], send_sem.at[slot])

    def on_kind(t, act_remote, act_local):
        is_tail = t >= early * n
        is_own = t % n == n - 1

        @pl.when(is_tail)
        def _():
            act_local(keep(t))

        @pl.when(jnp.logical_and(jnp.logical_not(is_tail), is_own))
        def _():
            act_local(own(t))

        @pl.when(jnp.logical_and(jnp.logical_not(is_tail), jnp.logical_not(is_own)))
        def _():
            act_remote(remote(t))

    def start(t):
        on_kind(t, lambda c: c.start(), lambda c: c.start())

    def sent(t):
        on_kind(t, lambda c: c.wait_send(), lambda c: c.wait())

    barrier = pltpu.get_barrier_semaphore()
    for j in range(n - 1):
        pl.semaphore_signal(barrier, inc=1, device_id={"x": peer(j, n)}, device_id_type=pl.DeviceIdType.MESH)
    for t in range(2):
        for c in load(t):
            c.start()
    pl.semaphore_wait(barrier, n - 1)

    @pl.loop(0, steps)
    def _(t):
        @pl.when(t >= depth)
        def _():
            sent(t - depth)

        for c in load(t):
            c.wait()
        slot, out = t % 2, t % depth
        left = lens_ref[peer(t % n, n) * req_local + t // n] - me * rows

        @pl.loop(0, rows, step=STRIPE)
        def _(r):
            r = pl.multiple_of(r, STRIPE)
            lat = c_buf[slot, pl.ds(r, STRIPE), :].astype(jnp.float32)
            inv = lax.rsqrt(jnp.mean(lat * lat, axis=-1, keepdims=True) + NORM_EPS)
            normed = lat * inv * gain_ref[...].astype(jnp.float32)
            valid = r + lax.broadcasted_iota(jnp.int32, (STRIPE, 1), 0) < left
            out_buf[out, pl.ds(r, STRIPE), :] = jnp.where(valid, normed, 0.0).astype(jnp.bfloat16)

        key = k_buf[slot].astype(jnp.float32)
        half = key.shape[0] // 2
        lo, hi = key[:half], key[half:]
        cos, sin = cos_ref[...], sin_ref[...]
        valid = lax.broadcasted_iota(jnp.int32, (1, rows), 1) < left
        store_rope(out_buf, out, 0, jnp.where(valid, lo * cos - hi * sin, 0.0).astype(jnp.bfloat16), rows, rank)
        store_rope(out_buf, out, half, jnp.where(valid, hi * cos + lo * sin, 0.0).astype(jnp.bfloat16), rows, rank)

        @pl.when(t + 2 < steps)
        def _():
            for c in load(t + 2):
                c.start()

        @pl.when(t >= 1)
        def _():
            start(t - 1)

    @pl.loop(steps - depth, steps - 1)
    def _(t):
        sent(t)

    start(steps - 1)
    sent(steps - 1)

    @pl.loop(0, early)
    def _(m):
        @pl.loop(0, n - 1)
        def _(j):
            src = peer(j, n)
            pltpu.make_async_remote_copy(
                src_ref=land_ref.at[m, src], dst_ref=land_ref.at[m, src], send_sem=send_sem.at[0],
                recv_sem=recv_sem.at[m * n + src], device_id={"x": src}, device_id_type=pl.DeviceIdType.MESH).wait_recv()


def store_rope(out_ref, slot, at, keys, rows, rank):
    half = keys.shape[0]
    rest = rows - rank
    side = (at // half) * rest
    out_ref[slot, rows + at : rows + at + half, :] = keys[:, :rank]
    out_ref[slot, rows + 2 * half : rows + 3 * half, side : side + rest] = keys[:, rank:]


def load_rope(land_ref, kr_ref, rows, rank):
    half = kr_ref.shape[1] // 2
    rest = rows - rank
    kr_ref[0, :, :rank] = land_ref[0, 0, rows : rows + 2 * half, :]
    for at in (0, 1):
        kr_ref[0, at * half : (at + 1) * half, rank:] = land_ref[0, 0, rows + 2 * half : rows + 3 * half, at * rest : (at + 1) * rest]


def send(lens, c_raw, k_raw, gain, cos, sin, n, req_local, tail):
    requests, rows, rank = c_raw.shape
    width = k_raw.shape[1]
    total = rows + rows * width // rank
    depth = DEPTH * n
    hbm = pl.BlockSpec(memory_space=pl.ANY)
    vmem = pl.BlockSpec(memory_space=pltpu.VMEM)
    early = req_local - tail
    return pl.pallas_call(
        functools.partial(send_kernel, n, req_local, tail),
        in_specs=[pl.BlockSpec(memory_space=pltpu.SMEM), hbm, hbm, vmem, vmem, vmem],
        out_specs=[hbm, hbm],
        out_shape=[jax.ShapeDtypeStruct((early, n, total, rank), jnp.bfloat16),
                   jax.ShapeDtypeStruct((n, tail, total, rank), jnp.bfloat16)],
        scratch_shapes=[
            pltpu.VMEM((2, rows, rank), jnp.bfloat16),
            pltpu.VMEM((2, width, rows), jnp.bfloat16),
            pltpu.VMEM((depth, total, rank), jnp.bfloat16),
            pltpu.SemaphoreType.DMA((2,)),
            pltpu.SemaphoreType.DMA((2,)),
            pltpu.SemaphoreType.DMA((depth,)),
            pltpu.SemaphoreType.DMA((early * n,)),
        ],
        compiler_params=pltpu.CompilerParams(vmem_limit_bytes=VMEM_BYTES, collective_id=0, has_side_effects=True),
        cost_estimate=pl.CostEstimate(flops=requests * rows * rank * 100, bytes_accessed=requests * total * rank * 4, transcendentals=0),
        name="send",
    )(lens, c_raw, k_raw, gain, cos, sin)


def attend_kernel(n, scale, lens_ref, land_ref, qa_ref, qr_ref, *rest):
    c_out, kr_out, o_out, m_scr, l_scr, acc_scr = rest[-6:]
    slot, blk = pl.program_id(0), pl.program_id(1)
    rows, rank = c_out.shape[1:]
    length = lens_ref[slot]

    @pl.when(blk == 0)
    def _():
        m_scr[...] = jnp.full_like(m_scr, -1e30)
        l_scr[...] = jnp.zeros_like(l_scr)
        acc_scr[...] = jnp.zeros_like(acc_scr)

    @pl.when(blk * rows >= length)
    def _():
        c_out[...] = jnp.zeros_like(c_out)
        kr_out[...] = jnp.zeros_like(kr_out)

    @pl.when(blk * rows < length)
    def _():
        lat = land_ref[0, 0, :rows, :]
        c_out[0] = lat
        load_rope(land_ref, kr_out, rows, rank)
        contract = (((1,), (1,)), ((), ()))
        s = lax.dot_general(qa_ref[0], lat, contract, preferred_element_type=jnp.float32)
        s = s + jnp.dot(qr_ref[0], kr_out[0], preferred_element_type=jnp.float32)
        pos = blk * rows + lax.broadcasted_iota(jnp.int32, (1, rows), 1)
        s = jnp.where(pos < length, s * scale, -1e30)
        m_old = m_scr[...]
        m_new = jnp.maximum(m_old, jnp.max(s, axis=-1, keepdims=True))
        alpha = jnp.exp(m_old - m_new)
        p = jnp.exp(s - m_new)
        l_scr[...] = l_scr[...] * alpha + jnp.sum(p, axis=-1, keepdims=True)
        m_scr[...] = m_new
        acc_scr[...] = acc_scr[...] * alpha + lax.dot_general(
            p.astype(jnp.bfloat16), lat, (((1,), (0,)), ((), ())), preferred_element_type=jnp.float32)

    @pl.when(blk == n - 1)
    def _():
        o_out[0] = (acc_scr[...] / l_scr[...]).astype(jnp.bfloat16)


def attend(own_lens, landed, by_slot, q_lat, q_rope, prev, n, rows, first, count):
    req_local, heads, rank = q_lat.shape
    width = q_rope.shape[2]
    total = landed.shape[2]
    scale = (rank + width) ** -0.5
    outs = [
        jax.ShapeDtypeStruct((req_local, n * rows, rank), jnp.bfloat16),
        jax.ShapeDtypeStruct((req_local, width, n * rows), jnp.bfloat16),
        jax.ShapeDtypeStruct((req_local, heads, rank), jnp.bfloat16),
    ]

    def land(m, i, lens):
        i = jnp.minimum(i, (lens[m] - 1) // rows)
        return (m, i, 0, 0) if by_slot else (i, m, 0, 0)

    slot = lambda m, i, lens: (first + m, 0, 0)
    any_spec = pl.BlockSpec(memory_space=pl.ANY)
    prev = list(prev) if prev is not None else []
    return pl.pallas_call(
        functools.partial(attend_kernel, n, scale),
        grid_spec=pltpu.PrefetchScalarGridSpec(
            num_scalar_prefetch=1,
            grid=(count, n),
            in_specs=[
                pl.BlockSpec((1, 1, total, rank), land),
                pl.BlockSpec((1, heads, rank), slot),
                pl.BlockSpec((1, heads, width), slot),
            ] + [any_spec] * len(prev),
            out_specs=[
                pl.BlockSpec((1, rows, rank), lambda m, i, lens: (first + m, i, 0)),
                pl.BlockSpec((1, width, rows), lambda m, i, lens: (first + m, 0, i)),
                pl.BlockSpec((1, heads, rank), slot),
            ],
            scratch_shapes=[
                pltpu.VMEM((heads, 1), jnp.float32),
                pltpu.VMEM((heads, 1), jnp.float32),
                pltpu.VMEM((heads, rank), jnp.float32),
            ],
        ),
        out_shape=outs,
        input_output_aliases={4 + k: k for k in range(len(prev))},
        compiler_params=pltpu.CompilerParams(vmem_limit_bytes=VMEM_BYTES),
        cost_estimate=pl.CostEstimate(flops=count * n * rows * heads * (2 * rank + width) * 2, bytes_accessed=count * n * rows * rank * 4, transcendentals=0),
        name=f"attend_{first}",
    )(own_lens[first : first + count], landed, q_lat, q_rope, *prev)


def solution(mesh):
    seq_spec = P("dp", "x", None)
    req_spec = P(("dp", "x"), None, None)
    n = mesh.shape["x"]

    def local_step(c_raw, k_raw, norm_gain, rope_cos, rope_sin, seq_lens, q_lat, q_rope):
        rows = c_raw.shape[1]
        req_local = q_lat.shape[0]
        own_lens = lax.dynamic_slice_in_dim(seq_lens, lax.axis_index("x") * req_local, req_local)
        k_raw = jnp.swapaxes(k_raw, 1, 2)
        tables = (norm_gain[None, :], rope_cos.T, rope_sin.T)
        early = req_local - TAIL
        landed, rest = send(seq_lens, c_raw, k_raw, *tables, n, req_local, TAIL)
        rest = lax.all_to_all(rest, "x", 0, 0, tiled=True)
        outs = attend(own_lens, landed, True, q_lat, q_rope, None, n, rows, 0, early)
        outs = attend(own_lens, rest, False, q_lat, q_rope, outs, n, rows, early, TAIL)
        return outs[0], jnp.swapaxes(outs[1], 1, 2), outs[2]

    return jax.shard_map(local_step, mesh=mesh, in_specs=(seq_spec, seq_spec, P(None), P("x", None), P("x", None), P("dp"), req_spec, req_spec), out_specs=(req_spec, req_spec, req_spec), check_vma=False)
```

```python
import functools

import jax
import jax.numpy as jnp
from jax import lax
from jax.experimental import pallas as pl
from jax.experimental.pallas import tpu as pltpu
from jax.sharding import PartitionSpec as P

NORM_EPS = 1e-6
HALVES = 2
ROUNDS = 6
LOADS = 4
STRIPE = 128
LANES, SUBLANES = 128, 16
VMEM_BYTES = 60 * 1024 * 1024
ATTEND_BYTES = 52 * 1024 * 1024
MESH = pl.DeviceIdType.MESH
HBM = pl.BlockSpec(memory_space=pltpu.HBM)
VMEM = pl.BlockSpec(memory_space=pltpu.VMEM)
SMEM = pl.BlockSpec(memory_space=pltpu.SMEM)


def peer(j, n):
    me = lax.axis_index("x")
    chip, core = me // 2, me % 2
    far = j % 3
    last = j // (n - 2)
    hop = (1 - last) * (1 + 2 * far - 3 * (far // 2))
    other = (j // 3) % 2 * (1 - last) + last * (1 - j % (n - 2))
    return (chip + hop) % (n // 2) * 2 + (core + other) % 2


def rope_tiles(width, rows):
    for r in range(width // SUBLANES):
        for c in range(rows // LANES):
            yield (slice(r * SUBLANES, (r + 1) * SUBLANES), slice(c * LANES, (c + 1) * LANES),
                   slice(rows + c * SUBLANES, rows + (c + 1) * SUBLANES), slice(r * LANES, (r + 1) * LANES))


def send_kernel(n, req_local, lens_ref, c_hbm, k_hbm, gain_ref, cos_ref, sin_ref, land_ref, rest_ref,
                c_buf, k_buf, out_buf, c_sem, k_sem, send_sem, recv_sem):
    me = lax.axis_index("x")
    rounds = req_local * HALVES
    steps = rounds * n
    early = (rounds - 1) * n
    depth = out_buf.shape[0]
    rows, rank = c_buf.shape[1:]
    width = k_buf.shape[1]

    def load(t):
        req = peer(t % n, n) * req_local + t // n // HALVES
        first = pl.multiple_of(t // n % HALVES * rows, rows)
        slot = t % LOADS
        return (pltpu.make_async_copy(c_hbm.at[req, pl.ds(first, rows), :], c_buf.at[slot], c_sem.at[slot]),
                pltpu.make_async_copy(k_hbm.at[req, :, pl.ds(first, rows)], k_buf.at[slot], k_sem.at[slot]))

    def landing(t):
        return land_ref.at[t // n // HALVES, me, t // n % HALVES]

    def remote(t):
        slot = t % depth
        return pltpu.make_async_remote_copy(
            src_ref=out_buf.at[slot], dst_ref=landing(t), send_sem=send_sem.at[slot],
            recv_sem=recv_sem.at[t // n * n + me], device_id={"x": peer(t % n, n)}, device_id_type=MESH)

    def own(t):
        return pltpu.make_async_copy(out_buf.at[t % depth], landing(t), send_sem.at[t % depth])

    def keep(t):
        return pltpu.make_async_copy(out_buf.at[t % depth], rest_ref.at[peer(t % n, n)], send_sem.at[t % depth])

    def on_kind(t, act_remote, act_local):
        is_own = t % n == n - 1

        @pl.when(t >= early)
        def _():
            act_local(keep(t))

        @pl.when(jnp.logical_and(t < early, is_own))
        def _():
            act_local(own(t))

        @pl.when(jnp.logical_and(t < early, jnp.logical_not(is_own)))
        def _():
            act_remote(remote(t))

    def start(t):
        on_kind(t, lambda c: c.start(), lambda c: c.start())

    def sent(t):
        on_kind(t, lambda c: c.wait_send(), lambda c: c.wait())

    def pack(t):
        for c in load(t):
            c.wait()
        slot, out = t % LOADS, t % depth
        first = t // n % HALVES * rows
        left = lens_ref[peer(t % n, n) * req_local + t // n // HALVES] - me * (rows * HALVES) - first
        gain = gain_ref[...].astype(jnp.float32)

        @pl.loop(0, rows, step=STRIPE)
        def _(r):
            r = pl.multiple_of(r, STRIPE)
            lat = c_buf[slot, pl.ds(r, STRIPE), :].astype(jnp.float32)
            inv = lax.rsqrt(jnp.mean(lat * lat, axis=-1, keepdims=True) + NORM_EPS)
            valid = r + lax.broadcasted_iota(jnp.int32, (STRIPE, 1), 0) < left
            out_buf[out, pl.ds(r, STRIPE), :] = jnp.where(valid, lat * inv * gain, 0.0).astype(jnp.bfloat16)

        key = k_buf[slot].astype(jnp.float32)
        half = width // 2
        lo, hi = key[:half], key[half:]
        first = pl.multiple_of(first, LANES)
        cos, sin = cos_ref[:, pl.ds(first, rows)], sin_ref[:, pl.ds(first, rows)]
        valid = lax.broadcasted_iota(jnp.int32, (1, rows), 1) < left
        rotated = (jnp.where(valid, lo * cos - hi * sin, 0.0).astype(jnp.bfloat16),
                   jnp.where(valid, hi * cos + lo * sin, 0.0).astype(jnp.bfloat16))
        for kr_rows, kr_cols, to_rows, to_cols in rope_tiles(width, rows):
            part, at = kr_rows.start // half, kr_rows.start % half
            out_buf[out, to_rows, to_cols] = rotated[part][at : at + SUBLANES, kr_cols]

    barrier = pltpu.get_barrier_semaphore()
    for j in range(n - 1):
        pl.semaphore_signal(barrier, inc=1, device_id={"x": peer(j, n)}, device_id_type=MESH)
    for t in range(LOADS):
        for c in load(t):
            c.start()
    pack(0)
    for c in load(LOADS):
        c.start()
    pl.semaphore_wait(barrier, n - 1)

    @pl.loop(1, steps)
    def _(t):
        @pl.when(t >= depth)
        def _():
            sent(t - depth)

        pack(t)

        @pl.when(t + LOADS < steps)
        def _():
            for c in load(t + LOADS):
                c.start()

        start(t - 1)

    @pl.loop(steps - depth, steps - 1)
    def _(t):
        sent(t)

    start(steps - 1)
    sent(steps - 1)

    @pl.loop(0, rounds - 1)
    def _(r):
        @pl.loop(0, n - 1)
        def _(j):
            src = peer(j, n)
            piece = land_ref.at[r // HALVES, src, r % HALVES]
            pltpu.make_async_remote_copy(
                src_ref=piece, dst_ref=piece, send_sem=send_sem.at[0], recv_sem=recv_sem.at[r * n + src],
                device_id={"x": src}, device_id_type=MESH).wait_recv()


def send(lens, c_raw, k_raw, gain, cos, sin, n, req_local):
    requests, block, rank = c_raw.shape
    width = k_raw.shape[1]
    rows = block // HALVES
    total = rows + rows * width // rank
    depth = ROUNDS * n
    return pl.pallas_call(
        functools.partial(send_kernel, n, req_local),
        in_specs=[SMEM, HBM, HBM, VMEM, VMEM, VMEM],
        out_specs=[HBM, HBM],
        out_shape=[jax.ShapeDtypeStruct((req_local, n, HALVES, total, rank), jnp.bfloat16),
                   jax.ShapeDtypeStruct((n, total, rank), jnp.bfloat16)],
        scratch_shapes=[
            pltpu.VMEM((LOADS, rows, rank), jnp.bfloat16),
            pltpu.VMEM((LOADS, width, rows), jnp.bfloat16),
            pltpu.VMEM((depth, total, rank), jnp.bfloat16),
            pltpu.SemaphoreType.DMA((LOADS,)),
            pltpu.SemaphoreType.DMA((LOADS,)),
            pltpu.SemaphoreType.DMA((depth,)),
            pltpu.SemaphoreType.DMA(((req_local * HALVES - 1) * n,)),
        ],
        compiler_params=pltpu.CompilerParams(vmem_limit_bytes=VMEM_BYTES, collective_id=0, has_side_effects=True),
        cost_estimate=pl.CostEstimate(flops=requests * block * rank * 100, bytes_accessed=requests * block * rank * 4, transcendentals=0),
        name="send",
    )(lens, c_raw, k_raw, gain, cos, sin)


def stream(n, req_local, scale, group, length, land, queries, c_out, kr_out, state, buf, kr_buf, zero_c, zero_k, in_sem, c_sem, k_sem, ahead):
    first_req, count, first_piece, pieces = group
    m_ref, l_ref, acc_ref = state
    depth = buf.shape[0]
    rank = buf.shape[3]
    width = kr_buf.shape[1]
    rows = buf.shape[2] * rank // (rank + width)
    span = rows * HALVES
    steps = count * n

    def used(t):
        return t % n * span + first_piece * rows < length(first_req + t // n)

    def load(t):
        return pltpu.make_async_copy(land(t // n, t % n), buf.at[t % depth, pl.ds(0, pieces)], in_sem.at[t % depth])

    def stores(t):
        slot, req = t % depth, first_req + t // n
        at = pl.multiple_of(t % n * span + first_piece * rows, rows)
        kr = pltpu.make_async_copy(kr_buf.at[slot, :, pl.ds(0, pieces * rows)], kr_out.at[req, :, pl.ds(at, pieces * rows)], k_sem.at[slot])
        cs = [pltpu.make_async_copy(buf.at[slot, h, pl.ds(0, rows), :], c_out.at[req, pl.ds(at + h * rows, rows), :], c_sem.at[slot, h]) for h in range(pieces)]
        return cs + [kr]

    def blanks(t):
        slot, req = t % depth, first_req + t // n
        at = pl.multiple_of(t % n * span + first_piece * rows, rows)
        kr = pltpu.make_async_copy(zero_k.at[:, pl.ds(0, pieces * rows)], kr_out.at[req, :, pl.ds(at, pieces * rows)], k_sem.at[slot])
        cs = [pltpu.make_async_copy(zero_c, c_out.at[req, pl.ds(at + h * rows, rows), :], c_sem.at[slot, h]) for h in range(pieces)]
        return cs + [kr]

    def fetch(t):
        @pl.when(used(t))
        def _():
            load(t).start()

    def work(t):
        slot, req = t % depth, first_req + t // n
        load(t).wait()
        for h in range(pieces):
            for kr_rows, kr_cols, from_rows, from_cols in rope_tiles(width, rows):
                cols = slice(h * rows + kr_cols.start, h * rows + kr_cols.stop)
                kr_buf[slot, kr_rows, cols] = buf[slot, h, from_rows, from_cols]
        for c in stores(t):
            c.start()
        qa, qr = queries(t)
        scores = []
        for h in range(pieces):
            s = lax.dot_general(qa, buf[slot, h, :rows, :], (((1,), (1,)), ((), ())), preferred_element_type=jnp.float32)
            s = s + lax.dot_general(qr, kr_buf[slot, :, h * rows : (h + 1) * rows], (((0,), (0,)), ((), ())), preferred_element_type=jnp.float32)
            pos = t % n * span + (first_piece + h) * rows + lax.broadcasted_iota(jnp.int32, (1, rows), 1)
            scores.append(jnp.where(pos < length(req), s * scale, -1e30))
        m_old = m_ref[...]
        m_new = m_old
        for s in scores:
            m_new = jnp.maximum(m_new, jnp.max(s, axis=-1, keepdims=True))
        alpha = jnp.exp(m_old - m_new)
        total, acc = l_ref[...] * alpha, acc_ref[...] * alpha
        for h, s in enumerate(scores):
            p = jnp.exp(s - m_new)
            total = total + jnp.sum(p, axis=-1, keepdims=True)
            acc = acc + jnp.dot(p.astype(jnp.bfloat16), buf[slot, h, :rows, :], preferred_element_type=jnp.float32)
        m_ref[...], l_ref[...], acc_ref[...] = m_new, total, acc

    def body(t, begin, finish):
        @pl.when(t % n == 0)
        def _():
            begin()

        @pl.when(used(t))
        def _():
            work(t)

        @pl.when(jnp.logical_not(used(t)))
        def _():
            for c in blanks(t):
                c.start()

        @pl.when(t + ahead < steps)
        def _():
            @pl.when(t + ahead >= depth)
            def _():
                for c in stores(t + ahead - depth):
                    c.wait()

            fetch(t + ahead)

        @pl.when(t % n == n - 1)
        def _():
            finish(first_req + t // n)

    def run(begin, finish):
        for t in range(min(ahead, steps)):
            fetch(t)

        @pl.loop(0, steps)
        def _(t):
            body(t, begin, finish)

        @pl.loop(max(steps - depth, 0), steps)
        def _(t):
            for c in stores(t):
                c.wait()

    return run


def clear(state):
    m_ref, l_ref, acc_ref = state
    m_ref[...] = jnp.full_like(m_ref, -1e30)
    l_ref[...] = jnp.zeros_like(l_ref)
    acc_ref[...] = jnp.zeros_like(acc_ref)


def first_kernel(n, req_local, scale, lens_ref, land_ref, qa_ref, qr_ref, c_out, kr_out, o_out, part_out,
                 m_ref, l_ref, acc_ref, part_ref, part_sem, zero_c, zero_k, buf, in_sem, kr_buf, c_sem, k_sem):
    length = lambda m: lens_ref[lax.axis_index("x") * req_local + m]
    zero_c[...] = jnp.zeros_like(zero_c)
    zero_k[...] = jnp.zeros_like(zero_k)
    state = (m_ref, l_ref, acc_ref)
    rest = (c_out, kr_out, state, buf, kr_buf, zero_c, zero_k, in_sem, c_sem, k_sem, buf.shape[0] // 2)
    last = req_local - 1
    rank = acc_ref.shape[1]

    def finish(m):
        o_out[m] = (acc_ref[...] / l_ref[...]).astype(jnp.bfloat16)

    def hand_over(m):
        part_ref[:, :rank] = acc_ref[...]
        part_ref[:, rank : rank + LANES] = jnp.broadcast_to(m_ref[...], (part_ref.shape[0], LANES))
        part_ref[:, rank + LANES :] = jnp.broadcast_to(l_ref[...], (part_ref.shape[0], LANES))
        copy = pltpu.make_async_copy(part_ref, part_out, part_sem)
        copy.start()
        copy.wait()

    whole = lambda m, i: land_ref.at[m, i]
    stream(n, req_local, scale, (0, last, 0, HALVES), length, whole, lambda t: (qa_ref[t // n], qr_ref[t // n]), *rest)(lambda: clear(state), finish)
    piece = lambda m, i: land_ref.at[last, i, pl.ds(0, HALVES - 1)]
    stream(n, req_local, scale, (last, 1, 0, HALVES - 1), length, piece, lambda t: (qa_ref[last], qr_ref[last]), *rest)(lambda: clear(state), hand_over)


def last_kernel(n, req_local, scale, lens_ref, land_ref, qa_hbm, qr_hbm, part_hbm, c_old, kr_old, o_old, c_out, kr_out, o_out,
                m_ref, l_ref, acc_ref, qa_ref, qr_ref, part_ref, o_buf, sems, zero_c, zero_k, buf, in_sem, kr_buf, c_sem, k_sem):
    length = lambda m: lens_ref[lax.axis_index("x") * req_local + m]
    last = req_local - 1
    state = (m_ref, l_ref, acc_ref)
    rank = acc_ref.shape[1]
    copies = [pltpu.make_async_copy(qa_hbm.at[last], qa_ref, sems.at[0]), pltpu.make_async_copy(qr_hbm.at[last], qr_ref, sems.at[1]),
              pltpu.make_async_copy(part_hbm, part_ref, sems.at[2])]
    for c in copies:
        c.start()
    zero_c[...] = jnp.zeros_like(zero_c)
    zero_k[...] = jnp.zeros_like(zero_k)

    def begin():
        clear(state)
        for c in copies:
            c.wait()

    def finish(m):
        m_part, l_part, acc_part = part_ref[:, rank : rank + 1], part_ref[:, rank + LANES : rank + LANES + 1], part_ref[:, :rank]
        m_new = jnp.maximum(m_ref[...], m_part)
        here, there = jnp.exp(m_ref[...] - m_new), jnp.exp(m_part - m_new)
        total = l_ref[...] * here + l_part * there
        o_buf[...] = ((acc_ref[...] * here + acc_part * there) / total).astype(jnp.bfloat16)
        copy = pltpu.make_async_copy(o_buf, o_out.at[m], sems.at[3])
        copy.start()
        copy.wait()

    stream(n, req_local, scale, (last, 1, HALVES - 1, 1), length, lambda m, i: land_ref.at[i], lambda t: (qa_ref[...], qr_ref[...]), c_out, kr_out, state, buf, kr_buf,
           zero_c, zero_k, in_sem, c_sem, k_sem, buf.shape[0])(begin, finish)


def attend(lens, landed, rest, q_lat, q_rope, n, block):
    req_local, heads, rank = q_lat.shape
    width = q_rope.shape[1]
    rows = block // HALVES
    total = rest.shape[2]
    scale = (rank + width) ** -0.5
    caches = [jax.ShapeDtypeStruct((req_local, n * block, rank), jnp.bfloat16),
              jax.ShapeDtypeStruct((req_local, width, n * block), jnp.bfloat16),
              jax.ShapeDtypeStruct((req_local, heads, rank), jnp.bfloat16)]
    part = jax.ShapeDtypeStruct((heads, rank + 2 * LANES), jnp.float32)
    state = [pltpu.VMEM((heads, 1), jnp.float32), pltpu.VMEM((heads, 1), jnp.float32), pltpu.VMEM((heads, rank), jnp.float32)]

    def scratch(depth, pieces):
        return [pltpu.VMEM((rows, rank), jnp.bfloat16), pltpu.VMEM((width, pieces * rows), jnp.bfloat16)], [
            pltpu.VMEM((depth, width, pieces * rows), jnp.bfloat16), pltpu.SemaphoreType.DMA((depth, pieces)), pltpu.SemaphoreType.DMA((depth,))]

    params = pltpu.CompilerParams(vmem_limit_bytes=ATTEND_BYTES)
    flops = req_local * n * block * heads * (2 * rank + width) * 2
    zeros, stores = scratch(n, HALVES)
    *outs, first_part = pl.pallas_call(
        functools.partial(first_kernel, n, req_local, scale),
        in_specs=[SMEM, HBM, VMEM, VMEM],
        out_specs=[HBM, HBM, VMEM, HBM],
        out_shape=caches + [part],
        scratch_shapes=state + [pltpu.VMEM(part.shape, part.dtype), pltpu.SemaphoreType.DMA] + zeros + [
            pltpu.VMEM((n, HALVES, total, rank), jnp.bfloat16), pltpu.SemaphoreType.DMA((n,))] + stores,
        compiler_params=params,
        cost_estimate=pl.CostEstimate(flops=flops, bytes_accessed=req_local * n * block * rank * 4, transcendentals=0),
        name="attend_first",
    )(lens, landed, q_lat, q_rope)
    zeros, stores = scratch(n, 1)
    return pl.pallas_call(
        functools.partial(last_kernel, n, req_local, scale),
        in_specs=[SMEM] + [HBM] * 7,
        out_specs=[HBM] * 3,
        out_shape=caches,
        scratch_shapes=state + [pltpu.VMEM((heads, rank), jnp.bfloat16), pltpu.VMEM((width, heads), jnp.bfloat16), pltpu.VMEM(part.shape, part.dtype),
                                pltpu.VMEM((heads, rank), jnp.bfloat16), pltpu.SemaphoreType.DMA((4,))] + zeros + [
            pltpu.VMEM((n, 1, total, rank), jnp.bfloat16), pltpu.SemaphoreType.DMA((n,))] + stores,
        input_output_aliases={5: 0, 6: 1, 7: 2},
        compiler_params=params,
        cost_estimate=pl.CostEstimate(flops=flops // req_local // HALVES, bytes_accessed=n * block * rank * 2, transcendentals=0),
        name="attend_last",
    )(lens, rest, q_lat, q_rope, first_part, *outs)


def solution(mesh):
    seq_spec = P("dp", "x", None)
    req_spec = P(("dp", "x"), None, None)
    n = mesh.shape["x"]

    def local_step(c_raw, k_raw, norm_gain, rope_cos, rope_sin, seq_lens, q_lat, q_rope):
        landed, rest = send(seq_lens, c_raw, jnp.swapaxes(k_raw, 1, 2), norm_gain, rope_cos.T, rope_sin.T, n, q_lat.shape[0])
        rest = lax.all_to_all(rest, "x", 0, 0, tiled=True)[:, None]
        c_cache, kr_cache, o_lat = attend(seq_lens, landed, rest, q_lat, jnp.swapaxes(q_rope, 1, 2), n, c_raw.shape[1])
        return c_cache, jnp.swapaxes(kr_cache, 1, 2), o_lat

    return jax.shard_map(local_step, mesh=mesh, in_specs=(seq_spec, seq_spec, P(None), P("x", None), P("x", None), P("dp"), req_spec, req_spec), out_specs=(req_spec, req_spec, req_spec), check_vma=False)
```

```python
import functools

import jax
import jax.numpy as jnp
from jax import lax
from jax.experimental import pallas as pl
from jax.experimental.pallas import tpu as pltpu
from jax.sharding import PartitionSpec as P

NORM_EPS = 1e-6
PIECES = 3
ROUNDS = 6
LOADS = 4
RING = 12
AHEAD = 3
STRIPE = 128
LANES, SUBLANES = 128, 16
VMEM_BYTES = 60 * 1024 * 1024
ATTEND_BYTES = 52 * 1024 * 1024
MESH = pl.DeviceIdType.MESH
HBM = pl.BlockSpec(memory_space=pltpu.HBM)
VMEM = pl.BlockSpec(memory_space=pltpu.VMEM)
SMEM = pl.BlockSpec(memory_space=pltpu.SMEM)


def peer(j, n):
    me = lax.axis_index("x")
    chip, core = me // 2, me % 2
    far = j % 3
    last = j // (n - 2)
    hop = (1 - last) * (1 + 2 * far - 3 * (far // 2))
    other = (j // 3) % 2 * (1 - last) + last * (1 - j % (n - 2))
    return (chip + hop) % (n // 2) * 2 + (core + other) % 2


def rope_tiles(width, rows):
    for r in range(width // SUBLANES):
        for c in range(rows // LANES):
            yield (slice(r * SUBLANES, (r + 1) * SUBLANES), slice(c * LANES, (c + 1) * LANES),
                   slice(rows + c * SUBLANES, rows + (c + 1) * SUBLANES), slice(r * LANES, (r + 1) * LANES))


def clear(state):
    m_ref, l_ref, acc_ref = state
    m_ref[...] = jnp.full_like(m_ref, -1e30)
    l_ref[...] = jnp.zeros_like(l_ref)
    acc_ref[...] = jnp.zeros_like(acc_ref)


def fold(state, qa, qr, pieces, first, length, scale):
    m_ref, l_ref, acc_ref = state
    scores = []
    for h, (lat, kr) in enumerate(pieces):
        s = lax.dot_general(qa, lat, (((1,), (1,)), ((), ())), preferred_element_type=jnp.float32)
        s = s + lax.dot_general(qr, kr, (((0,), (0,)), ((), ())), preferred_element_type=jnp.float32)
        rows = lat.shape[0]
        pos = first + h * rows + lax.broadcasted_iota(jnp.int32, (1, rows), 1)
        scores.append(jnp.where(pos < length, s * scale, -1e30))
    m_old = m_ref[...]
    m_new = m_old
    for s in scores:
        m_new = jnp.maximum(m_new, jnp.max(s, axis=-1, keepdims=True))
    alpha = jnp.exp(m_old - m_new)
    total, acc = l_ref[...] * alpha, acc_ref[...] * alpha
    for s, (lat, _) in zip(scores, pieces):
        p = jnp.exp(s - m_new)
        total = total + jnp.sum(p, axis=-1, keepdims=True)
        acc = acc + jnp.dot(p.astype(jnp.bfloat16), lat, preferred_element_type=jnp.float32)
    m_ref[...], l_ref[...], acc_ref[...] = m_new, total, acc


def send_kernel(n, req_local, scale, lens_ref, c_hbm, k_hbm, gain_ref, cos_ref, sin_ref, qa_ref, qr_ref, land_ref, rest_ref, o_out,
                c_buf, k_buf, out_buf, c_sem, k_sem, send_sem, recv_sem, m_ref, l_ref, acc_ref, fold_buf, kr_buf, fold_sem):
    me = lax.axis_index("x")
    rounds = req_local * PIECES
    steps = rounds * n
    early = (rounds - 1) * n
    depth = out_buf.shape[0]
    rows, rank = c_buf.shape[1:]
    width = k_buf.shape[1]

    def load(t):
        req = peer(t % n, n) * req_local + t // n // PIECES
        first = pl.multiple_of(t // n % PIECES * rows, rows)
        slot = t % LOADS
        return (pltpu.make_async_copy(c_hbm.at[req, pl.ds(first, rows), :], c_buf.at[slot], c_sem.at[slot]),
                pltpu.make_async_copy(k_hbm.at[req, :, pl.ds(first, rows)], k_buf.at[slot], k_sem.at[slot]))

    def landing(t):
        return land_ref.at[t // n // PIECES, me, t // n % PIECES]

    def remote(t):
        slot = t % depth
        return pltpu.make_async_remote_copy(
            src_ref=out_buf.at[slot], dst_ref=landing(t), send_sem=send_sem.at[slot],
            recv_sem=recv_sem.at[t // n * n + me], device_id={"x": peer(t % n, n)}, device_id_type=MESH)

    def own(t):
        return pltpu.make_async_copy(out_buf.at[t % depth], landing(t), send_sem.at[t % depth])

    def keep(t):
        return pltpu.make_async_copy(out_buf.at[t % depth], rest_ref.at[peer(t % n, n)], send_sem.at[t % depth])

    def on_kind(t, act_remote, act_local):
        is_own = t % n == n - 1

        @pl.when(t >= early)
        def _():
            act_local(keep(t))

        @pl.when(jnp.logical_and(t < early, is_own))
        def _():
            act_local(own(t))

        @pl.when(jnp.logical_and(t < early, jnp.logical_not(is_own)))
        def _():
            act_remote(remote(t))

    def start(t):
        on_kind(t, lambda c: c.start(), lambda c: c.start())

    def sent(t):
        on_kind(t, lambda c: c.wait_send(), lambda c: c.wait())

    def pack(t):
        for c in load(t):
            c.wait()
        slot, out = t % LOADS, t % depth
        first = t // n % PIECES * rows
        left = lens_ref[peer(t % n, n) * req_local + t // n // PIECES] - me * (rows * PIECES) - first
        gain = gain_ref[...].astype(jnp.float32)

        @pl.loop(0, rows, step=STRIPE)
        def _(r):
            r = pl.multiple_of(r, STRIPE)
            lat = c_buf[slot, pl.ds(r, STRIPE), :].astype(jnp.float32)
            inv = lax.rsqrt(jnp.mean(lat * lat, axis=-1, keepdims=True) + NORM_EPS)
            valid = r + lax.broadcasted_iota(jnp.int32, (STRIPE, 1), 0) < left
            out_buf[out, pl.ds(r, STRIPE), :] = jnp.where(valid, lat * inv * gain, 0.0).astype(jnp.bfloat16)

        key = k_buf[slot].astype(jnp.float32)
        half = width // 2
        lo, hi = key[:half], key[half:]
        first = pl.multiple_of(first, LANES)
        cos, sin = cos_ref[:, pl.ds(first, rows)], sin_ref[:, pl.ds(first, rows)]
        valid = lax.broadcasted_iota(jnp.int32, (1, rows), 1) < left
        rotated = (jnp.where(valid, lo * cos - hi * sin, 0.0).astype(jnp.bfloat16),
                   jnp.where(valid, hi * cos + lo * sin, 0.0).astype(jnp.bfloat16))
        for kr_rows, kr_cols, to_rows, to_cols in rope_tiles(width, rows):
            part, at = kr_rows.start // half, kr_rows.start % half
            out_buf[out, to_rows, to_cols] = rotated[part][at : at + SUBLANES, kr_cols]

    barrier = pltpu.get_barrier_semaphore()
    for j in range(n - 1):
        pl.semaphore_signal(barrier, inc=1, device_id={"x": peer(j, n)}, device_id_type=MESH)
    for t in range(LOADS):
        for c in load(t):
            c.start()
    pack(0)
    for c in load(LOADS):
        c.start()
    pl.semaphore_wait(barrier, n - 1)

    state = (m_ref, l_ref, acc_ref)
    per_req = PIECES * n
    folds = (req_local - 1) * per_req
    lag = depth + n

    def received(a):
        src = peer(a % n, n)
        piece = land_ref.at[a // per_req, src, a // n % PIECES]
        pltpu.make_async_remote_copy(
            src_ref=piece, dst_ref=piece, send_sem=send_sem.at[0], recv_sem=recv_sem.at[a // n * n + src],
            device_id={"x": src}, device_id_type=MESH).wait_recv()

    def fetch(a):
        return pltpu.make_async_copy(land_ref.at[a // per_req, peer(a % n, n), a // n % PIECES], fold_buf.at[a % (AHEAD + 1)], fold_sem.at[a % (AHEAD + 1)])

    @pl.loop(1, folds + lag)
    def _(t):
        @pl.when(t >= depth)
        def _():
            sent(t - depth)

        @pl.when(t < steps)
        def _():
            pack(t)

            @pl.when(t + LOADS < steps)
            def _():
                for c in load(t + LOADS):
                    c.start()

        @pl.when(t <= steps)
        def _():
            start(t - 1)

        arriving = t - lag + AHEAD

        @pl.when(jnp.logical_and(arriving >= 0, arriving < folds))
        def _():
            @pl.when(arriving % n < n - 1)
            def _():
                received(arriving)

            fetch(arriving).start()

        a = t - lag

        @pl.when(a >= 0)
        def _():
            m, src, slot = a // per_req, peer(a % n, n), a % (AHEAD + 1)

            @pl.when(a % per_req == 0)
            def _():
                clear(state)

            fetch(a).wait()
            for kr_rows, kr_cols, from_rows, from_cols in rope_tiles(width, rows):
                kr_buf[kr_rows, kr_cols] = fold_buf[slot, from_rows, from_cols]
            first = (src * PIECES + a // n % PIECES) * rows
            fold(state, qa_ref[m], qr_ref[m], [(fold_buf[slot, :rows, :], kr_buf[...])], first, lens_ref[me * req_local + m], scale)

            @pl.when(a % per_req == per_req - 1)
            def _():
                o_out[m] = (acc_ref[...] / l_ref[...]).astype(jnp.bfloat16)

    @pl.loop(folds + lag - depth, steps)
    def _(t):
        sent(t)

    @pl.loop(folds, early)
    def _(a):
        @pl.when(a % n < n - 1)
        def _():
            received(a)


def send(lens, c_raw, k_raw, gain, cos, sin, q_lat, q_rope, n):
    req_local, heads, _ = q_lat.shape
    requests, block, rank = c_raw.shape
    width = k_raw.shape[1]
    rows = block // PIECES
    total = rows + rows * width // rank
    depth = ROUNDS * n
    return pl.pallas_call(
        functools.partial(send_kernel, n, req_local, (rank + width) ** -0.5),
        in_specs=[SMEM, HBM, HBM] + [VMEM] * 5,
        out_specs=[HBM, HBM, VMEM],
        out_shape=[jax.ShapeDtypeStruct((req_local, n, PIECES, total, rank), jnp.bfloat16),
                   jax.ShapeDtypeStruct((n, total, rank), jnp.bfloat16),
                   jax.ShapeDtypeStruct((req_local - 1, heads, rank), jnp.bfloat16)],
        scratch_shapes=[
            pltpu.VMEM((LOADS, rows, rank), jnp.bfloat16),
            pltpu.VMEM((LOADS, width, rows), jnp.bfloat16),
            pltpu.VMEM((depth, total, rank), jnp.bfloat16),
            pltpu.SemaphoreType.DMA((LOADS,)),
            pltpu.SemaphoreType.DMA((LOADS,)),
            pltpu.SemaphoreType.DMA((depth,)),
            pltpu.SemaphoreType.DMA(((req_local * PIECES - 1) * n,)),
            pltpu.VMEM((heads, 1), jnp.float32),
            pltpu.VMEM((heads, 1), jnp.float32),
            pltpu.VMEM((heads, rank), jnp.float32),
            pltpu.VMEM((AHEAD + 1, total, rank), jnp.bfloat16),
            pltpu.VMEM((width, rows), jnp.bfloat16),
            pltpu.SemaphoreType.DMA((AHEAD + 1,)),
        ],
        compiler_params=pltpu.CompilerParams(vmem_limit_bytes=VMEM_BYTES, collective_id=0, has_side_effects=True),
        cost_estimate=pl.CostEstimate(flops=requests * block * rank * 100, bytes_accessed=requests * block * rank * 4, transcendentals=0),
        name="send",
    )(lens, c_raw, k_raw, gain, cos, sin, q_lat, q_rope)


def stream(n, req_local, scale, group, length, land, queries, c_out, kr_out, state, buf, kr_buf, zero_c, zero_k, in_sem, c_sem, k_sem, ahead):
    first_req, count, first_piece, pieces = group
    depth = buf.shape[0]
    rank = buf.shape[3]
    width = kr_buf.shape[1]
    rows = buf.shape[2] * rank // (rank + width)
    span = rows * PIECES
    steps = count * n

    def used(t):
        return t % n * span + first_piece * rows < length(first_req + t // n)

    def load(t):
        return pltpu.make_async_copy(land(t // n, t % n), buf.at[t % depth, pl.ds(0, pieces)], in_sem.at[t % depth])

    def stores(t):
        slot, req = t % depth, first_req + t // n
        at = pl.multiple_of(t % n * span + first_piece * rows, rows)
        kr = pltpu.make_async_copy(kr_buf.at[slot, :, pl.ds(0, pieces * rows)], kr_out.at[req, :, pl.ds(at, pieces * rows)], k_sem.at[slot])
        cs = [pltpu.make_async_copy(buf.at[slot, h, pl.ds(0, rows), :], c_out.at[req, pl.ds(at + h * rows, rows), :], c_sem.at[slot, h]) for h in range(pieces)]
        return cs + [kr]

    def blanks(t):
        slot, req = t % depth, first_req + t // n
        at = pl.multiple_of(t % n * span + first_piece * rows, rows)
        kr = pltpu.make_async_copy(zero_k.at[:, pl.ds(0, pieces * rows)], kr_out.at[req, :, pl.ds(at, pieces * rows)], k_sem.at[slot])
        cs = [pltpu.make_async_copy(zero_c, c_out.at[req, pl.ds(at + h * rows, rows), :], c_sem.at[slot, h]) for h in range(pieces)]
        return cs + [kr]

    def fetch(t):
        @pl.when(used(t))
        def _():
            load(t).start()

    def work(t):
        slot, req = t % depth, first_req + t // n
        load(t).wait()
        for h in range(pieces):
            for kr_rows, kr_cols, from_rows, from_cols in rope_tiles(width, rows):
                cols = slice(h * rows + kr_cols.start, h * rows + kr_cols.stop)
                kr_buf[slot, kr_rows, cols] = buf[slot, h, from_rows, from_cols]
        for c in stores(t):
            c.start()
        if queries is not None:
            qa, qr = queries(t)
            blocks = [(buf[slot, h, :rows, :], kr_buf[slot, :, h * rows : (h + 1) * rows]) for h in range(pieces)]
            fold(state, qa, qr, blocks, t % n * span + first_piece * rows, length(req), scale)

    def body(t, begin, finish):
        @pl.when(t % n == 0)
        def _():
            begin()

        @pl.when(used(t))
        def _():
            work(t)

        @pl.when(jnp.logical_not(used(t)))
        def _():
            for c in blanks(t):
                c.start()

        @pl.when(t + ahead < steps)
        def _():
            @pl.when(t + ahead >= depth)
            def _():
                for c in stores(t + ahead - depth):
                    c.wait()

            fetch(t + ahead)

        @pl.when(t % n == n - 1)
        def _():
            finish(first_req + t // n)

    def run(begin, finish):
        for t in range(min(ahead, steps)):
            fetch(t)

        @pl.loop(0, steps)
        def _(t):
            body(t, begin, finish)

        @pl.loop(max(steps - depth, 0), steps)
        def _(t):
            for c in stores(t):
                c.wait()

    return run


def first_kernel(n, req_local, scale, lens_ref, land_ref, qa_ref, qr_ref, o_done, c_out, kr_out, o_out, part_out, o_sem,
                 m_ref, l_ref, acc_ref, part_ref, part_sem, zero_c, zero_k, buf, in_sem, kr_buf, c_sem, k_sem):
    length = lambda m: lens_ref[lax.axis_index("x") * req_local + m]
    zero_c[...] = jnp.zeros_like(zero_c)
    zero_k[...] = jnp.zeros_like(zero_k)
    state = (m_ref, l_ref, acc_ref)
    rest = (c_out, kr_out, state, buf, kr_buf, zero_c, zero_k, in_sem, c_sem, k_sem, buf.shape[0] // 2)
    last = req_local - 1
    rank = acc_ref.shape[1]

    done = pltpu.make_async_copy(o_done, o_out.at[pl.ds(0, last)], o_sem)
    done.start()

    def hand_over(m):
        part_ref[:, :rank] = acc_ref[...]
        part_ref[:, rank : rank + LANES] = jnp.broadcast_to(m_ref[...], (part_ref.shape[0], LANES))
        part_ref[:, rank + LANES :] = jnp.broadcast_to(l_ref[...], (part_ref.shape[0], LANES))
        copy = pltpu.make_async_copy(part_ref, part_out, part_sem)
        copy.start()
        copy.wait()

    piece = lambda m, i: land_ref.at[last, i, pl.ds(0, PIECES - 1)]
    stream(n, req_local, scale, (last, 1, 0, PIECES - 1), length, piece, lambda t: (qa_ref[last], qr_ref[last]), *rest)(lambda: clear(state), hand_over)
    whole = lambda m, i: land_ref.at[m, i]
    stream(n, req_local, scale, (0, last, 0, PIECES), length, whole, None, *rest)(lambda: None, lambda m: None)
    done.wait()


def last_kernel(n, req_local, scale, lens_ref, land_ref, qa_hbm, qr_hbm, part_hbm, c_old, kr_old, o_old, c_out, kr_out, o_out,
                m_ref, l_ref, acc_ref, qa_ref, qr_ref, part_ref, o_buf, sems, zero_c, zero_k, buf, in_sem, kr_buf, c_sem, k_sem):
    length = lambda m: lens_ref[lax.axis_index("x") * req_local + m]
    last = req_local - 1
    state = (m_ref, l_ref, acc_ref)
    rank = acc_ref.shape[1]
    copies = [pltpu.make_async_copy(qa_hbm.at[last], qa_ref, sems.at[0]), pltpu.make_async_copy(qr_hbm.at[last], qr_ref, sems.at[1]),
              pltpu.make_async_copy(part_hbm, part_ref, sems.at[2])]
    for c in copies:
        c.start()
    zero_c[...] = jnp.zeros_like(zero_c)
    zero_k[...] = jnp.zeros_like(zero_k)

    def begin():
        clear(state)
        for c in copies:
            c.wait()

    def finish(m):
        m_part, l_part, acc_part = part_ref[:, rank : rank + 1], part_ref[:, rank + LANES : rank + LANES + 1], part_ref[:, :rank]
        m_new = jnp.maximum(m_ref[...], m_part)
        here, there = jnp.exp(m_ref[...] - m_new), jnp.exp(m_part - m_new)
        total = l_ref[...] * here + l_part * there
        o_buf[...] = ((acc_ref[...] * here + acc_part * there) / total).astype(jnp.bfloat16)
        copy = pltpu.make_async_copy(o_buf, o_out.at[m], sems.at[3])
        copy.start()
        copy.wait()

    stream(n, req_local, scale, (last, 1, PIECES - 1, 1), length, lambda m, i: land_ref.at[pl.ds(i, 1)], lambda t: (qa_ref[...], qr_ref[...]), c_out, kr_out, state, buf, kr_buf,
           zero_c, zero_k, in_sem, c_sem, k_sem, buf.shape[0])(begin, finish)


def attend(lens, landed, rest, o_done, q_lat, q_rope, n, block):
    req_local, heads, rank = q_lat.shape
    width = q_rope.shape[1]
    rows = block // PIECES
    total = rest.shape[1]
    scale = (rank + width) ** -0.5
    caches = [jax.ShapeDtypeStruct((req_local, n * block, rank), jnp.bfloat16),
              jax.ShapeDtypeStruct((req_local, width, n * block), jnp.bfloat16),
              jax.ShapeDtypeStruct((req_local, heads, rank), jnp.bfloat16)]
    part = jax.ShapeDtypeStruct((heads, rank + 2 * LANES), jnp.float32)
    state = [pltpu.VMEM((heads, 1), jnp.float32), pltpu.VMEM((heads, 1), jnp.float32), pltpu.VMEM((heads, rank), jnp.float32)]

    def scratch(depth, pieces):
        return [pltpu.VMEM((rows, rank), jnp.bfloat16), pltpu.VMEM((width, pieces * rows), jnp.bfloat16)], [
            pltpu.VMEM((depth, width, pieces * rows), jnp.bfloat16), pltpu.SemaphoreType.DMA((depth, pieces)), pltpu.SemaphoreType.DMA((depth,))]

    params = pltpu.CompilerParams(vmem_limit_bytes=ATTEND_BYTES)
    flops = 2 * req_local * n * block * heads * rank
    zeros, stores = scratch(RING, PIECES)
    *outs, first_part = pl.pallas_call(
        functools.partial(first_kernel, n, req_local, scale),
        in_specs=[SMEM, HBM, VMEM, VMEM, HBM],
        out_specs=[HBM] * 4,
        out_shape=caches + [part],
        scratch_shapes=[pltpu.SemaphoreType.DMA] + state + [pltpu.VMEM(part.shape, part.dtype), pltpu.SemaphoreType.DMA] + zeros + [
            pltpu.VMEM((RING, PIECES, total, rank), jnp.bfloat16), pltpu.SemaphoreType.DMA((RING,))] + stores,
        compiler_params=params,
        cost_estimate=pl.CostEstimate(flops=flops, bytes_accessed=req_local * n * block * rank * 4, transcendentals=0),
        name="attend_first",
    )(lens, landed, q_lat, q_rope, o_done)
    zeros, stores = scratch(n, 1)
    return pl.pallas_call(
        functools.partial(last_kernel, n, req_local, scale),
        in_specs=[SMEM] + [HBM] * 7,
        out_specs=[HBM] * 3,
        out_shape=caches,
        scratch_shapes=state + [pltpu.VMEM((heads, rank), jnp.bfloat16), pltpu.VMEM((width, heads), jnp.bfloat16), pltpu.VMEM(part.shape, part.dtype),
                                pltpu.VMEM((heads, rank), jnp.bfloat16), pltpu.SemaphoreType.DMA((4,))] + zeros + [
            pltpu.VMEM((n, 1, total, rank), jnp.bfloat16), pltpu.SemaphoreType.DMA((n,))] + stores,
        input_output_aliases={5: 0, 6: 1, 7: 2},
        compiler_params=params,
        cost_estimate=pl.CostEstimate(flops=flops // req_local // PIECES, bytes_accessed=n * block * rank * 2, transcendentals=0),
        name="attend_last",
    )(lens, rest, q_lat, q_rope, first_part, *outs)


def solution(mesh):
    seq_spec = P("dp", "x", None)
    req_spec = P(("dp", "x"), None, None)
    n = mesh.shape["x"]

    def local_step(c_raw, k_raw, norm_gain, rope_cos, rope_sin, seq_lens, q_lat, q_rope):
        q_rope = jnp.swapaxes(q_rope, 1, 2)
        landed, rest, o_done = send(seq_lens, c_raw, jnp.swapaxes(k_raw, 1, 2), norm_gain, rope_cos.T, rope_sin.T, q_lat, q_rope, n)
        rest = lax.all_to_all(rest, "x", 0, 0, tiled=True)
        c_cache, kr_cache, o_lat = attend(seq_lens, landed, rest, o_done, q_lat, q_rope, n, c_raw.shape[1])
        return c_cache, jnp.swapaxes(kr_cache, 1, 2), o_lat

    return jax.shard_map(local_step, mesh=mesh, in_specs=(seq_spec, seq_spec, P(None), P("x", None), P("x", None), P("dp"), req_spec, req_spec), out_specs=(req_spec, req_spec, req_spec), check_vma=False)
```

```python
import functools

import jax
import jax.numpy as jnp
from jax import lax
from jax.experimental import pallas as pl
from jax.experimental.pallas import tpu as pltpu
from jax.sharding import PartitionSpec as P

NORM_EPS = 1e-6
PIECES = 3
ROUNDS = 6
LOADS = 4
RING = 12
BATCH = 4
AHEAD = 3
STRIPE = 128
LANES, SUBLANES = 128, 16
VMEM_BYTES = 60 * 1024 * 1024
ATTEND_BYTES = 52 * 1024 * 1024
MESH = pl.DeviceIdType.MESH
HBM = pl.BlockSpec(memory_space=pltpu.HBM)
VMEM = pl.BlockSpec(memory_space=pltpu.VMEM)
SMEM = pl.BlockSpec(memory_space=pltpu.SMEM)


def peer(j, n):
    me = lax.axis_index("x")
    chip, core = me // 2, me % 2
    far = j % 3
    last = j // (n - 2)
    hop = (1 - last) * (1 + 2 * far - 3 * (far // 2))
    other = (j // 3) % 2 * (1 - last) + last * (1 - j % (n - 2))
    return (chip + hop) % (n // 2) * 2 + (core + other) % 2


def rope_tiles(width, rows):
    for r in range(width // SUBLANES):
        for c in range(rows // LANES):
            yield (slice(r * SUBLANES, (r + 1) * SUBLANES), slice(c * LANES, (c + 1) * LANES),
                   slice(rows + c * SUBLANES, rows + (c + 1) * SUBLANES), slice(r * LANES, (r + 1) * LANES))


def clear(state):
    m_ref, l_ref, acc_ref = state
    m_ref[...] = jnp.full_like(m_ref, -1e30)
    l_ref[...] = jnp.zeros_like(l_ref)
    acc_ref[...] = jnp.zeros_like(acc_ref)


def fold(state, qa, qr, pieces, firsts, length, scale):
    m_ref, l_ref, acc_ref = state
    scores = []
    for first, (lat, kr) in zip(firsts, pieces):
        s = lax.dot_general(qa, lat, (((1,), (1,)), ((), ())), preferred_element_type=jnp.float32)
        s = s + lax.dot_general(qr, kr, (((0,), (0,)), ((), ())), preferred_element_type=jnp.float32)
        rows = lat.shape[0]
        pos = first + lax.broadcasted_iota(jnp.int32, (1, rows), 1)
        scores.append(jnp.where(pos < length, s * scale, -1e30))
    m_old = m_ref[...]
    m_new = m_old
    for s in scores:
        m_new = jnp.maximum(m_new, jnp.max(s, axis=-1, keepdims=True))
    alpha = jnp.exp(m_old - m_new)
    total, acc = l_ref[...] * alpha, acc_ref[...] * alpha
    for s, (lat, _) in zip(scores, pieces):
        p = jnp.exp(s - m_new)
        total = total + jnp.sum(p, axis=-1, keepdims=True)
        acc = acc + jnp.dot(p.astype(jnp.bfloat16), lat, preferred_element_type=jnp.float32)
    m_ref[...], l_ref[...], acc_ref[...] = m_new, total, acc


def send_kernel(n, req_local, scale, lens_ref, c_hbm, k_hbm, gain_ref, cos_ref, sin_ref, qa_ref, qr_ref, land_ref, rest_ref, o_out,
                c_buf, k_buf, out_buf, c_sem, k_sem, send_sem, recv_sem, m_ref, l_ref, acc_ref, fold_buf, kr_buf, fold_sem):
    me = lax.axis_index("x")
    rounds = req_local * PIECES
    steps = rounds * n
    early = (rounds - 1) * n
    depth = out_buf.shape[0]
    rows, rank = c_buf.shape[1:]
    width = k_buf.shape[1]

    def load(t):
        req = peer(t % n, n) * req_local + t // n // PIECES
        first = pl.multiple_of(t // n % PIECES * rows, rows)
        slot = t % LOADS
        return (pltpu.make_async_copy(c_hbm.at[req, pl.ds(first, rows), :], c_buf.at[slot], c_sem.at[slot]),
                pltpu.make_async_copy(k_hbm.at[req, :, pl.ds(first, rows)], k_buf.at[slot], k_sem.at[slot]))

    def landing(t):
        return land_ref.at[t // n // PIECES, me, t // n % PIECES]

    def remote(t):
        slot = t % depth
        return pltpu.make_async_remote_copy(
            src_ref=out_buf.at[slot], dst_ref=landing(t), send_sem=send_sem.at[slot],
            recv_sem=recv_sem.at[t // n * n + me], device_id={"x": peer(t % n, n)}, device_id_type=MESH)

    def own(t):
        return pltpu.make_async_copy(out_buf.at[t % depth], landing(t), send_sem.at[t % depth])

    def keep(t):
        return pltpu.make_async_copy(out_buf.at[t % depth], rest_ref.at[peer(t % n, n)], send_sem.at[t % depth])

    def on_kind(t, act_remote, act_local):
        is_own = t % n == n - 1

        @pl.when(t >= early)
        def _():
            act_local(keep(t))

        @pl.when(jnp.logical_and(t < early, is_own))
        def _():
            act_local(own(t))

        @pl.when(jnp.logical_and(t < early, jnp.logical_not(is_own)))
        def _():
            act_remote(remote(t))

    def start(t):
        on_kind(t, lambda c: c.start(), lambda c: c.start())

    def sent(t):
        on_kind(t, lambda c: c.wait_send(), lambda c: c.wait())

    def pack(t):
        for c in load(t):
            c.wait()
        slot, out = t % LOADS, t % depth
        first = t // n % PIECES * rows
        left = lens_ref[peer(t % n, n) * req_local + t // n // PIECES] - me * (rows * PIECES) - first
        gain = gain_ref[...].astype(jnp.float32)

        @pl.loop(0, rows, step=STRIPE)
        def _(r):
            r = pl.multiple_of(r, STRIPE)
            lat = c_buf[slot, pl.ds(r, STRIPE), :].astype(jnp.float32)
            inv = lax.rsqrt(jnp.mean(lat * lat, axis=-1, keepdims=True) + NORM_EPS)
            valid = r + lax.broadcasted_iota(jnp.int32, (STRIPE, 1), 0) < left
            out_buf[out, pl.ds(r, STRIPE), :] = jnp.where(valid, lat * inv * gain, 0.0).astype(jnp.bfloat16)

        key = k_buf[slot].astype(jnp.float32)
        half = width // 2
        lo, hi = key[:half], key[half:]
        first = pl.multiple_of(first, LANES)
        cos, sin = cos_ref[:, pl.ds(first, rows)], sin_ref[:, pl.ds(first, rows)]
        valid = lax.broadcasted_iota(jnp.int32, (1, rows), 1) < left
        rotated = (jnp.where(valid, lo * cos - hi * sin, 0.0).astype(jnp.bfloat16),
                   jnp.where(valid, hi * cos + lo * sin, 0.0).astype(jnp.bfloat16))
        for kr_rows, kr_cols, to_rows, to_cols in rope_tiles(width, rows):
            part, at = kr_rows.start // half, kr_rows.start % half
            out_buf[out, to_rows, to_cols] = rotated[part][at : at + SUBLANES, kr_cols]

    barrier = pltpu.get_barrier_semaphore()
    for j in range(n - 1):
        pl.semaphore_signal(barrier, inc=1, device_id={"x": peer(j, n)}, device_id_type=MESH)
    for t in range(LOADS):
        for c in load(t):
            c.start()
    pack(0)
    for c in load(LOADS):
        c.start()
    pl.semaphore_wait(barrier, n - 1)

    state = (m_ref, l_ref, acc_ref)
    per_req = PIECES * n
    folds = (req_local - 1) * per_req
    lag = depth + n

    def received(a):
        src = peer(a % n, n)
        piece = land_ref.at[a // per_req, src, a // n % PIECES]
        pltpu.make_async_remote_copy(
            src_ref=piece, dst_ref=piece, send_sem=send_sem.at[0], recv_sem=recv_sem.at[a // n * n + src],
            device_id={"x": src}, device_id_type=MESH).wait_recv()

    def fetch(a):
        return pltpu.make_async_copy(land_ref.at[a // per_req, peer(a % n, n), a // n % PIECES], fold_buf.at[a % (AHEAD + 1)], fold_sem.at[a % (AHEAD + 1)])

    @pl.loop(1, folds + lag)
    def _(t):
        @pl.when(t >= depth)
        def _():
            sent(t - depth)

        @pl.when(t < steps)
        def _():
            pack(t)

            @pl.when(t + LOADS < steps)
            def _():
                for c in load(t + LOADS):
                    c.start()

        @pl.when(t <= steps)
        def _():
            start(t - 1)

        arriving = t - lag + AHEAD

        @pl.when(jnp.logical_and(arriving >= 0, arriving < folds))
        def _():
            @pl.when(arriving % n < n - 1)
            def _():
                received(arriving)

            fetch(arriving).start()

        a = t - lag

        @pl.when(a >= 0)
        def _():
            m, src, slot = a // per_req, peer(a % n, n), a % (AHEAD + 1)

            @pl.when(a % per_req == 0)
            def _():
                clear(state)

            fetch(a).wait()
            for kr_rows, kr_cols, from_rows, from_cols in rope_tiles(width, rows):
                kr_buf[kr_rows, kr_cols] = fold_buf[slot, from_rows, from_cols]
            first = (src * PIECES + a // n % PIECES) * rows
            fold(state, qa_ref[m], qr_ref[m], [(fold_buf[slot, :rows, :], kr_buf[...])], [first], lens_ref[me * req_local + m], scale)

            @pl.when(a % per_req == per_req - 1)
            def _():
                o_out[m] = (acc_ref[...] / l_ref[...]).astype(jnp.bfloat16)

    @pl.loop(folds + lag - depth, steps)
    def _(t):
        sent(t)

    @pl.loop(folds, early)
    def _(a):
        @pl.when(a % n < n - 1)
        def _():
            received(a)


def send(lens, c_raw, k_raw, gain, cos, sin, q_lat, q_rope, n):
    req_local, heads, _ = q_lat.shape
    requests, block, rank = c_raw.shape
    width = k_raw.shape[1]
    rows = block // PIECES
    total = rows + rows * width // rank
    depth = ROUNDS * n
    return pl.pallas_call(
        functools.partial(send_kernel, n, req_local, (rank + width) ** -0.5),
        in_specs=[SMEM, HBM, HBM] + [VMEM] * 5,
        out_specs=[HBM, HBM, VMEM],
        out_shape=[jax.ShapeDtypeStruct((req_local, n, PIECES, total, rank), jnp.bfloat16),
                   jax.ShapeDtypeStruct((n, total, rank), jnp.bfloat16),
                   jax.ShapeDtypeStruct((req_local - 1, heads, rank), jnp.bfloat16)],
        scratch_shapes=[
            pltpu.VMEM((LOADS, rows, rank), jnp.bfloat16),
            pltpu.VMEM((LOADS, width, rows), jnp.bfloat16),
            pltpu.VMEM((depth, total, rank), jnp.bfloat16),
            pltpu.SemaphoreType.DMA((LOADS,)),
            pltpu.SemaphoreType.DMA((LOADS,)),
            pltpu.SemaphoreType.DMA((depth,)),
            pltpu.SemaphoreType.DMA(((req_local * PIECES - 1) * n,)),
            pltpu.VMEM((heads, 1), jnp.float32),
            pltpu.VMEM((heads, 1), jnp.float32),
            pltpu.VMEM((heads, rank), jnp.float32),
            pltpu.VMEM((AHEAD + 1, total, rank), jnp.bfloat16),
            pltpu.VMEM((width, rows), jnp.bfloat16),
            pltpu.SemaphoreType.DMA((AHEAD + 1,)),
        ],
        compiler_params=pltpu.CompilerParams(vmem_limit_bytes=VMEM_BYTES, collective_id=0, has_side_effects=True),
        cost_estimate=pl.CostEstimate(flops=requests * block * rank * 100, bytes_accessed=requests * block * rank * 4, transcendentals=0),
        name="send",
    )(lens, c_raw, k_raw, gain, cos, sin, q_lat, q_rope)


def stream(n, req_local, scale, group, length, land, queries, c_out, kr_out, state, buf, kr_buf, zero_c, zero_k, in_sem, c_sem, k_sem, ahead):
    first_req, count, first_piece, pieces = group
    depth = buf.shape[0]
    rank = buf.shape[3]
    width = kr_buf.shape[1]
    rows = buf.shape[2] * rank // (rank + width)
    span = rows * PIECES
    steps = count * n

    def used(t):
        return t % n * span + first_piece * rows < length(first_req + t // n)

    def load(t):
        return pltpu.make_async_copy(land(t // n, t % n), buf.at[t % depth, pl.ds(0, pieces)], in_sem.at[t % depth])

    def stores(t):
        slot, req = t % depth, first_req + t // n
        at = pl.multiple_of(t % n * span + first_piece * rows, rows)
        kr = pltpu.make_async_copy(kr_buf.at[slot, :, pl.ds(0, pieces * rows)], kr_out.at[req, :, pl.ds(at, pieces * rows)], k_sem.at[slot])
        cs = [pltpu.make_async_copy(buf.at[slot, h, pl.ds(0, rows), :], c_out.at[req, pl.ds(at + h * rows, rows), :], c_sem.at[slot, h]) for h in range(pieces)]
        return cs + [kr]

    def blanks(t):
        slot, req = t % depth, first_req + t // n
        at = pl.multiple_of(t % n * span + first_piece * rows, rows)
        kr = pltpu.make_async_copy(zero_k.at[:, pl.ds(0, pieces * rows)], kr_out.at[req, :, pl.ds(at, pieces * rows)], k_sem.at[slot])
        cs = [pltpu.make_async_copy(zero_c, c_out.at[req, pl.ds(at + h * rows, rows), :], c_sem.at[slot, h]) for h in range(pieces)]
        return cs + [kr]

    def fetch(t):
        @pl.when(used(t))
        def _():
            load(t).start()

    def work(t):
        slot, req = t % depth, first_req + t // n
        load(t).wait()
        for h in range(pieces):
            for kr_rows, kr_cols, from_rows, from_cols in rope_tiles(width, rows):
                cols = slice(h * rows + kr_cols.start, h * rows + kr_cols.stop)
                kr_buf[slot, kr_rows, cols] = buf[slot, h, from_rows, from_cols]
        for c in stores(t):
            c.start()
        if queries is not None:
            qa, qr = queries(t)
            blocks = [(buf[slot, h, :rows, :], kr_buf[slot, :, h * rows : (h + 1) * rows]) for h in range(pieces)]
            firsts = [t % n * span + (first_piece + h) * rows for h in range(pieces)]
            fold(state, qa, qr, blocks, firsts, length(req), scale)

    def body(t):
        @pl.when(used(t))
        def _():
            work(t)

        @pl.when(jnp.logical_not(used(t)))
        def _():
            for c in blanks(t):
                c.start()

        @pl.when(t + ahead < steps)
        def _():
            @pl.when(t + ahead >= depth)
            def _():
                for c in stores(t + ahead - depth):
                    c.wait()

            fetch(t + ahead)

    def prologue():
        for t in range(min(ahead, steps)):
            fetch(t)

    def drain():
        @pl.loop(max(steps - depth, 0), steps)
        def _(t):
            for c in stores(t):
                c.wait()

    return steps, prologue, body, drain


def first_kernel(n, req_local, scale, lens_ref, land_ref, qa_ref, qr_ref, o_done, c_out, kr_out, o_out, part_out, o_sem,
                 m_ref, l_ref, acc_ref, part_ref, part_sem, zero_c, zero_k, buf, in_sem, kr_buf, c_sem, k_sem,
                 side_buf, side_in_sem, side_kr_buf, side_c_sem, side_k_sem):
    length = lambda m: lens_ref[lax.axis_index("x") * req_local + m]
    state = (m_ref, l_ref, acc_ref)
    last = req_local - 1
    rank = acc_ref.shape[1]
    done = pltpu.make_async_copy(o_done, o_out.at[pl.ds(0, last)], o_sem)
    piece = lambda m, i: land_ref.at[last, i, pl.ds(0, PIECES - 1)]
    whole = lambda m, i: land_ref.at[m, i]
    side_steps, side_prologue, side_body, side_drain = stream(
        n, req_local, scale, (last, 1, 0, PIECES - 1), length, piece, lambda t: (qa_ref[last], qr_ref[last]), c_out, kr_out, state,
        side_buf, side_kr_buf, zero_c, zero_k, side_in_sem, side_c_sem, side_k_sem, n)
    steps, prologue, body, drain = stream(
        n, req_local, scale, (0, last, 0, PIECES), length, whole, None, c_out, kr_out, state,
        buf, kr_buf, zero_c, zero_k, in_sem, c_sem, k_sem, buf.shape[0] // 2)

    side_prologue()
    prologue()
    done.start()
    zero_c[...] = jnp.zeros_like(zero_c)
    zero_k[...] = jnp.zeros_like(zero_k)
    clear(state)
    every = steps // side_steps

    @pl.loop(0, steps)
    def _(t):
        body(t)

        @pl.when(t % every == 0)
        def _():
            side_body(t // every)

    part_ref[:, :rank] = acc_ref[...]
    part_ref[:, rank : rank + LANES] = jnp.broadcast_to(m_ref[...], (part_ref.shape[0], LANES))
    part_ref[:, rank + LANES :] = jnp.broadcast_to(l_ref[...], (part_ref.shape[0], LANES))
    copy = pltpu.make_async_copy(part_ref, part_out, part_sem)
    copy.start()
    copy.wait()
    drain()
    side_drain()
    done.wait()


def last_kernel(n, req_local, scale, lens_ref, land_ref, qa_hbm, qr_hbm, part_hbm, c_old, kr_old, o_old, c_out, kr_out, o_out,
                m_ref, l_ref, acc_ref, qa_ref, qr_ref, part_ref, o_buf, sems, buf, in_sem, kr_buf, c_sem, k_sem):
    last = req_local - 1
    length = lens_ref[lax.axis_index("x") * req_local + last]
    state = (m_ref, l_ref, acc_ref)
    rank = acc_ref.shape[1]
    width = kr_buf.shape[1]
    rows = kr_buf.shape[2]
    block = rows * PIECES
    loads = [pltpu.make_async_copy(land_ref.at[i], buf.at[i], in_sem.at[i]) for i in range(n)]
    for c in loads:
        c.start()
    copies = [pltpu.make_async_copy(qa_hbm.at[last], qa_ref, sems.at[0]), pltpu.make_async_copy(qr_hbm.at[last], qr_ref, sems.at[1]),
              pltpu.make_async_copy(part_hbm, part_ref, sems.at[2])]
    for c in copies:
        c.start()
    clear(state)
    stores = []
    for at in range(0, n, BATCH):
        batch = range(at, at + BATCH)
        for i in batch:
            first = i * block + block - rows
            loads[i].wait()
            stores.append(pltpu.make_async_copy(buf.at[i, pl.ds(0, rows), :], c_out.at[last, pl.ds(first, rows), :], c_sem.at[i]))
            stores[-1].start()
            for kr_rows, kr_cols, from_rows, from_cols in rope_tiles(width, rows):
                kr_buf[i, kr_rows, kr_cols] = buf[i, from_rows, from_cols]
            stores.append(pltpu.make_async_copy(kr_buf.at[i], kr_out.at[last, :, pl.ds(first, rows)], k_sem.at[i]))
            stores[-1].start()
        if at == 0:
            for c in copies:
                c.wait()

        @pl.when(at * block + block - rows < length)
        def _():
            blocks = [(buf[i, :rows, :], kr_buf[i]) for i in batch]
            fold(state, qa_ref[...], qr_ref[...], blocks, [i * block + block - rows for i in batch], length, scale)

    m_part, l_part, acc_part = part_ref[:, rank : rank + 1], part_ref[:, rank + LANES : rank + LANES + 1], part_ref[:, :rank]
    m_new = jnp.maximum(m_ref[...], m_part)
    here, there = jnp.exp(m_ref[...] - m_new), jnp.exp(m_part - m_new)
    total = l_ref[...] * here + l_part * there
    o_buf[...] = ((acc_ref[...] * here + acc_part * there) / total).astype(jnp.bfloat16)
    copy = pltpu.make_async_copy(o_buf, o_out.at[last], sems.at[3])
    copy.start()
    for c in stores + [copy]:
        c.wait()


def attend(lens, landed, rest, o_done, q_lat, q_rope, n, block):
    req_local, heads, rank = q_lat.shape
    width = q_rope.shape[1]
    rows = block // PIECES
    total = rest.shape[1]
    scale = (rank + width) ** -0.5
    caches = [jax.ShapeDtypeStruct((req_local, n * block, rank), jnp.bfloat16),
              jax.ShapeDtypeStruct((req_local, width, n * block), jnp.bfloat16),
              jax.ShapeDtypeStruct((req_local, heads, rank), jnp.bfloat16)]
    part = jax.ShapeDtypeStruct((heads, rank + 2 * LANES), jnp.float32)
    state = [pltpu.VMEM((heads, 1), jnp.float32), pltpu.VMEM((heads, 1), jnp.float32), pltpu.VMEM((heads, rank), jnp.float32)]

    def ring(depth, *pieces):
        count = pieces[0] if pieces else 1
        return [pltpu.VMEM((depth, *pieces, total, rank), jnp.bfloat16), pltpu.SemaphoreType.DMA((depth,)),
                pltpu.VMEM((depth, width, count * rows), jnp.bfloat16), pltpu.SemaphoreType.DMA((depth, *pieces)), pltpu.SemaphoreType.DMA((depth,))]

    params = pltpu.CompilerParams(vmem_limit_bytes=ATTEND_BYTES)
    flops = 2 * req_local * n * block * heads * rank
    *outs, first_part = pl.pallas_call(
        functools.partial(first_kernel, n, req_local, scale),
        in_specs=[SMEM, HBM, VMEM, VMEM, HBM],
        out_specs=[HBM] * 4,
        out_shape=caches + [part],
        scratch_shapes=[pltpu.SemaphoreType.DMA] + state + [pltpu.VMEM(part.shape, part.dtype), pltpu.SemaphoreType.DMA,
                                                            pltpu.VMEM((rows, rank), jnp.bfloat16), pltpu.VMEM((width, block), jnp.bfloat16)]
        + ring(RING, PIECES) + ring(n, PIECES - 1),
        compiler_params=params,
        cost_estimate=pl.CostEstimate(flops=flops, bytes_accessed=req_local * n * block * rank * 4, transcendentals=0),
        name="attend_first",
    )(lens, landed, q_lat, q_rope, o_done)
    return pl.pallas_call(
        functools.partial(last_kernel, n, req_local, scale),
        in_specs=[SMEM] + [HBM] * 7,
        out_specs=[HBM] * 3,
        out_shape=caches,
        scratch_shapes=state + [pltpu.VMEM((heads, rank), jnp.bfloat16), pltpu.VMEM((width, heads), jnp.bfloat16), pltpu.VMEM(part.shape, part.dtype),
                                pltpu.VMEM((heads, rank), jnp.bfloat16), pltpu.SemaphoreType.DMA((4,))] + ring(n),
        input_output_aliases={5: 0, 6: 1, 7: 2},
        compiler_params=params,
        cost_estimate=pl.CostEstimate(flops=flops // req_local // PIECES, bytes_accessed=n * block * rank * 2, transcendentals=0),
        name="attend_last",
    )(lens, rest, q_lat, q_rope, first_part, *outs)


def solution(mesh):
    seq_spec = P("dp", "x", None)
    req_spec = P(("dp", "x"), None, None)
    n = mesh.shape["x"]

    def local_step(c_raw, k_raw, norm_gain, rope_cos, rope_sin, seq_lens, q_lat, q_rope):
        q_rope = jnp.swapaxes(q_rope, 1, 2)
        landed, rest, o_done = send(seq_lens, c_raw, jnp.swapaxes(k_raw, 1, 2), norm_gain, rope_cos.T, rope_sin.T, q_lat, q_rope, n)
        rest = lax.all_to_all(rest, "x", 0, 0, tiled=True)
        c_cache, kr_cache, o_lat = attend(seq_lens, landed, rest, o_done, q_lat, q_rope, n, c_raw.shape[1])
        return c_cache, jnp.swapaxes(kr_cache, 1, 2), o_lat

    return jax.shard_map(local_step, mesh=mesh, in_specs=(seq_spec, seq_spec, P(None), P("x", None), P("x", None), P("dp"), req_spec, req_spec), out_specs=(req_spec, req_spec, req_spec), check_vma=False)
```

```python
import functools

import jax
import jax.numpy as jnp
from jax import lax
from jax.experimental import pallas as pl
from jax.experimental.pallas import tpu as pltpu
from jax.sharding import PartitionSpec as P

NORM_EPS = 1e-6
PIECES = 3
ROUNDS = 6
LOADS = 4
RING = 12
BATCH = 4
AHEAD = 3
STRIPE = 128
LANES, SUBLANES = 128, 16
VMEM_BYTES = 60 * 1024 * 1024
ATTEND_BYTES = 44 * 1024 * 1024
MESH = pl.DeviceIdType.MESH
HBM = pl.BlockSpec(memory_space=pltpu.HBM)
VMEM = pl.BlockSpec(memory_space=pltpu.VMEM)
SMEM = pl.BlockSpec(memory_space=pltpu.SMEM)


def move(me, j, n, way):
    chip, core = me // 2, me % 2
    far = j % 3
    last = j // (n - 2)
    hop = (1 - last) * (1 + 2 * far - 3 * (far // 2))
    other = (j // 3) % 2 * (1 - last) + last * (1 - j % (n - 2))
    return (chip + n // 2 + way * hop) % (n // 2) * 2 + (core + other) % 2


def peer(j, n):
    return move(lax.axis_index("x"), j, n, 1)


def rope_tiles(width, rows):
    for r in range(width // SUBLANES):
        for c in range(rows // LANES):
            yield (slice(r * SUBLANES, (r + 1) * SUBLANES), slice(c * LANES, (c + 1) * LANES),
                   slice(rows + c * SUBLANES, rows + (c + 1) * SUBLANES), slice(r * LANES, (r + 1) * LANES))


def clear(state):
    m_ref, l_ref, acc_ref = state
    m_ref[...] = jnp.full_like(m_ref, -1e30)
    l_ref[...] = jnp.zeros_like(l_ref)
    acc_ref[...] = jnp.zeros_like(acc_ref)


def fold(state, qa, qr, pieces, firsts, length, scale):
    m_ref, l_ref, acc_ref = state
    scores = []
    for first, (lat, kr) in zip(firsts, pieces):
        s = lax.dot_general(qa, lat, (((1,), (1,)), ((), ())), preferred_element_type=jnp.float32)
        s = s + lax.dot_general(qr, kr, (((0,), (0,)), ((), ())), preferred_element_type=jnp.float32)
        rows = lat.shape[0]
        pos = first + lax.broadcasted_iota(jnp.int32, (1, rows), 1)
        scores.append(jnp.where(pos < length, s * scale, -1e30))
    m_old = m_ref[...]
    m_new = m_old
    for s in scores:
        m_new = jnp.maximum(m_new, jnp.max(s, axis=-1, keepdims=True))
    alpha = jnp.exp(m_old - m_new)
    total, acc = l_ref[...] * alpha, acc_ref[...] * alpha
    for s, (lat, _) in zip(scores, pieces):
        p = jnp.exp(s - m_new)
        total = total + jnp.sum(p, axis=-1, keepdims=True)
        acc = acc + jnp.dot(p.astype(jnp.bfloat16), lat, preferred_element_type=jnp.float32)
    m_ref[...], l_ref[...], acc_ref[...] = m_new, total, acc


def send_kernel(n, req_local, scale, lens_ref, c_hbm, k_hbm, gain_ref, cos_ref, sin_ref, qa_ref, qr_ref, land_ref, o_out, *scratch):
    rest_refs, scratch = scratch[:n], scratch[n:]
    c_buf, k_buf, out_buf, c_sem, k_sem, send_sem, recv_sem, m_ref, l_ref, acc_ref, fold_buf, kr_buf, fold_sem = scratch
    me = lax.axis_index("x")
    rounds = req_local * PIECES
    steps = rounds * n
    early = (rounds - 1) * n
    depth = out_buf.shape[0]
    rows, rank = c_buf.shape[1:]
    width = k_buf.shape[1]

    def load(t):
        req = peer(t % n, n) * req_local + t // n // PIECES
        first = pl.multiple_of(t // n % PIECES * rows, rows)
        slot = t % LOADS
        return (pltpu.make_async_copy(c_hbm.at[req, pl.ds(first, rows), :], c_buf.at[slot], c_sem.at[slot]),
                pltpu.make_async_copy(k_hbm.at[req, :, pl.ds(first, rows)], k_buf.at[slot], k_sem.at[slot]))

    def landing(t):
        return land_ref.at[t // n // PIECES, me, t // n % PIECES]

    def remote(t):
        slot = t % depth
        return pltpu.make_async_remote_copy(
            src_ref=out_buf.at[slot], dst_ref=landing(t), send_sem=send_sem.at[slot],
            recv_sem=recv_sem.at[t // n * n + me], device_id={"x": peer(t % n, n)}, device_id_type=MESH)

    def own(t):
        return pltpu.make_async_copy(out_buf.at[t % depth], landing(t), send_sem.at[t % depth])

    def keep(t, j):
        return pltpu.make_async_copy(out_buf.at[t % depth], rest_refs[j], send_sem.at[t % depth])

    def on_kind(t, act_remote, act_local):
        is_own = t % n == n - 1

        for j in range(n):
            @pl.when(t == early + j)
            def _():
                act_local(keep(t, j))

        @pl.when(jnp.logical_and(t < early, is_own))
        def _():
            act_local(own(t))

        @pl.when(jnp.logical_and(t < early, jnp.logical_not(is_own)))
        def _():
            act_remote(remote(t))

    def start(t):
        on_kind(t, lambda c: c.start(), lambda c: c.start())

    def sent(t):
        on_kind(t, lambda c: c.wait_send(), lambda c: c.wait())

    def pack(t):
        for c in load(t):
            c.wait()
        slot, out = t % LOADS, t % depth
        first = t // n % PIECES * rows
        left = lens_ref[peer(t % n, n) * req_local + t // n // PIECES] - me * (rows * PIECES) - first
        gain = gain_ref[...].astype(jnp.float32)

        @pl.loop(0, rows, step=STRIPE)
        def _(r):
            r = pl.multiple_of(r, STRIPE)
            lat = c_buf[slot, pl.ds(r, STRIPE), :].astype(jnp.float32)
            inv = lax.rsqrt(jnp.mean(lat * lat, axis=-1, keepdims=True) + NORM_EPS)
            valid = r + lax.broadcasted_iota(jnp.int32, (STRIPE, 1), 0) < left
            out_buf[out, pl.ds(r, STRIPE), :] = jnp.where(valid, lat * inv * gain, 0.0).astype(jnp.bfloat16)

        key = k_buf[slot].astype(jnp.float32)
        half = width // 2
        lo, hi = key[:half], key[half:]
        first = pl.multiple_of(first, LANES)
        cos, sin = cos_ref[:, pl.ds(first, rows)], sin_ref[:, pl.ds(first, rows)]
        valid = lax.broadcasted_iota(jnp.int32, (1, rows), 1) < left
        rotated = (jnp.where(valid, lo * cos - hi * sin, 0.0).astype(jnp.bfloat16),
                   jnp.where(valid, hi * cos + lo * sin, 0.0).astype(jnp.bfloat16))
        for kr_rows, kr_cols, to_rows, to_cols in rope_tiles(width, rows):
            part, at = kr_rows.start // half, kr_rows.start % half
            out_buf[out, to_rows, to_cols] = rotated[part][at : at + SUBLANES, kr_cols]

    barrier = pltpu.get_barrier_semaphore()
    for j in range(n - 1):
        pl.semaphore_signal(barrier, inc=1, device_id={"x": peer(j, n)}, device_id_type=MESH)
    for t in range(LOADS):
        for c in load(t):
            c.start()
    pack(0)
    for c in load(LOADS):
        c.start()
    pl.semaphore_wait(barrier, n - 1)

    state = (m_ref, l_ref, acc_ref)
    per_req = PIECES * n
    folds = (req_local - 1) * per_req
    lag = depth + n

    def received(a):
        src = peer(a % n, n)
        piece = land_ref.at[a // per_req, src, a // n % PIECES]
        pltpu.make_async_remote_copy(
            src_ref=piece, dst_ref=piece, send_sem=send_sem.at[0], recv_sem=recv_sem.at[a // n * n + src],
            device_id={"x": src}, device_id_type=MESH).wait_recv()

    def fetch(a):
        return pltpu.make_async_copy(land_ref.at[a // per_req, peer(a % n, n), a // n % PIECES], fold_buf.at[a % (AHEAD + 1)], fold_sem.at[a % (AHEAD + 1)])

    @pl.loop(1, folds + lag)
    def _(t):
        @pl.when(t >= depth)
        def _():
            sent(t - depth)

        @pl.when(t < steps)
        def _():
            pack(t)

            @pl.when(t + LOADS < steps)
            def _():
                for c in load(t + LOADS):
                    c.start()

        @pl.when(t <= steps)
        def _():
            start(t - 1)

        arriving = t - lag + AHEAD

        @pl.when(jnp.logical_and(arriving >= 0, arriving < folds))
        def _():
            @pl.when(arriving % n < n - 1)
            def _():
                received(arriving)

            fetch(arriving).start()

        a = t - lag

        @pl.when(a >= 0)
        def _():
            m, src, slot = a // per_req, peer(a % n, n), a % (AHEAD + 1)

            @pl.when(a % per_req == 0)
            def _():
                clear(state)

            fetch(a).wait()
            for kr_rows, kr_cols, from_rows, from_cols in rope_tiles(width, rows):
                kr_buf[kr_rows, kr_cols] = fold_buf[slot, from_rows, from_cols]
            first = (src * PIECES + a // n % PIECES) * rows
            fold(state, qa_ref[m], qr_ref[m], [(fold_buf[slot, :rows, :], kr_buf[...])], [first], lens_ref[me * req_local + m], scale)

            @pl.when(a % per_req == per_req - 1)
            def _():
                o_out[m] = (acc_ref[...] / l_ref[...]).astype(jnp.bfloat16)

    @pl.loop(folds + lag - depth, steps)
    def _(t):
        sent(t)

    @pl.loop(folds, early)
    def _(a):
        @pl.when(a % n < n - 1)
        def _():
            received(a)


def send(lens, c_raw, k_raw, gain, cos, sin, q_lat, q_rope, n):
    req_local, heads, _ = q_lat.shape
    requests, block, rank = c_raw.shape
    width = k_raw.shape[1]
    rows = block // PIECES
    total = rows + rows * width // rank
    depth = ROUNDS * n
    return pl.pallas_call(
        functools.partial(send_kernel, n, req_local, (rank + width) ** -0.5),
        in_specs=[SMEM, HBM, HBM] + [VMEM] * 5,
        out_specs=[HBM, VMEM] + [HBM] * n,
        out_shape=[jax.ShapeDtypeStruct((req_local, n, PIECES, total, rank), jnp.bfloat16),
                   jax.ShapeDtypeStruct((req_local - 1, heads, rank), jnp.bfloat16)]
        + [jax.ShapeDtypeStruct((total, rank), jnp.bfloat16)] * n,
        scratch_shapes=[
            pltpu.VMEM((LOADS, rows, rank), jnp.bfloat16),
            pltpu.VMEM((LOADS, width, rows), jnp.bfloat16),
            pltpu.VMEM((depth, total, rank), jnp.bfloat16),
            pltpu.SemaphoreType.DMA((LOADS,)),
            pltpu.SemaphoreType.DMA((LOADS,)),
            pltpu.SemaphoreType.DMA((depth,)),
            pltpu.SemaphoreType.DMA(((req_local * PIECES - 1) * n,)),
            pltpu.VMEM((heads, 1), jnp.float32),
            pltpu.VMEM((heads, 1), jnp.float32),
            pltpu.VMEM((heads, rank), jnp.float32),
            pltpu.VMEM((AHEAD + 1, total, rank), jnp.bfloat16),
            pltpu.VMEM((width, rows), jnp.bfloat16),
            pltpu.SemaphoreType.DMA((AHEAD + 1,)),
        ],
        compiler_params=pltpu.CompilerParams(vmem_limit_bytes=VMEM_BYTES, collective_id=0, has_side_effects=True),
        cost_estimate=pl.CostEstimate(flops=requests * block * rank * 100, bytes_accessed=requests * block * rank * 4, transcendentals=0),
        name="send",
    )(lens, c_raw, k_raw, gain, cos, sin, q_lat, q_rope)


def stream(n, req_local, scale, group, length, land, queries, c_out, kr_out, state, buf, kr_buf, zero_c, zero_k, in_sem, c_sem, k_sem, ahead):
    first_req, count, first_piece, pieces = group
    depth = buf.shape[0]
    rank = buf.shape[3]
    width = kr_buf.shape[1]
    rows = buf.shape[2] * rank // (rank + width)
    span = rows * PIECES
    steps = count * n

    def used(t):
        return t % n * span + first_piece * rows < length(first_req + t // n)

    def load(t):
        return pltpu.make_async_copy(land(t // n, t % n), buf.at[t % depth, pl.ds(0, pieces)], in_sem.at[t % depth])

    def stores(t):
        slot, req = t % depth, first_req + t // n
        at = pl.multiple_of(t % n * span + first_piece * rows, rows)
        kr = pltpu.make_async_copy(kr_buf.at[slot, :, pl.ds(0, pieces * rows)], kr_out.at[req, :, pl.ds(at, pieces * rows)], k_sem.at[slot])
        cs = [pltpu.make_async_copy(buf.at[slot, h, pl.ds(0, rows), :], c_out.at[req, pl.ds(at + h * rows, rows), :], c_sem.at[slot, h]) for h in range(pieces)]
        return cs + [kr]

    def blanks(t):
        slot, req = t % depth, first_req + t // n
        at = pl.multiple_of(t % n * span + first_piece * rows, rows)
        kr = pltpu.make_async_copy(zero_k.at[:, pl.ds(0, pieces * rows)], kr_out.at[req, :, pl.ds(at, pieces * rows)], k_sem.at[slot])
        cs = [pltpu.make_async_copy(zero_c, c_out.at[req, pl.ds(at + h * rows, rows), :], c_sem.at[slot, h]) for h in range(pieces)]
        return cs + [kr]

    def fetch(t):
        @pl.when(used(t))
        def _():
            load(t).start()

    def work(t):
        slot, req = t % depth, first_req + t // n
        load(t).wait()
        for h in range(pieces):
            for kr_rows, kr_cols, from_rows, from_cols in rope_tiles(width, rows):
                cols = slice(h * rows + kr_cols.start, h * rows + kr_cols.stop)
                kr_buf[slot, kr_rows, cols] = buf[slot, h, from_rows, from_cols]
        for c in stores(t):
            c.start()
        if queries is not None:
            qa, qr = queries(t)
            blocks = [(buf[slot, h, :rows, :], kr_buf[slot, :, h * rows : (h + 1) * rows]) for h in range(pieces)]
            firsts = [t % n * span + (first_piece + h) * rows for h in range(pieces)]
            fold(state, qa, qr, blocks, firsts, length(req), scale)

    def body(t):
        @pl.when(used(t))
        def _():
            work(t)

        @pl.when(jnp.logical_not(used(t)))
        def _():
            for c in blanks(t):
                c.start()

        @pl.when(t + ahead < steps)
        def _():
            @pl.when(t + ahead >= depth)
            def _():
                for c in stores(t + ahead - depth):
                    c.wait()

            fetch(t + ahead)

    def prologue():
        for t in range(min(ahead, steps)):
            fetch(t)

    def drain():
        @pl.loop(max(steps - depth, 0), steps)
        def _(t):
            for c in stores(t):
                c.wait()

    return steps, prologue, body, drain


def first_kernel(n, req_local, scale, lens_ref, land_ref, qa_ref, qr_ref, o_done, c_out, kr_out, o_out, part_out, o_sem,
                 m_ref, l_ref, acc_ref, part_ref, part_sem, zero_c, zero_k, buf, in_sem, kr_buf, c_sem, k_sem,
                 side_buf, side_in_sem, side_kr_buf, side_c_sem, side_k_sem):
    length = lambda m: lens_ref[lax.axis_index("x") * req_local + m]
    state = (m_ref, l_ref, acc_ref)
    last = req_local - 1
    rank = acc_ref.shape[1]
    done = pltpu.make_async_copy(o_done, o_out.at[pl.ds(0, last)], o_sem)
    piece = lambda m, i: land_ref.at[last, i, pl.ds(0, PIECES - 1)]
    whole = lambda m, i: land_ref.at[m, i]
    side_steps, side_prologue, side_body, side_drain = stream(
        n, req_local, scale, (last, 1, 0, PIECES - 1), length, piece, lambda t: (qa_ref[last], qr_ref[last]), c_out, kr_out, state,
        side_buf, side_kr_buf, zero_c, zero_k, side_in_sem, side_c_sem, side_k_sem, n)
    steps, prologue, body, drain = stream(
        n, req_local, scale, (0, last, 0, PIECES), length, whole, None, c_out, kr_out, state,
        buf, kr_buf, zero_c, zero_k, in_sem, c_sem, k_sem, buf.shape[0] // 2)

    side_prologue()
    prologue()
    done.start()
    zero_c[...] = jnp.zeros_like(zero_c)
    zero_k[...] = jnp.zeros_like(zero_k)
    clear(state)
    every = steps // side_steps

    @pl.loop(0, steps)
    def _(t):
        body(t)

        @pl.when(t % every == 0)
        def _():
            side_body(t // every)

    part_ref[:, :rank] = acc_ref[...]
    part_ref[:, rank : rank + LANES] = jnp.broadcast_to(m_ref[...], (part_ref.shape[0], LANES))
    part_ref[:, rank + LANES :] = jnp.broadcast_to(l_ref[...], (part_ref.shape[0], LANES))
    copy = pltpu.make_async_copy(part_ref, part_out, part_sem)
    copy.start()
    copy.wait()
    drain()
    side_drain()
    done.wait()


def last_kernel(n, req_local, scale, lens_ref, *refs):
    land_refs, refs = refs[:n], refs[n:]
    qa_ref, qr_ref, part_ref, c_old, kr_old, o_old, c_out, kr_out, o_out, *refs = refs
    m_ref, l_ref, acc_ref, o_buf, o_sem, kr_buf, c_sem, k_sem = refs
    last = req_local - 1
    length = lens_ref[lax.axis_index("x") * req_local + last]
    state = (m_ref, l_ref, acc_ref)
    rank = acc_ref.shape[1]
    width = kr_buf.shape[1]
    rows = kr_buf.shape[2]
    block = rows * PIECES
    firsts = [pl.multiple_of(move(lax.axis_index("x"), i, n, -1) * block + block - rows, rows) for i in range(n)]
    clear(state)
    stores = []
    for at in range(0, n, BATCH):
        batch = range(at, at + BATCH)
        for i in batch:
            first = firsts[i]
            stores.append(pltpu.make_async_copy(land_refs[i].at[pl.ds(0, rows), :], c_out.at[last, pl.ds(first, rows), :], c_sem.at[i]))
            stores[-1].start()
            for kr_rows, kr_cols, from_rows, from_cols in rope_tiles(width, rows):
                kr_buf[i, kr_rows, kr_cols] = land_refs[i][from_rows, from_cols]
            stores.append(pltpu.make_async_copy(kr_buf.at[i], kr_out.at[last, :, pl.ds(first, rows)], k_sem.at[i]))
            stores[-1].start()

        @pl.when(functools.reduce(jnp.minimum, [firsts[i] for i in batch]) < length)
        def _():
            blocks = [(land_refs[i][:rows, :], kr_buf[i]) for i in batch]
            fold(state, qa_ref[last], qr_ref[last], blocks, [firsts[i] for i in batch], length, scale)

    m_part, l_part, acc_part = part_ref[:, rank : rank + 1], part_ref[:, rank + LANES : rank + LANES + 1], part_ref[:, :rank]
    m_new = jnp.maximum(m_ref[...], m_part)
    here, there = jnp.exp(m_ref[...] - m_new), jnp.exp(m_part - m_new)
    total = l_ref[...] * here + l_part * there
    o_buf[...] = ((acc_ref[...] * here + acc_part * there) / total).astype(jnp.bfloat16)
    copy = pltpu.make_async_copy(o_buf, o_out.at[last], o_sem)
    copy.start()
    for c in stores + [copy]:
        c.wait()


def attend(lens, landed, rest, o_done, q_lat, q_rope, n, block):
    req_local, heads, rank = q_lat.shape
    width = q_rope.shape[1]
    rows = block // PIECES
    total = rest[0].shape[0]
    scale = (rank + width) ** -0.5
    caches = [jax.ShapeDtypeStruct((req_local, n * block, rank), jnp.bfloat16),
              jax.ShapeDtypeStruct((req_local, width, n * block), jnp.bfloat16),
              jax.ShapeDtypeStruct((req_local, heads, rank), jnp.bfloat16)]
    part = jax.ShapeDtypeStruct((heads, rank + 2 * LANES), jnp.float32)
    state = [pltpu.VMEM((heads, 1), jnp.float32), pltpu.VMEM((heads, 1), jnp.float32), pltpu.VMEM((heads, rank), jnp.float32)]

    def ring(depth, *pieces):
        count = pieces[0] if pieces else 1
        return [pltpu.VMEM((depth, *pieces, total, rank), jnp.bfloat16), pltpu.SemaphoreType.DMA((depth,)),
                pltpu.VMEM((depth, width, count * rows), jnp.bfloat16), pltpu.SemaphoreType.DMA((depth, *pieces)), pltpu.SemaphoreType.DMA((depth,))]

    params = pltpu.CompilerParams(vmem_limit_bytes=ATTEND_BYTES)
    flops = 2 * req_local * n * block * heads * rank
    *outs, first_part = pl.pallas_call(
        functools.partial(first_kernel, n, req_local, scale),
        in_specs=[SMEM, HBM, VMEM, VMEM, HBM],
        out_specs=[HBM] * 4,
        out_shape=caches + [part],
        scratch_shapes=[pltpu.SemaphoreType.DMA] + state + [pltpu.VMEM(part.shape, part.dtype), pltpu.SemaphoreType.DMA,
                                                            pltpu.VMEM((rows, rank), jnp.bfloat16), pltpu.VMEM((width, block), jnp.bfloat16)]
        + ring(RING, PIECES) + ring(n, PIECES - 1),
        compiler_params=params,
        cost_estimate=pl.CostEstimate(flops=flops, bytes_accessed=req_local * n * block * rank * 4, transcendentals=0),
        name="attend_first",
    )(lens, landed, q_lat, q_rope, o_done)
    return pl.pallas_call(
        functools.partial(last_kernel, n, req_local, scale),
        in_specs=[SMEM] + [VMEM] * (n + 3) + [HBM] * 3,
        out_specs=[HBM] * 3,
        out_shape=caches,
        scratch_shapes=state + [pltpu.VMEM((heads, rank), jnp.bfloat16), pltpu.SemaphoreType.DMA] + ring(n)[2:],
        input_output_aliases={n + 4: 0, n + 5: 1, n + 6: 2},
        compiler_params=params,
        cost_estimate=pl.CostEstimate(flops=flops // req_local // PIECES, bytes_accessed=n * block * rank * 2, transcendentals=0),
        name="attend_last",
    )(lens, *rest, q_lat, q_rope, first_part, *outs)


def solution(mesh):
    seq_spec = P("dp", "x", None)
    req_spec = P(("dp", "x"), None, None)
    n = mesh.shape["x"]

    def local_step(c_raw, k_raw, norm_gain, rope_cos, rope_sin, seq_lens, q_lat, q_rope):
        q_rope = jnp.swapaxes(q_rope, 1, 2)
        landed, o_done, *rest = send(seq_lens, c_raw, jnp.swapaxes(k_raw, 1, 2), norm_gain, rope_cos.T, rope_sin.T, q_lat, q_rope, n)
        rest = [lax.ppermute(piece, "x", [(i, move(i, j, n, 1)) for i in range(n)]) for j, piece in enumerate(rest[:-1])] + rest[-1:]
        c_cache, kr_cache, o_lat = attend(seq_lens, landed, rest, o_done, q_lat, q_rope, n, c_raw.shape[1])
        return c_cache, jnp.swapaxes(kr_cache, 1, 2), o_lat

    return jax.shard_map(local_step, mesh=mesh, in_specs=(seq_spec, seq_spec, P(None), P("x", None), P("x", None), P("dp"), req_spec, req_spec), out_specs=(req_spec, req_spec, req_spec), check_vma=False)
```

```python
import functools

import jax
import jax.numpy as jnp
from jax import lax
from jax.experimental import pallas as pl
from jax.experimental.pallas import tpu as pltpu
from jax.sharding import PartitionSpec as P

NORM_EPS = 1e-6
PIECES = 3
ROUNDS = 6
LOADS = 4
RING = 12
LATE = 2
BATCH = 4
AHEAD = 3
STRIPE = 128
LANES, SUBLANES = 128, 16
VMEM_BYTES = 60 * 1024 * 1024
ATTEND_BYTES = 44 * 1024 * 1024
MESH = pl.DeviceIdType.MESH
HBM = pl.BlockSpec(memory_space=pltpu.HBM)
VMEM = pl.BlockSpec(memory_space=pltpu.VMEM)
SMEM = pl.BlockSpec(memory_space=pltpu.SMEM)


def move(me, j, n, way):
    chip, core = me // 2, me % 2
    far = j % 3
    last = j // (n - 2)
    hop = (1 - last) * (1 + 2 * far - 3 * (far // 2))
    other = (j // 3) % 2 * (1 - last) + last * (1 - j % (n - 2))
    return (chip + n // 2 + way * hop) % (n // 2) * 2 + (core + other) % 2


def peer(j, n):
    return move(lax.axis_index("x"), j, n, 1)


def is_late(j, n):
    return jnp.logical_and(j % 3 < 2, j < n - 2)


def late_steps(n):
    return [j for j in range(n - 2) if j % 3 < 2]


def result_place(land_ref, m, n):
    count = len(late_steps(n))
    j = m % count // 2 * 3 + m % count % 2
    return land_ref.at[land_ref.shape[0] - 1, move(lax.axis_index("x"), j, n, -1), PIECES - LATE + m // count]


def rope_tiles(width, rows):
    for r in range(width // SUBLANES):
        for c in range(rows // LANES):
            yield (slice(r * SUBLANES, (r + 1) * SUBLANES), slice(c * LANES, (c + 1) * LANES),
                   slice(rows + c * SUBLANES, rows + (c + 1) * SUBLANES), slice(r * LANES, (r + 1) * LANES))


def clear(state):
    m_ref, l_ref, acc_ref = state
    m_ref[...] = jnp.full_like(m_ref, -1e30)
    l_ref[...] = jnp.zeros_like(l_ref)
    acc_ref[...] = jnp.zeros_like(acc_ref)


def fold(state, qa, qr, pieces, firsts, length, scale):
    m_ref, l_ref, acc_ref = state
    scores = []
    for first, (lat, kr) in zip(firsts, pieces):
        s = lax.dot_general(qa, lat, (((1,), (1,)), ((), ())), preferred_element_type=jnp.float32)
        s = s + lax.dot_general(qr, kr, (((0,), (0,)), ((), ())), preferred_element_type=jnp.float32)
        rows = lat.shape[0]
        pos = first + lax.broadcasted_iota(jnp.int32, (1, rows), 1)
        scores.append(jnp.where(pos < length, s * scale, -1e30))
    m_old = m_ref[...]
    m_new = m_old
    for s in scores:
        m_new = jnp.maximum(m_new, jnp.max(s, axis=-1, keepdims=True))
    alpha = jnp.exp(m_old - m_new)
    total, acc = l_ref[...] * alpha, acc_ref[...] * alpha
    for s, (lat, _) in zip(scores, pieces):
        p = jnp.exp(s - m_new)
        total = total + jnp.sum(p, axis=-1, keepdims=True)
        acc = acc + jnp.dot(p.astype(jnp.bfloat16), lat, preferred_element_type=jnp.float32)
    m_ref[...], l_ref[...], acc_ref[...] = m_new, total, acc


def send_kernel(n, req_local, scale, lens_ref, c_hbm, k_hbm, gain_ref, cos_ref, sin_ref, qa_ref, qr_ref, land_ref, *scratch):
    late = late_steps(n)
    rest_refs, scratch = scratch[:len(late)], scratch[len(late):]
    c_buf, k_buf, out_buf, c_sem, k_sem, send_sem, recv_sem, m_ref, l_ref, acc_ref, fold_buf, kr_buf, fold_sem, o_buf, o_sem = scratch
    me = lax.axis_index("x")
    rounds = req_local * PIECES
    steps = rounds * n
    early = (rounds - LATE) * n
    depth = out_buf.shape[0]
    rows, rank = c_buf.shape[1:]
    width = k_buf.shape[1]

    def load(t):
        req = peer(t % n, n) * req_local + t // n // PIECES
        first = pl.multiple_of(t // n % PIECES * rows, rows)
        slot = t % LOADS
        return (pltpu.make_async_copy(c_hbm.at[req, pl.ds(first, rows), :], c_buf.at[slot], c_sem.at[slot]),
                pltpu.make_async_copy(k_hbm.at[req, :, pl.ds(first, rows)], k_buf.at[slot], k_sem.at[slot]))

    def landing(t):
        return land_ref.at[t // n // PIECES, me, t // n % PIECES]

    def remote(t):
        slot = t % depth
        return pltpu.make_async_remote_copy(
            src_ref=out_buf.at[slot], dst_ref=landing(t), send_sem=send_sem.at[slot],
            recv_sem=recv_sem.at[t // n * n + me], device_id={"x": peer(t % n, n)}, device_id_type=MESH)

    def own(t):
        return pltpu.make_async_copy(out_buf.at[t % depth], landing(t), send_sem.at[t % depth])

    def keep(t, k, h):
        return pltpu.make_async_copy(out_buf.at[t % depth], rest_refs[k].at[h], send_sem.at[t % depth])

    def on_kind(t, act_remote, act_local):
        is_own = t % n == n - 1
        is_kept = jnp.logical_and(t >= early, is_late(t % n, n))

        for k, j in enumerate(late):
            for h in range(LATE):
                @pl.when(t == early + h * n + j)
                def _():
                    act_local(keep(t, k, h))

        @pl.when(is_own)
        def _():
            act_local(own(t))

        @pl.when(jnp.logical_not(jnp.logical_or(is_own, is_kept)))
        def _():
            act_remote(remote(t))

    def start(t):
        on_kind(t, lambda c: c.start(), lambda c: c.start())

    def sent(t):
        on_kind(t, lambda c: c.wait_send(), lambda c: c.wait())

    def pack(t):
        for c in load(t):
            c.wait()
        slot, out = t % LOADS, t % depth
        first = t // n % PIECES * rows
        left = lens_ref[peer(t % n, n) * req_local + t // n // PIECES] - me * (rows * PIECES) - first
        gain = gain_ref[...].astype(jnp.float32)

        @pl.loop(0, rows, step=STRIPE)
        def _(r):
            r = pl.multiple_of(r, STRIPE)
            lat = c_buf[slot, pl.ds(r, STRIPE), :].astype(jnp.float32)
            inv = lax.rsqrt(jnp.mean(lat * lat, axis=-1, keepdims=True) + NORM_EPS)
            valid = r + lax.broadcasted_iota(jnp.int32, (STRIPE, 1), 0) < left
            out_buf[out, pl.ds(r, STRIPE), :] = jnp.where(valid, lat * inv * gain, 0.0).astype(jnp.bfloat16)

        key = k_buf[slot].astype(jnp.float32)
        half = width // 2
        lo, hi = key[:half], key[half:]
        first = pl.multiple_of(first, LANES)
        cos, sin = cos_ref[:, pl.ds(first, rows)], sin_ref[:, pl.ds(first, rows)]
        valid = lax.broadcasted_iota(jnp.int32, (1, rows), 1) < left
        rotated = (jnp.where(valid, lo * cos - hi * sin, 0.0).astype(jnp.bfloat16),
                   jnp.where(valid, hi * cos + lo * sin, 0.0).astype(jnp.bfloat16))
        for kr_rows, kr_cols, to_rows, to_cols in rope_tiles(width, rows):
            part, at = kr_rows.start // half, kr_rows.start % half
            out_buf[out, to_rows, to_cols] = rotated[part][at : at + SUBLANES, kr_cols]

    barrier = pltpu.get_barrier_semaphore()
    for j in range(n - 1):
        pl.semaphore_signal(barrier, inc=1, device_id={"x": peer(j, n)}, device_id_type=MESH)
    for t in range(LOADS):
        for c in load(t):
            c.start()
    pack(0)
    for c in load(LOADS):
        c.start()
    pl.semaphore_wait(barrier, n - 1)

    state = (m_ref, l_ref, acc_ref)
    per_req = PIECES * n
    folds = (req_local - 1) * per_req
    lag = depth + n

    def received(a):
        src = peer(a % n, n)
        piece = land_ref.at[a // per_req, src, a // n % PIECES]
        pltpu.make_async_remote_copy(
            src_ref=piece, dst_ref=piece, send_sem=send_sem.at[0], recv_sem=recv_sem.at[a // n * n + src],
            device_id={"x": src}, device_id_type=MESH).wait_recv()

    def result(m):
        return pltpu.make_async_copy(o_buf.at[m], result_place(land_ref, m, n).at[pl.ds(0, o_buf.shape[1]), :], o_sem.at[m])

    def fetch(a):
        return pltpu.make_async_copy(land_ref.at[a // per_req, peer(a % n, n), a // n % PIECES], fold_buf.at[a % (AHEAD + 1)], fold_sem.at[a % (AHEAD + 1)])

    @pl.loop(1, folds + lag)
    def _(t):
        @pl.when(t >= depth)
        def _():
            sent(t - depth)

        @pl.when(t < steps)
        def _():
            pack(t)

            @pl.when(t + LOADS < steps)
            def _():
                for c in load(t + LOADS):
                    c.start()

        @pl.when(t <= steps)
        def _():
            start(t - 1)

        arriving = t - lag + AHEAD

        @pl.when(jnp.logical_and(arriving >= 0, arriving < folds))
        def _():
            @pl.when(arriving % n < n - 1)
            def _():
                received(arriving)

            fetch(arriving).start()

        a = t - lag

        @pl.when(a >= 0)
        def _():
            m, src, slot = a // per_req, peer(a % n, n), a % (AHEAD + 1)

            @pl.when(a % per_req == 0)
            def _():
                clear(state)

            fetch(a).wait()
            for kr_rows, kr_cols, from_rows, from_cols in rope_tiles(width, rows):
                kr_buf[kr_rows, kr_cols] = fold_buf[slot, from_rows, from_cols]
            first = (src * PIECES + a // n % PIECES) * rows
            fold(state, qa_ref[m], qr_ref[m], [(fold_buf[slot, :rows, :], kr_buf[...])], [first], lens_ref[me * req_local + m], scale)

            @pl.when(a % per_req == per_req - 1)
            def _():
                o_buf[m] = (acc_ref[...] / l_ref[...]).astype(jnp.bfloat16)
                result(m).start()

    @pl.loop(folds + lag - depth, steps)
    def _(t):
        sent(t)

    @pl.loop(folds, steps)
    def _(a):
        @pl.when(jnp.logical_and(a % n < n - 1, jnp.logical_not(jnp.logical_and(a >= early, is_late(a % n, n)))))
        def _():
            received(a)

    for m in range(req_local - 1):
        result(m).wait()


def send(lens, c_raw, k_raw, gain, cos, sin, q_lat, q_rope, n):
    req_local, heads, _ = q_lat.shape
    requests, block, rank = c_raw.shape
    width = k_raw.shape[1]
    rows = block // PIECES
    total = rows + rows * width // rank
    depth = ROUNDS * n
    return pl.pallas_call(
        functools.partial(send_kernel, n, req_local, (rank + width) ** -0.5),
        in_specs=[SMEM, HBM, HBM] + [VMEM] * 5,
        out_specs=[HBM] * (1 + len(late_steps(n))),
        out_shape=[jax.ShapeDtypeStruct((req_local, n, PIECES, total, rank), jnp.bfloat16)]
        + [jax.ShapeDtypeStruct((LATE, total, rank), jnp.bfloat16)] * len(late_steps(n)),
        scratch_shapes=[
            pltpu.VMEM((LOADS, rows, rank), jnp.bfloat16),
            pltpu.VMEM((LOADS, width, rows), jnp.bfloat16),
            pltpu.VMEM((depth, total, rank), jnp.bfloat16),
            pltpu.SemaphoreType.DMA((LOADS,)),
            pltpu.SemaphoreType.DMA((LOADS,)),
            pltpu.SemaphoreType.DMA((depth,)),
            pltpu.SemaphoreType.DMA((req_local * PIECES * n,)),
            pltpu.VMEM((heads, 1), jnp.float32),
            pltpu.VMEM((heads, 1), jnp.float32),
            pltpu.VMEM((heads, rank), jnp.float32),
            pltpu.VMEM((AHEAD + 1, total, rank), jnp.bfloat16),
            pltpu.VMEM((width, rows), jnp.bfloat16),
            pltpu.SemaphoreType.DMA((AHEAD + 1,)),
            pltpu.VMEM((req_local - 1, heads, rank), jnp.bfloat16),
            pltpu.SemaphoreType.DMA((req_local - 1,)),
        ],
        compiler_params=pltpu.CompilerParams(vmem_limit_bytes=VMEM_BYTES, collective_id=0, has_side_effects=True),
        cost_estimate=pl.CostEstimate(flops=requests * block * rank * 100, bytes_accessed=requests * block * rank * 4, transcendentals=0),
        name="send",
    )(lens, c_raw, k_raw, gain, cos, sin, q_lat, q_rope)


def stream(steps, place, first_piece, pieces, scale, length, land_ref, queries, c_out, kr_out, state, zero_c, zero_k, ring, ahead):
    buf, in_sem, kr_buf, c_sem, k_sem = ring
    depth = buf.shape[0]
    rank = buf.shape[3]
    width = kr_buf.shape[1]
    rows = kr_buf.shape[2] // pieces

    def first(t):
        return pl.multiple_of((place(t)[1] * PIECES + first_piece) * rows, rows)

    def used(t):
        return first(t) < length(place(t)[0])

    def load(t):
        req, src = place(t)
        return pltpu.make_async_copy(land_ref.at[req, src, pl.ds(first_piece, pieces)], buf.at[t % depth], in_sem.at[t % depth])

    def writes(t, c_of, kr):
        slot, req, at = t % depth, place(t)[0], first(t)
        return [pltpu.make_async_copy(c_of(h), c_out.at[req, pl.ds(at + h * rows, rows), :], c_sem.at[slot, h]) for h in range(pieces)] + [
            pltpu.make_async_copy(kr, kr_out.at[req, :, pl.ds(at, pieces * rows)], k_sem.at[slot])]

    def stores(t):
        return writes(t, lambda h: buf.at[t % depth, h, pl.ds(0, rows), :], kr_buf.at[t % depth])

    def blanks(t):
        return writes(t, lambda h: zero_c, zero_k.at[:, pl.ds(0, pieces * rows)])

    def fetch(t):
        @pl.when(used(t))
        def _():
            load(t).start()

    def work(t):
        slot = t % depth
        load(t).wait()
        for h in range(pieces):
            for kr_rows, kr_cols, from_rows, from_cols in rope_tiles(width, rows):
                cols = slice(h * rows + kr_cols.start, h * rows + kr_cols.stop)
                kr_buf[slot, kr_rows, cols] = buf[slot, h, from_rows, from_cols]
        for c in stores(t):
            c.start()
        if queries is not None:
            qa, qr = queries()
            blocks = [(buf[slot, h, :rows, :], kr_buf[slot, :, h * rows : (h + 1) * rows]) for h in range(pieces)]
            fold(state, qa, qr, blocks, [first(t) + h * rows for h in range(pieces)], length(place(t)[0]), scale)

    def body(t):
        @pl.when(used(t))
        def _():
            work(t)

        @pl.when(jnp.logical_not(used(t)))
        def _():
            for c in blanks(t):
                c.start()

        @pl.when(t + ahead < steps)
        def _():
            @pl.when(t + ahead >= depth)
            def _():
                for c in stores(t + ahead - depth):
                    c.wait()

            fetch(t + ahead)

    def prologue():
        for t in range(min(ahead, steps)):
            fetch(t)

    def drain():
        @pl.loop(max(steps - depth, 0), steps)
        def _(t):
            for c in stores(t):
                c.wait()

    return steps, prologue, body, drain


def first_kernel(n, req_local, scale, lens_ref, land_ref, qa_ref, qr_ref, c_out, kr_out, o_out, part_out,
                 m_ref, l_ref, acc_ref, part_ref, part_sem, zero_c, zero_k, o_buf, o_in_sem, o_out_sem, *rings):
    length = lambda m: lens_ref[lax.axis_index("x") * req_local + m]
    state = (m_ref, l_ref, acc_ref)
    last = req_local - 1
    rank = acc_ref.shape[1]
    near = [j for j in range(n) if j not in late_steps(n)]
    base = move(lax.axis_index("x"), 2, n, 1) // 2, lax.axis_index("x") // 2
    queries = lambda: (qa_ref[last], qr_ref[last])
    common = (scale, length, land_ref)
    outs = (c_out, kr_out, state, zero_c, zero_k)
    main = stream(last * n, lambda t: (t // n, t % n), 0, PIECES, *common, None, *outs, rings[:5], RING // 2)
    front = stream(n, lambda t: (last, t), 0, PIECES - LATE, *common, queries, *outs, rings[5:10], n)
    back = stream(len(near), lambda t: (last, (base[0] + t // 2 * (base[1] - base[0])) * 2 + t % 2), PIECES - LATE, LATE, *common, queries, *outs, rings[10:], len(near))
    results = [(pltpu.make_async_copy(result_place(land_ref, m, n).at[pl.ds(0, o_buf.shape[1]), :], o_buf.at[m], o_in_sem.at[m]),
                pltpu.make_async_copy(o_buf.at[m], o_out.at[m], o_out_sem.at[m])) for m in range(last)]

    for part in (front, back, main):
        part[1]()
    for take, _ in results:
        take.start()
    zero_c[...] = jnp.zeros_like(zero_c)
    zero_k[...] = jnp.zeros_like(zero_k)
    clear(state)
    steps = main[0]

    @pl.loop(0, steps)
    def _(t):
        main[2](t)

        @pl.when(t % (steps // n) == 0)
        def _():
            front[2](t // (steps // n))

        every = steps // len(near)

        @pl.when(t % every == every // 2)
        def _():
            back[2](t // every)

    for take, give in results:
        take.wait()
        give.start()
    part_ref[:, :rank] = acc_ref[...]
    part_ref[:, rank : rank + LANES] = jnp.broadcast_to(m_ref[...], (part_ref.shape[0], LANES))
    part_ref[:, rank + LANES :] = jnp.broadcast_to(l_ref[...], (part_ref.shape[0], LANES))
    copy = pltpu.make_async_copy(part_ref, part_out, part_sem)
    copy.start()
    copy.wait()
    for part in (main, front, back):
        part[3]()
    for _, give in results:
        give.wait()


def last_kernel(n, req_local, scale, lens_ref, *refs):
    late = late_steps(n)
    land_refs, refs = refs[:len(late)], refs[len(late):]
    qa_ref, qr_ref, part_ref, c_old, kr_old, o_old, c_out, kr_out, o_out, *refs = refs
    m_ref, l_ref, acc_ref, o_buf, o_sem, kr_buf, c_sem, k_sem = refs
    last = req_local - 1
    length = lens_ref[lax.axis_index("x") * req_local + last]
    state = (m_ref, l_ref, acc_ref)
    rank = acc_ref.shape[1]
    width = kr_buf.shape[1]
    rows = kr_buf.shape[2]
    pieces = [(k, h) for k in range(len(late)) for h in range(LATE)]
    firsts = [pl.multiple_of((move(lax.axis_index("x"), late[k], n, -1) * PIECES + PIECES - LATE + h) * rows, rows) for k, h in pieces]
    clear(state)
    stores = []
    for at in range(0, len(pieces), BATCH):
        batch = range(at, at + BATCH)
        for i in batch:
            (k, h), first = pieces[i], firsts[i]
            stores.append(pltpu.make_async_copy(land_refs[k].at[h, pl.ds(0, rows), :], c_out.at[last, pl.ds(first, rows), :], c_sem.at[i, 0]))
            stores[-1].start()
            for kr_rows, kr_cols, from_rows, from_cols in rope_tiles(width, rows):
                kr_buf[i, kr_rows, kr_cols] = land_refs[k][h, from_rows, from_cols]
            stores.append(pltpu.make_async_copy(kr_buf.at[i], kr_out.at[last, :, pl.ds(first, rows)], k_sem.at[i]))
            stores[-1].start()

        @pl.when(functools.reduce(jnp.minimum, [firsts[i] for i in batch]) < length)
        def _():
            blocks = [(land_refs[pieces[i][0]][pieces[i][1], :rows, :], kr_buf[i]) for i in batch]
            fold(state, qa_ref[last], qr_ref[last], blocks, [firsts[i] for i in batch], length, scale)

    m_part, l_part, acc_part = part_ref[:, rank : rank + 1], part_ref[:, rank + LANES : rank + LANES + 1], part_ref[:, :rank]
    m_new = jnp.maximum(m_ref[...], m_part)
    here, there = jnp.exp(m_ref[...] - m_new), jnp.exp(m_part - m_new)
    total = l_ref[...] * here + l_part * there
    o_buf[...] = ((acc_ref[...] * here + acc_part * there) / total).astype(jnp.bfloat16)
    copy = pltpu.make_async_copy(o_buf, o_out.at[last], o_sem)
    copy.start()
    for c in stores + [copy]:
        c.wait()


def attend(lens, landed, rest, q_lat, q_rope, n, block):
    req_local, heads, rank = q_lat.shape
    width = q_rope.shape[1]
    rows = block // PIECES
    total = rest[0].shape[1]
    late = len(late_steps(n))
    scale = (rank + width) ** -0.5
    caches = [jax.ShapeDtypeStruct((req_local, n * block, rank), jnp.bfloat16),
              jax.ShapeDtypeStruct((req_local, width, n * block), jnp.bfloat16),
              jax.ShapeDtypeStruct((req_local, heads, rank), jnp.bfloat16)]
    part = jax.ShapeDtypeStruct((heads, rank + 2 * LANES), jnp.float32)
    state = [pltpu.VMEM((heads, 1), jnp.float32), pltpu.VMEM((heads, 1), jnp.float32), pltpu.VMEM((heads, rank), jnp.float32)]

    def stores(depth, pieces):
        return [pltpu.VMEM((depth, width, pieces * rows), jnp.bfloat16), pltpu.SemaphoreType.DMA((depth, pieces)), pltpu.SemaphoreType.DMA((depth,))]

    def ring(depth, pieces):
        return [pltpu.VMEM((depth, pieces, total, rank), jnp.bfloat16), pltpu.SemaphoreType.DMA((depth,))] + stores(depth, pieces)

    params = pltpu.CompilerParams(vmem_limit_bytes=ATTEND_BYTES)
    flops = 2 * req_local * n * block * heads * rank
    *outs, first_part = pl.pallas_call(
        functools.partial(first_kernel, n, req_local, scale),
        in_specs=[SMEM, HBM, VMEM, VMEM],
        out_specs=[HBM] * 4,
        out_shape=caches + [part],
        scratch_shapes=state + [pltpu.VMEM(part.shape, part.dtype), pltpu.SemaphoreType.DMA,
                                pltpu.VMEM((rows, rank), jnp.bfloat16), pltpu.VMEM((width, block), jnp.bfloat16),
                                pltpu.VMEM((req_local - 1, heads, rank), jnp.bfloat16),
                                pltpu.SemaphoreType.DMA((req_local - 1,)), pltpu.SemaphoreType.DMA((req_local - 1,))]
        + ring(RING, PIECES) + ring(n, PIECES - LATE) + ring(n - late, LATE),
        compiler_params=params,
        cost_estimate=pl.CostEstimate(flops=flops, bytes_accessed=req_local * n * block * rank * 4, transcendentals=0),
        name="attend_first",
    )(lens, landed, q_lat, q_rope)
    return pl.pallas_call(
        functools.partial(last_kernel, n, req_local, scale),
        in_specs=[SMEM] + [VMEM] * (late + 3) + [HBM] * 3,
        out_specs=[HBM] * 3,
        out_shape=caches,
        scratch_shapes=state + [pltpu.VMEM((heads, rank), jnp.bfloat16), pltpu.SemaphoreType.DMA] + stores(late * LATE, 1),
        input_output_aliases={late + 4: 0, late + 5: 1, late + 6: 2},
        compiler_params=params,
        cost_estimate=pl.CostEstimate(flops=flops // req_local // PIECES, bytes_accessed=n * block * rank * 2, transcendentals=0),
        name="attend_last",
    )(lens, *rest, q_lat, q_rope, first_part, *outs)


def solution(mesh):
    seq_spec = P("dp", "x", None)
    req_spec = P(("dp", "x"), None, None)
    n = mesh.shape["x"]

    def local_step(c_raw, k_raw, norm_gain, rope_cos, rope_sin, seq_lens, q_lat, q_rope):
        q_rope = jnp.swapaxes(q_rope, 1, 2)
        landed, *rest = send(seq_lens, c_raw, jnp.swapaxes(k_raw, 1, 2), norm_gain, rope_cos.T, rope_sin.T, q_lat, q_rope, n)
        rest = [lax.ppermute(pieces, "x", [(i, move(i, j, n, 1)) for i in range(n)]) for j, pieces in zip(late_steps(n), rest)]
        c_cache, kr_cache, o_lat = attend(seq_lens, landed, rest, q_lat, q_rope, n, c_raw.shape[1])
        return c_cache, jnp.swapaxes(kr_cache, 1, 2), o_lat

    return jax.shard_map(local_step, mesh=mesh, in_specs=(seq_spec, seq_spec, P(None), P("x", None), P("x", None), P("dp"), req_spec, req_spec), out_specs=(req_spec, req_spec, req_spec), check_vma=False)
```

```python
import functools

import jax
import jax.numpy as jnp
from jax import lax
from jax.experimental import pallas as pl
from jax.experimental.pallas import tpu as pltpu
from jax.sharding import PartitionSpec as P

NORM_EPS = 1e-6
PIECES = 3
ROUNDS = 6
LOADS = 4
RING = 12
LATE = (3, 3, 1)
BATCH = 4
AHEAD = 3
STRIPE = 128
LANES, SUBLANES = 128, 16
VMEM_BYTES = 60 * 1024 * 1024
ATTEND_BYTES = 44 * 1024 * 1024
MESH = pl.DeviceIdType.MESH
HBM = pl.BlockSpec(memory_space=pltpu.HBM)
VMEM = pl.BlockSpec(memory_space=pltpu.VMEM)
SMEM = pl.BlockSpec(memory_space=pltpu.SMEM)


def move(me, j, n, way):
    chip, core = me // 2, me % 2
    far = j % 3
    last = j // (n - 2)
    hop = (1 - last) * (1 + 2 * far - 3 * (far // 2))
    other = (j // 3) % 2 * (1 - last) + last * (1 - j % (n - 2))
    return (chip + n // 2 + way * hop) % (n // 2) * 2 + (core + other) % 2


def peer(j, n):
    return move(lax.axis_index("x"), j, n, 1)


def late_pieces():
    return [(j, h) for j, count in enumerate(LATE) for h in range(PIECES - count, PIECES)]


def result_place(land_ref, m, n):
    return land_ref.at[land_ref.shape[0] - 1, move(lax.axis_index("x"), m // PIECES, n, -1), m % PIECES]


def rope_tiles(width, rows):
    for r in range(width // SUBLANES):
        for c in range(rows // LANES):
            yield (slice(r * SUBLANES, (r + 1) * SUBLANES), slice(c * LANES, (c + 1) * LANES),
                   slice(rows + c * SUBLANES, rows + (c + 1) * SUBLANES), slice(r * LANES, (r + 1) * LANES))


def clear(state):
    m_ref, l_ref, acc_ref = state
    m_ref[...] = jnp.full_like(m_ref, -1e30)
    l_ref[...] = jnp.zeros_like(l_ref)
    acc_ref[...] = jnp.zeros_like(acc_ref)


def fold(state, qa, qr, pieces, firsts, length, scale):
    m_ref, l_ref, acc_ref = state
    scores = []
    for first, (lat, kr) in zip(firsts, pieces):
        s = lax.dot_general(qa, lat, (((1,), (1,)), ((), ())), preferred_element_type=jnp.float32)
        s = s + lax.dot_general(qr, kr, (((0,), (0,)), ((), ())), preferred_element_type=jnp.float32)
        rows = lat.shape[0]
        pos = first + lax.broadcasted_iota(jnp.int32, (1, rows), 1)
        scores.append(jnp.where(pos < length, s * scale, -1e30))
    m_old = m_ref[...]
    m_new = m_old
    for s in scores:
        m_new = jnp.maximum(m_new, jnp.max(s, axis=-1, keepdims=True))
    alpha = jnp.exp(m_old - m_new)
    total, acc = l_ref[...] * alpha, acc_ref[...] * alpha
    for s, (lat, _) in zip(scores, pieces):
        p = jnp.exp(s - m_new)
        total = total + jnp.sum(p, axis=-1, keepdims=True)
        acc = acc + jnp.dot(p.astype(jnp.bfloat16), lat, preferred_element_type=jnp.float32)
    m_ref[...], l_ref[...], acc_ref[...] = m_new, total, acc


def send_kernel(n, req_local, scale, lens_ref, c_hbm, k_hbm, gain_ref, cos_ref, sin_ref, qa_ref, qr_ref, land_ref, *scratch):
    rest_refs, scratch = scratch[: len(LATE)], scratch[len(LATE) :]
    c_buf, k_buf, out_buf, c_sem, k_sem, send_sem, recv_sem, m_ref, l_ref, acc_ref, fold_buf, kr_buf, fold_sem, o_buf, o_sem = scratch
    me = lax.axis_index("x")
    rounds = req_local * PIECES
    steps = rounds * n
    early = (rounds - PIECES) * n
    depth = out_buf.shape[0]
    rows, rank = c_buf.shape[1:]
    width = k_buf.shape[1]

    def load(t):
        req = peer(t % n, n) * req_local + t // n // PIECES
        first = pl.multiple_of(t // n % PIECES * rows, rows)
        slot = t % LOADS
        return (pltpu.make_async_copy(c_hbm.at[req, pl.ds(first, rows), :], c_buf.at[slot], c_sem.at[slot]),
                pltpu.make_async_copy(k_hbm.at[req, :, pl.ds(first, rows)], k_buf.at[slot], k_sem.at[slot]))

    def landing(t):
        return land_ref.at[t // n // PIECES, me, t // n % PIECES]

    def remote(t):
        slot = t % depth
        return pltpu.make_async_remote_copy(
            src_ref=out_buf.at[slot], dst_ref=landing(t), send_sem=send_sem.at[slot],
            recv_sem=recv_sem.at[t // n * n + me], device_id={"x": peer(t % n, n)}, device_id_type=MESH)

    def own(t):
        return pltpu.make_async_copy(out_buf.at[t % depth], landing(t), send_sem.at[t % depth])

    def keep(t, j, h):
        return pltpu.make_async_copy(out_buf.at[t % depth], rest_refs[j].at[h - PIECES + LATE[j]], send_sem.at[t % depth])

    def is_kept(t):
        return functools.reduce(jnp.logical_or, [t == early + h * n + j for j, h in late_pieces()])

    def on_kind(t, act_remote, act_local):
        is_own = t % n == n - 1

        for j, h in late_pieces():
            @pl.when(t == early + h * n + j)
            def _():
                act_local(keep(t, j, h))

        @pl.when(is_own)
        def _():
            act_local(own(t))

        @pl.when(jnp.logical_not(jnp.logical_or(is_own, is_kept(t))))
        def _():
            act_remote(remote(t))

    def start(t):
        on_kind(t, lambda c: c.start(), lambda c: c.start())

    def sent(t):
        on_kind(t, lambda c: c.wait_send(), lambda c: c.wait())

    def pack(t):
        for c in load(t):
            c.wait()
        slot, out = t % LOADS, t % depth
        first = t // n % PIECES * rows
        left = lens_ref[peer(t % n, n) * req_local + t // n // PIECES] - me * (rows * PIECES) - first
        gain = gain_ref[...].astype(jnp.float32)

        @pl.loop(0, rows, step=STRIPE)
        def _(r):
            r = pl.multiple_of(r, STRIPE)
            lat = c_buf[slot, pl.ds(r, STRIPE), :].astype(jnp.float32)
            inv = lax.rsqrt(jnp.mean(lat * lat, axis=-1, keepdims=True) + NORM_EPS)
            valid = r + lax.broadcasted_iota(jnp.int32, (STRIPE, 1), 0) < left
            out_buf[out, pl.ds(r, STRIPE), :] = jnp.where(valid, lat * inv * gain, 0.0).astype(jnp.bfloat16)

        key = k_buf[slot].astype(jnp.float32)
        half = width // 2
        lo, hi = key[:half], key[half:]
        first = pl.multiple_of(first, LANES)
        cos, sin = cos_ref[:, pl.ds(first, rows)], sin_ref[:, pl.ds(first, rows)]
        valid = lax.broadcasted_iota(jnp.int32, (1, rows), 1) < left
        rotated = (jnp.where(valid, lo * cos - hi * sin, 0.0).astype(jnp.bfloat16),
                   jnp.where(valid, hi * cos + lo * sin, 0.0).astype(jnp.bfloat16))
        for kr_rows, kr_cols, to_rows, to_cols in rope_tiles(width, rows):
            part, at = kr_rows.start // half, kr_rows.start % half
            out_buf[out, to_rows, to_cols] = rotated[part][at : at + SUBLANES, kr_cols]

    barrier = pltpu.get_barrier_semaphore()
    for j in range(n - 1):
        pl.semaphore_signal(barrier, inc=1, device_id={"x": peer(j, n)}, device_id_type=MESH)
    for t in range(LOADS):
        for c in load(t):
            c.start()
    pack(0)
    for c in load(LOADS):
        c.start()
    pl.semaphore_wait(barrier, n - 1)

    state = (m_ref, l_ref, acc_ref)
    per_req = PIECES * n
    folds = (req_local - 1) * per_req
    lag = depth + n

    def received(a):
        src = peer(a % n, n)
        piece = land_ref.at[a // per_req, src, a // n % PIECES]
        pltpu.make_async_remote_copy(
            src_ref=piece, dst_ref=piece, send_sem=send_sem.at[0], recv_sem=recv_sem.at[a // n * n + src],
            device_id={"x": src}, device_id_type=MESH).wait_recv()

    def result(m):
        return pltpu.make_async_copy(o_buf.at[m], result_place(land_ref, m, n).at[pl.ds(0, o_buf.shape[1]), :], o_sem.at[m])

    def fetch(a):
        return pltpu.make_async_copy(land_ref.at[a // per_req, peer(a % n, n), a // n % PIECES], fold_buf.at[a % (AHEAD + 1)], fold_sem.at[a % (AHEAD + 1)])

    @pl.loop(1, folds + lag)
    def _(t):
        @pl.when(t >= depth)
        def _():
            sent(t - depth)

        @pl.when(t < steps)
        def _():
            pack(t)

            @pl.when(t + LOADS < steps)
            def _():
                for c in load(t + LOADS):
                    c.start()

        @pl.when(t <= steps)
        def _():
            start(t - 1)

        arriving = t - lag + AHEAD

        @pl.when(jnp.logical_and(arriving >= 0, arriving < folds))
        def _():
            @pl.when(arriving % n < n - 1)
            def _():
                received(arriving)

            fetch(arriving).start()

        a = t - lag

        @pl.when(a >= 0)
        def _():
            m, src, slot = a // per_req, peer(a % n, n), a % (AHEAD + 1)

            @pl.when(a % per_req == 0)
            def _():
                clear(state)

            fetch(a).wait()
            for kr_rows, kr_cols, from_rows, from_cols in rope_tiles(width, rows):
                kr_buf[kr_rows, kr_cols] = fold_buf[slot, from_rows, from_cols]
            first = (src * PIECES + a // n % PIECES) * rows
            fold(state, qa_ref[m], qr_ref[m], [(fold_buf[slot, :rows, :], kr_buf[...])], [first], lens_ref[me * req_local + m], scale)

            @pl.when(a % per_req == per_req - 1)
            def _():
                o_buf[m] = (acc_ref[...] / l_ref[...]).astype(jnp.bfloat16)
                result(m).start()

    @pl.loop(folds + lag - depth, steps)
    def _(t):
        sent(t)

    @pl.loop(folds, steps)
    def _(a):
        @pl.when(jnp.logical_and(a % n < n - 1, jnp.logical_not(is_kept(a))))
        def _():
            received(a)

    for m in range(req_local - 1):
        result(m).wait()


def send(lens, c_raw, k_raw, gain, cos, sin, q_lat, q_rope, n):
    req_local, heads, _ = q_lat.shape
    requests, block, rank = c_raw.shape
    width = k_raw.shape[1]
    rows = block // PIECES
    total = rows + rows * width // rank
    depth = ROUNDS * n
    return pl.pallas_call(
        functools.partial(send_kernel, n, req_local, (rank + width) ** -0.5),
        in_specs=[SMEM, HBM, HBM] + [VMEM] * 5,
        out_specs=[HBM] * (1 + len(LATE)),
        out_shape=[jax.ShapeDtypeStruct((req_local, n, PIECES, total, rank), jnp.bfloat16)]
        + [jax.ShapeDtypeStruct((count, total, rank), jnp.bfloat16) for count in LATE],
        scratch_shapes=[
            pltpu.VMEM((LOADS, rows, rank), jnp.bfloat16),
            pltpu.VMEM((LOADS, width, rows), jnp.bfloat16),
            pltpu.VMEM((depth, total, rank), jnp.bfloat16),
            pltpu.SemaphoreType.DMA((LOADS,)),
            pltpu.SemaphoreType.DMA((LOADS,)),
            pltpu.SemaphoreType.DMA((depth,)),
            pltpu.SemaphoreType.DMA((req_local * PIECES * n,)),
            pltpu.VMEM((heads, 1), jnp.float32),
            pltpu.VMEM((heads, 1), jnp.float32),
            pltpu.VMEM((heads, rank), jnp.float32),
            pltpu.VMEM((AHEAD + 1, total, rank), jnp.bfloat16),
            pltpu.VMEM((width, rows), jnp.bfloat16),
            pltpu.SemaphoreType.DMA((AHEAD + 1,)),
            pltpu.VMEM((req_local - 1, heads, rank), jnp.bfloat16),
            pltpu.SemaphoreType.DMA((req_local - 1,)),
        ],
        compiler_params=pltpu.CompilerParams(vmem_limit_bytes=VMEM_BYTES, collective_id=0, has_side_effects=True),
        cost_estimate=pl.CostEstimate(flops=requests * block * rank * 100, bytes_accessed=requests * block * rank * 4, transcendentals=0),
        name="send",
    )(lens, c_raw, k_raw, gain, cos, sin, q_lat, q_rope)


def stream(steps, place, first_piece, pieces, scale, length, land_ref, queries, c_out, kr_out, state, zero_c, zero_k, ring, ahead):
    buf, in_sem, kr_buf, c_sem, k_sem = ring
    depth = buf.shape[0]
    rank = buf.shape[3]
    width = kr_buf.shape[1]
    rows = kr_buf.shape[2] // pieces

    def first(t):
        return pl.multiple_of((place(t)[1] * PIECES + first_piece) * rows, rows)

    def used(t):
        return first(t) < length(place(t)[0])

    def load(t):
        req, src = place(t)
        return pltpu.make_async_copy(land_ref.at[req, src, pl.ds(first_piece, pieces)], buf.at[t % depth], in_sem.at[t % depth])

    def writes(t, c_of, kr):
        slot, req, at = t % depth, place(t)[0], first(t)
        return [pltpu.make_async_copy(c_of(h), c_out.at[req, pl.ds(at + h * rows, rows), :], c_sem.at[slot, h]) for h in range(pieces)] + [
            pltpu.make_async_copy(kr, kr_out.at[req, :, pl.ds(at, pieces * rows)], k_sem.at[slot])]

    def stores(t):
        return writes(t, lambda h: buf.at[t % depth, h, pl.ds(0, rows), :], kr_buf.at[t % depth])

    def blanks(t):
        return writes(t, lambda h: zero_c, zero_k.at[:, pl.ds(0, pieces * rows)])

    def fetch(t):
        @pl.when(used(t))
        def _():
            load(t).start()

    def work(t):
        slot = t % depth
        load(t).wait()
        for h in range(pieces):
            for kr_rows, kr_cols, from_rows, from_cols in rope_tiles(width, rows):
                cols = slice(h * rows + kr_cols.start, h * rows + kr_cols.stop)
                kr_buf[slot, kr_rows, cols] = buf[slot, h, from_rows, from_cols]
        for c in stores(t):
            c.start()
        if queries is not None:
            qa, qr = queries()
            blocks = [(buf[slot, h, :rows, :], kr_buf[slot, :, h * rows : (h + 1) * rows]) for h in range(pieces)]
            fold(state, qa, qr, blocks, [first(t) + h * rows for h in range(pieces)], length(place(t)[0]), scale)

    def body(t):
        @pl.when(used(t))
        def _():
            work(t)

        @pl.when(jnp.logical_not(used(t)))
        def _():
            for c in blanks(t):
                c.start()

        @pl.when(t + ahead < steps)
        def _():
            @pl.when(t + ahead >= depth)
            def _():
                for c in stores(t + ahead - depth):
                    c.wait()

            fetch(t + ahead)

    def prologue():
        for t in range(min(ahead, steps)):
            fetch(t)

    def drain():
        @pl.loop(max(steps - depth, 0), steps)
        def _(t):
            for c in stores(t):
                c.wait()

    return steps, prologue, body, drain


def first_kernel(n, req_local, scale, lens_ref, land_ref, qa_ref, qr_ref, c_out, kr_out, o_out, part_out,
                 m_ref, l_ref, acc_ref, part_ref, part_sem, zero_c, zero_k, o_buf, o_in_sem, o_out_sem, *rings):
    length = lambda m: lens_ref[lax.axis_index("x") * req_local + m]
    state = (m_ref, l_ref, acc_ref)
    last = req_local - 1
    rank = acc_ref.shape[1]
    me = lax.axis_index("x")
    across = len(LATE) - 1
    queries = lambda: (qa_ref[last], qr_ref[last])
    common = (scale, length, land_ref)
    outs = (c_out, kr_out, state, zero_c, zero_k)
    main = stream(last * n, lambda t: (t // n, t % n), 0, PIECES, *common, None, *outs, rings[:5], RING // 2)
    front = stream(1, lambda t: (last, move(me, across, n, -1)), 0, PIECES - LATE[across], *common, queries, *outs, rings[5:10], 1)
    back = stream(n - len(LATE), lambda t: (last, move(me, len(LATE) + t, n, -1)), 0, PIECES, *common, queries, *outs, rings[10:], n - len(LATE))
    results = [(pltpu.make_async_copy(result_place(land_ref, m, n).at[pl.ds(0, o_buf.shape[1]), :], o_buf.at[m], o_in_sem.at[m]),
                pltpu.make_async_copy(o_buf.at[m], o_out.at[m], o_out_sem.at[m])) for m in range(last)]

    for part in (front, back, main):
        part[1]()
    for take, _ in results:
        take.start()
    zero_c[...] = jnp.zeros_like(zero_c)
    zero_k[...] = jnp.zeros_like(zero_k)
    clear(state)
    steps = main[0]

    @pl.loop(0, steps)
    def _(t):
        main[2](t)

        every = steps // back[0]

        @pl.when(t % every == 0)
        def _():
            back[2](t // every)

        @pl.when(t == every // 2)
        def _():
            front[2](0)

    for take, give in results:
        take.wait()
        give.start()
    part_ref[:, :rank] = acc_ref[...]
    part_ref[:, rank : rank + LANES] = jnp.broadcast_to(m_ref[...], (part_ref.shape[0], LANES))
    part_ref[:, rank + LANES :] = jnp.broadcast_to(l_ref[...], (part_ref.shape[0], LANES))
    copy = pltpu.make_async_copy(part_ref, part_out, part_sem)
    copy.start()
    copy.wait()
    for part in (main, front, back):
        part[3]()
    for _, give in results:
        give.wait()


def last_kernel(n, req_local, scale, lens_ref, *refs):
    land_refs, refs = refs[: len(LATE)], refs[len(LATE) :]
    qa_ref, qr_ref, part_ref, c_old, kr_old, o_old, c_out, kr_out, o_out, *refs = refs
    m_ref, l_ref, acc_ref, o_buf, o_sem, kr_buf, c_sem, k_sem = refs
    last = req_local - 1
    length = lens_ref[lax.axis_index("x") * req_local + last]
    state = (m_ref, l_ref, acc_ref)
    rank = acc_ref.shape[1]
    width = kr_buf.shape[1]
    rows = kr_buf.shape[2]
    pieces = late_pieces()
    firsts = [pl.multiple_of((move(lax.axis_index("x"), j, n, -1) * PIECES + h) * rows, rows) for j, h in pieces]
    pieces = [(j, h - PIECES + LATE[j]) for j, h in pieces]
    clear(state)
    stores = []
    for at in range(0, len(pieces), BATCH):
        batch = range(at, min(at + BATCH, len(pieces)))
        for i in batch:
            (k, h), first = pieces[i], firsts[i]
            stores.append(pltpu.make_async_copy(land_refs[k].at[h, pl.ds(0, rows), :], c_out.at[last, pl.ds(first, rows), :], c_sem.at[i, 0]))
            stores[-1].start()
            for kr_rows, kr_cols, from_rows, from_cols in rope_tiles(width, rows):
                kr_buf[i, kr_rows, kr_cols] = land_refs[k][h, from_rows, from_cols]
            stores.append(pltpu.make_async_copy(kr_buf.at[i], kr_out.at[last, :, pl.ds(first, rows)], k_sem.at[i]))
            stores[-1].start()

        @pl.when(functools.reduce(jnp.minimum, [firsts[i] for i in batch]) < length)
        def _():
            blocks = [(land_refs[pieces[i][0]][pieces[i][1], :rows, :], kr_buf[i]) for i in batch]
            fold(state, qa_ref[last], qr_ref[last], blocks, [firsts[i] for i in batch], length, scale)

    m_part, l_part, acc_part = part_ref[:, rank : rank + 1], part_ref[:, rank + LANES : rank + LANES + 1], part_ref[:, :rank]
    m_new = jnp.maximum(m_ref[...], m_part)
    here, there = jnp.exp(m_ref[...] - m_new), jnp.exp(m_part - m_new)
    total = l_ref[...] * here + l_part * there
    o_buf[...] = ((acc_ref[...] * here + acc_part * there) / total).astype(jnp.bfloat16)
    copy = pltpu.make_async_copy(o_buf, o_out.at[last], o_sem)
    copy.start()
    for c in stores + [copy]:
        c.wait()


def attend(lens, landed, rest, q_lat, q_rope, n, block):
    req_local, heads, rank = q_lat.shape
    width = q_rope.shape[1]
    rows = block // PIECES
    total = rest[0].shape[1]
    late = len(late_pieces())
    scale = (rank + width) ** -0.5
    caches = [jax.ShapeDtypeStruct((req_local, n * block, rank), jnp.bfloat16),
              jax.ShapeDtypeStruct((req_local, width, n * block), jnp.bfloat16),
              jax.ShapeDtypeStruct((req_local, heads, rank), jnp.bfloat16)]
    part = jax.ShapeDtypeStruct((heads, rank + 2 * LANES), jnp.float32)
    state = [pltpu.VMEM((heads, 1), jnp.float32), pltpu.VMEM((heads, 1), jnp.float32), pltpu.VMEM((heads, rank), jnp.float32)]

    def stores(depth, pieces):
        return [pltpu.VMEM((depth, width, pieces * rows), jnp.bfloat16), pltpu.SemaphoreType.DMA((depth, pieces)), pltpu.SemaphoreType.DMA((depth,))]

    def ring(depth, pieces):
        return [pltpu.VMEM((depth, pieces, total, rank), jnp.bfloat16), pltpu.SemaphoreType.DMA((depth,))] + stores(depth, pieces)

    params = pltpu.CompilerParams(vmem_limit_bytes=ATTEND_BYTES)
    flops = 2 * req_local * n * block * heads * rank
    *outs, first_part = pl.pallas_call(
        functools.partial(first_kernel, n, req_local, scale),
        in_specs=[SMEM, HBM, VMEM, VMEM],
        out_specs=[HBM] * 4,
        out_shape=caches + [part],
        scratch_shapes=state + [pltpu.VMEM(part.shape, part.dtype), pltpu.SemaphoreType.DMA,
                                pltpu.VMEM((rows, rank), jnp.bfloat16), pltpu.VMEM((width, block), jnp.bfloat16),
                                pltpu.VMEM((req_local - 1, heads, rank), jnp.bfloat16),
                                pltpu.SemaphoreType.DMA((req_local - 1,)), pltpu.SemaphoreType.DMA((req_local - 1,))]
        + ring(RING, PIECES) + ring(1, PIECES - LATE[-1]) + ring(n - len(LATE), PIECES),
        compiler_params=params,
        cost_estimate=pl.CostEstimate(flops=flops, bytes_accessed=req_local * n * block * rank * 4, transcendentals=0),
        name="attend_first",
    )(lens, landed, q_lat, q_rope)
    return pl.pallas_call(
        functools.partial(last_kernel, n, req_local, scale),
        in_specs=[SMEM] + [VMEM] * (len(LATE) + 3) + [HBM] * 3,
        out_specs=[HBM] * 3,
        out_shape=caches,
        scratch_shapes=state + [pltpu.VMEM((heads, rank), jnp.bfloat16), pltpu.SemaphoreType.DMA] + stores(late, 1),
        input_output_aliases={len(LATE) + 4 + k: k for k in range(3)},
        compiler_params=params,
        cost_estimate=pl.CostEstimate(flops=flops // req_local // PIECES, bytes_accessed=n * block * rank * 2, transcendentals=0),
        name="attend_last",
    )(lens, *rest, q_lat, q_rope, first_part, *outs)


def solution(mesh):
    seq_spec = P("dp", "x", None)
    req_spec = P(("dp", "x"), None, None)
    n = mesh.shape["x"]

    def local_step(c_raw, k_raw, norm_gain, rope_cos, rope_sin, seq_lens, q_lat, q_rope):
        q_rope = jnp.swapaxes(q_rope, 1, 2)
        landed, *rest = send(seq_lens, c_raw, jnp.swapaxes(k_raw, 1, 2), norm_gain, rope_cos.T, rope_sin.T, q_lat, q_rope, n)
        rest = [lax.ppermute(pieces, "x", [(i, move(i, j, n, 1)) for i in range(n)]) for j, pieces in enumerate(rest)]
        c_cache, kr_cache, o_lat = attend(seq_lens, landed, rest, q_lat, q_rope, n, c_raw.shape[1])
        return c_cache, jnp.swapaxes(kr_cache, 1, 2), o_lat

    return jax.shard_map(local_step, mesh=mesh, in_specs=(seq_spec, seq_spec, P(None), P("x", None), P("x", None), P("dp"), req_spec, req_spec), out_specs=(req_spec, req_spec, req_spec), check_vma=False)
```

```python
import functools

import jax
import jax.numpy as jnp
from jax import lax
from jax.experimental import pallas as pl
from jax.experimental.pallas import tpu as pltpu
from jax.sharding import PartitionSpec as P

NORM_EPS = 1e-6
PIECES = 3
ROUNDS = 6
LOADS = 4
RING = 12
LATE = (3, 3, 1)
BATCH = 7
AHEAD = 3
STRIPE = 128
LANES, SUBLANES = 128, 16
VMEM_BYTES = 60 * 1024 * 1024
ATTEND_BYTES = 44 * 1024 * 1024
MESH = pl.DeviceIdType.MESH
HBM = pl.BlockSpec(memory_space=pltpu.HBM)
VMEM = pl.BlockSpec(memory_space=pltpu.VMEM)
SMEM = pl.BlockSpec(memory_space=pltpu.SMEM)


def move(me, j, n, way):
    chip, core = me // 2, me % 2
    far = j % 3
    last = j // (n - 2)
    other = (j // 3) % 2 * (1 - last) + last * (1 - j % (n - 2))
    there = (core + other) % 2
    sender = core if way == 1 else there
    hop = (1 - last) * (1 + 2 * far - 3 * (far // 2)) * (1 - 2 * sender)
    return (chip + n // 2 + way * hop) % (n // 2) * 2 + there


def peer(j, n):
    return move(lax.axis_index("x"), j, n, 1)


def late_pieces():
    return [(j, h) for j, count in enumerate(LATE) for h in range(PIECES - count, PIECES)]


def result_place(land_ref, m, n):
    return land_ref.at[land_ref.shape[0] - 1, move(lax.axis_index("x"), m // PIECES, n, -1), m % PIECES]


def rope_tiles(width, rows):
    for r in range(width // SUBLANES):
        for c in range(rows // LANES):
            yield (slice(r * SUBLANES, (r + 1) * SUBLANES), slice(c * LANES, (c + 1) * LANES),
                   slice(rows + c * SUBLANES, rows + (c + 1) * SUBLANES), slice(r * LANES, (r + 1) * LANES))


def clear(state):
    m_ref, l_ref, acc_ref = state
    m_ref[...] = jnp.full_like(m_ref, -1e30)
    l_ref[...] = jnp.zeros_like(l_ref)
    acc_ref[...] = jnp.zeros_like(acc_ref)


def fold(state, qa, qr, pieces, firsts, length, scale):
    m_ref, l_ref, acc_ref = state
    scores = []
    for first, (lat, kr) in zip(firsts, pieces):
        s = lax.dot_general(qa, lat, (((1,), (1,)), ((), ())), preferred_element_type=jnp.float32)
        s = s + lax.dot_general(qr, kr, (((0,), (0,)), ((), ())), preferred_element_type=jnp.float32)
        rows = lat.shape[0]
        pos = first + lax.broadcasted_iota(jnp.int32, (1, rows), 1)
        scores.append(jnp.where(pos < length, s * scale, -1e30))
    m_old = m_ref[...]
    m_new = m_old
    for s in scores:
        m_new = jnp.maximum(m_new, jnp.max(s, axis=-1, keepdims=True))
    alpha = jnp.exp(m_old - m_new)
    total, acc = l_ref[...] * alpha, acc_ref[...] * alpha
    for s, (lat, _) in zip(scores, pieces):
        p = jnp.exp(s - m_new)
        total = total + jnp.sum(p, axis=-1, keepdims=True)
        acc = acc + jnp.dot(p.astype(jnp.bfloat16), lat, preferred_element_type=jnp.float32)
    m_ref[...], l_ref[...], acc_ref[...] = m_new, total, acc


def send_kernel(n, req_local, scale, lens_ref, c_hbm, k_hbm, gain_ref, cos_ref, sin_ref, qa_ref, qr_ref, land_ref, *scratch):
    rest_refs, scratch = scratch[: len(LATE)], scratch[len(LATE) :]
    c_buf, k_buf, out_buf, c_sem, k_sem, send_sem, recv_sem, m_ref, l_ref, acc_ref, fold_buf, kr_buf, fold_sem, o_buf, o_sem = scratch
    me = lax.axis_index("x")
    rounds = req_local * PIECES
    steps = rounds * n
    early = (rounds - PIECES) * n
    depth = out_buf.shape[0]
    rows, rank = c_buf.shape[1:]
    width = k_buf.shape[1]

    def load(t):
        req = peer(t % n, n) * req_local + t // n // PIECES
        first = pl.multiple_of(t // n % PIECES * rows, rows)
        slot = t % LOADS
        return (pltpu.make_async_copy(c_hbm.at[req, pl.ds(first, rows), :], c_buf.at[slot], c_sem.at[slot]),
                pltpu.make_async_copy(k_hbm.at[req, :, pl.ds(first, rows)], k_buf.at[slot], k_sem.at[slot]))

    def landing(t):
        return land_ref.at[t // n // PIECES, me, t // n % PIECES]

    def remote(t):
        slot = t % depth
        return pltpu.make_async_remote_copy(
            src_ref=out_buf.at[slot], dst_ref=landing(t), send_sem=send_sem.at[slot],
            recv_sem=recv_sem.at[t // n * n + me], device_id={"x": peer(t % n, n)}, device_id_type=MESH)

    def own(t):
        return pltpu.make_async_copy(out_buf.at[t % depth], landing(t), send_sem.at[t % depth])

    def keep(t, j, h):
        return pltpu.make_async_copy(out_buf.at[t % depth], rest_refs[j].at[h - PIECES + LATE[j]], send_sem.at[t % depth])

    def is_kept(t):
        return functools.reduce(jnp.logical_or, [t == early + h * n + j for j, h in late_pieces()])

    def on_kind(t, act_remote, act_local):
        is_own = t % n == n - 1

        for j, h in late_pieces():
            @pl.when(t == early + h * n + j)
            def _():
                act_local(keep(t, j, h))

        @pl.when(is_own)
        def _():
            act_local(own(t))

        @pl.when(jnp.logical_not(jnp.logical_or(is_own, is_kept(t))))
        def _():
            act_remote(remote(t))

    def start(t):
        on_kind(t, lambda c: c.start(), lambda c: c.start())

    def sent(t):
        on_kind(t, lambda c: c.wait_send(), lambda c: c.wait())

    def pack(t):
        for c in load(t):
            c.wait()
        slot, out = t % LOADS, t % depth
        first = t // n % PIECES * rows
        left = lens_ref[peer(t % n, n) * req_local + t // n // PIECES] - me * (rows * PIECES) - first
        gain = gain_ref[...].astype(jnp.float32)

        @pl.loop(0, rows, step=STRIPE)
        def _(r):
            r = pl.multiple_of(r, STRIPE)
            lat = c_buf[slot, pl.ds(r, STRIPE), :].astype(jnp.float32)
            inv = lax.rsqrt(jnp.mean(lat * lat, axis=-1, keepdims=True) + NORM_EPS)
            valid = r + lax.broadcasted_iota(jnp.int32, (STRIPE, 1), 0) < left
            out_buf[out, pl.ds(r, STRIPE), :] = jnp.where(valid, lat * inv * gain, 0.0).astype(jnp.bfloat16)

        key = k_buf[slot].astype(jnp.float32)
        half = width // 2
        lo, hi = key[:half], key[half:]
        first = pl.multiple_of(first, LANES)
        cos, sin = cos_ref[:, pl.ds(first, rows)], sin_ref[:, pl.ds(first, rows)]
        valid = lax.broadcasted_iota(jnp.int32, (1, rows), 1) < left
        rotated = (jnp.where(valid, lo * cos - hi * sin, 0.0).astype(jnp.bfloat16),
                   jnp.where(valid, hi * cos + lo * sin, 0.0).astype(jnp.bfloat16))
        for kr_rows, kr_cols, to_rows, to_cols in rope_tiles(width, rows):
            part, at = kr_rows.start // half, kr_rows.start % half
            out_buf[out, to_rows, to_cols] = rotated[part][at : at + SUBLANES, kr_cols]

    barrier = pltpu.get_barrier_semaphore()
    for j in range(n - 1):
        pl.semaphore_signal(barrier, inc=1, device_id={"x": peer(j, n)}, device_id_type=MESH)
    for t in range(LOADS):
        for c in load(t):
            c.start()
    pack(0)
    for c in load(LOADS):
        c.start()
    pl.semaphore_wait(barrier, n - 1)

    state = (m_ref, l_ref, acc_ref)
    per_req = PIECES * n
    folds = (req_local - 1) * per_req
    lag = depth + n

    def received(a):
        src = peer(a % n, n)
        piece = land_ref.at[a // per_req, src, a // n % PIECES]
        pltpu.make_async_remote_copy(
            src_ref=piece, dst_ref=piece, send_sem=send_sem.at[0], recv_sem=recv_sem.at[a // n * n + src],
            device_id={"x": src}, device_id_type=MESH).wait_recv()

    def result(m):
        return pltpu.make_async_copy(o_buf.at[m], result_place(land_ref, m, n).at[pl.ds(0, o_buf.shape[1]), :], o_sem.at[m])

    def fetch(a):
        return pltpu.make_async_copy(land_ref.at[a // per_req, peer(a % n, n), a // n % PIECES], fold_buf.at[a % (AHEAD + 1)], fold_sem.at[a % (AHEAD + 1)])

    @pl.loop(1, folds + lag)
    def _(t):
        @pl.when(t >= depth)
        def _():
            sent(t - depth)

        @pl.when(t < steps)
        def _():
            pack(t)

            @pl.when(t + LOADS < steps)
            def _():
                for c in load(t + LOADS):
                    c.start()

        @pl.when(t <= steps)
        def _():
            start(t - 1)

        arriving = t - lag + AHEAD

        @pl.when(jnp.logical_and(arriving >= 0, arriving < folds))
        def _():
            @pl.when(arriving % n < n - 1)
            def _():
                received(arriving)

            fetch(arriving).start()

        a = t - lag

        @pl.when(a >= 0)
        def _():
            m, src, slot = a // per_req, peer(a % n, n), a % (AHEAD + 1)

            @pl.when(a % per_req == 0)
            def _():
                clear(state)

            fetch(a).wait()
            for kr_rows, kr_cols, from_rows, from_cols in rope_tiles(width, rows):
                kr_buf[kr_rows, kr_cols] = fold_buf[slot, from_rows, from_cols]
            first = (src * PIECES + a // n % PIECES) * rows
            fold(state, qa_ref[m], qr_ref[m], [(fold_buf[slot, :rows, :], kr_buf[...])], [first], lens_ref[me * req_local + m], scale)

            @pl.when(a % per_req == per_req - 1)
            def _():
                o_buf[m] = (acc_ref[...] / l_ref[...]).astype(jnp.bfloat16)
                result(m).start()

    @pl.loop(folds + lag - depth, steps)
    def _(t):
        sent(t)

    @pl.loop(folds, steps)
    def _(a):
        @pl.when(jnp.logical_and(a % n < n - 1, jnp.logical_not(is_kept(a))))
        def _():
            received(a)

    for m in range(req_local - 1):
        result(m).wait()


def send(lens, c_raw, k_raw, gain, cos, sin, q_lat, q_rope, n):
    req_local, heads, _ = q_lat.shape
    requests, block, rank = c_raw.shape
    width = k_raw.shape[1]
    rows = block // PIECES
    total = rows + rows * width // rank
    depth = ROUNDS * n
    return pl.pallas_call(
        functools.partial(send_kernel, n, req_local, (rank + width) ** -0.5),
        in_specs=[SMEM, HBM, HBM] + [VMEM] * 5,
        out_specs=[HBM] * (1 + len(LATE)),
        out_shape=[jax.ShapeDtypeStruct((req_local, n, PIECES, total, rank), jnp.bfloat16)]
        + [jax.ShapeDtypeStruct((count, total, rank), jnp.bfloat16) for count in LATE],
        scratch_shapes=[
            pltpu.VMEM((LOADS, rows, rank), jnp.bfloat16),
            pltpu.VMEM((LOADS, width, rows), jnp.bfloat16),
            pltpu.VMEM((depth, total, rank), jnp.bfloat16),
            pltpu.SemaphoreType.DMA((LOADS,)),
            pltpu.SemaphoreType.DMA((LOADS,)),
            pltpu.SemaphoreType.DMA((depth,)),
            pltpu.SemaphoreType.DMA((req_local * PIECES * n,)),
            pltpu.VMEM((heads, 1), jnp.float32),
            pltpu.VMEM((heads, 1), jnp.float32),
            pltpu.VMEM((heads, rank), jnp.float32),
            pltpu.VMEM((AHEAD + 1, total, rank), jnp.bfloat16),
            pltpu.VMEM((width, rows), jnp.bfloat16),
            pltpu.SemaphoreType.DMA((AHEAD + 1,)),
            pltpu.VMEM((req_local - 1, heads, rank), jnp.bfloat16),
            pltpu.SemaphoreType.DMA((req_local - 1,)),
        ],
        compiler_params=pltpu.CompilerParams(vmem_limit_bytes=VMEM_BYTES, collective_id=0, has_side_effects=True),
        cost_estimate=pl.CostEstimate(flops=requests * block * rank * 100, bytes_accessed=requests * block * rank * 4, transcendentals=0),
        name="send",
    )(lens, c_raw, k_raw, gain, cos, sin, q_lat, q_rope)


def stream(steps, place, first_piece, pieces, scale, length, land_ref, queries, c_out, kr_out, state, zero_c, zero_k, ring, ahead):
    buf, in_sem, kr_buf, c_sem, k_sem = ring
    depth = buf.shape[0]
    rank = buf.shape[3]
    width = kr_buf.shape[1]
    rows = kr_buf.shape[2] // pieces

    def first(t):
        return pl.multiple_of((place(t)[1] * PIECES + first_piece) * rows, rows)

    def used(t):
        return first(t) < length(place(t)[0])

    def load(t):
        req, src = place(t)
        return pltpu.make_async_copy(land_ref.at[req, src, pl.ds(first_piece, pieces)], buf.at[t % depth], in_sem.at[t % depth])

    def writes(t, c_of, kr):
        slot, req, at = t % depth, place(t)[0], first(t)
        return [pltpu.make_async_copy(c_of(h), c_out.at[req, pl.ds(at + h * rows, rows), :], c_sem.at[slot, h]) for h in range(pieces)] + [
            pltpu.make_async_copy(kr, kr_out.at[req, :, pl.ds(at, pieces * rows)], k_sem.at[slot])]

    def stores(t):
        return writes(t, lambda h: buf.at[t % depth, h, pl.ds(0, rows), :], kr_buf.at[t % depth])

    def blanks(t):
        return writes(t, lambda h: zero_c, zero_k.at[:, pl.ds(0, pieces * rows)])

    def fetch(t):
        @pl.when(used(t))
        def _():
            load(t).start()

    def work(t):
        slot = t % depth
        load(t).wait()
        for h in range(pieces):
            for kr_rows, kr_cols, from_rows, from_cols in rope_tiles(width, rows):
                cols = slice(h * rows + kr_cols.start, h * rows + kr_cols.stop)
                kr_buf[slot, kr_rows, cols] = buf[slot, h, from_rows, from_cols]
        for c in stores(t):
            c.start()
        if queries is not None:
            qa, qr = queries()
            blocks = [(buf[slot, h, :rows, :], kr_buf[slot, :, h * rows : (h + 1) * rows]) for h in range(pieces)]
            fold(state, qa, qr, blocks, [first(t) + h * rows for h in range(pieces)], length(place(t)[0]), scale)

    def body(t):
        @pl.when(used(t))
        def _():
            work(t)

        @pl.when(jnp.logical_not(used(t)))
        def _():
            for c in blanks(t):
                c.start()

        @pl.when(t + ahead < steps)
        def _():
            @pl.when(t + ahead >= depth)
            def _():
                for c in stores(t + ahead - depth):
                    c.wait()

            fetch(t + ahead)

    def prologue():
        for t in range(min(ahead, steps)):
            fetch(t)

    def drain():
        @pl.loop(max(steps - depth, 0), steps)
        def _(t):
            for c in stores(t):
                c.wait()

    return steps, prologue, body, drain


def first_kernel(n, req_local, scale, lens_ref, land_ref, qa_ref, qr_ref, c_out, kr_out, o_out, part_out,
                 m_ref, l_ref, acc_ref, part_ref, part_sem, zero_c, zero_k, o_buf, o_in_sem, o_out_sem, *rings):
    length = lambda m: lens_ref[lax.axis_index("x") * req_local + m]
    state = (m_ref, l_ref, acc_ref)
    last = req_local - 1
    rank = acc_ref.shape[1]
    me = lax.axis_index("x")
    across = len(LATE) - 1
    queries = lambda: (qa_ref[last], qr_ref[last])
    common = (scale, length, land_ref)
    outs = (c_out, kr_out, state, zero_c, zero_k)
    main = stream(last * n, lambda t: (t // n, t % n), 0, PIECES, *common, None, *outs, rings[:5], RING // 2)
    front = stream(1, lambda t: (last, move(me, across, n, -1)), 0, PIECES - LATE[across], *common, queries, *outs, rings[5:10], 1)
    back = stream(n - len(LATE), lambda t: (last, move(me, len(LATE) + t, n, -1)), 0, PIECES, *common, queries, *outs, rings[10:], n - len(LATE))
    results = [(pltpu.make_async_copy(result_place(land_ref, m, n).at[pl.ds(0, o_buf.shape[1]), :], o_buf.at[m], o_in_sem.at[m]),
                pltpu.make_async_copy(o_buf.at[m], o_out.at[m], o_out_sem.at[m])) for m in range(last)]

    for part in (front, back, main):
        part[1]()
    for take, _ in results:
        take.start()
    zero_c[...] = jnp.zeros_like(zero_c)
    zero_k[...] = jnp.zeros_like(zero_k)
    clear(state)
    steps = main[0]

    @pl.loop(0, steps)
    def _(t):
        main[2](t)

        every = steps // back[0]

        @pl.when(t % every == 0)
        def _():
            back[2](t // every)

        @pl.when(t == every // 2)
        def _():
            front[2](0)

    for take, give in results:
        take.wait()
        give.start()
    part_ref[:, :rank] = acc_ref[...]
    part_ref[:, rank : rank + LANES] = jnp.broadcast_to(m_ref[...], (part_ref.shape[0], LANES))
    part_ref[:, rank + LANES :] = jnp.broadcast_to(l_ref[...], (part_ref.shape[0], LANES))
    copy = pltpu.make_async_copy(part_ref, part_out, part_sem)
    copy.start()
    copy.wait()
    for part in (main, front, back):
        part[3]()
    for _, give in results:
        give.wait()


def last_kernel(n, req_local, scale, lens_ref, *refs):
    land_refs, refs = refs[: len(LATE)], refs[len(LATE) :]
    qa_ref, qr_ref, part_ref, c_old, kr_old, o_old, c_out, kr_out, o_out, *refs = refs
    m_ref, l_ref, acc_ref, o_buf, o_sem, kr_buf, c_sem, k_sem = refs
    last = req_local - 1
    length = lens_ref[lax.axis_index("x") * req_local + last]
    state = (m_ref, l_ref, acc_ref)
    rank = acc_ref.shape[1]
    width = kr_buf.shape[1]
    rows = kr_buf.shape[2]
    pieces = late_pieces()
    firsts = [pl.multiple_of((move(lax.axis_index("x"), j, n, -1) * PIECES + h) * rows, rows) for j, h in pieces]
    pieces = [(j, h - PIECES + LATE[j]) for j, h in pieces]
    clear(state)
    stores = []
    for at in range(0, len(pieces), BATCH):
        batch = range(at, min(at + BATCH, len(pieces)))
        for i in batch:
            (k, h), first = pieces[i], firsts[i]
            stores.append(pltpu.make_async_copy(land_refs[k].at[h, pl.ds(0, rows), :], c_out.at[last, pl.ds(first, rows), :], c_sem.at[i, 0]))
            stores[-1].start()
            for kr_rows, kr_cols, from_rows, from_cols in rope_tiles(width, rows):
                kr_buf[i, kr_rows, kr_cols] = land_refs[k][h, from_rows, from_cols]
            stores.append(pltpu.make_async_copy(kr_buf.at[i], kr_out.at[last, :, pl.ds(first, rows)], k_sem.at[i]))
            stores[-1].start()

        @pl.when(functools.reduce(jnp.minimum, [firsts[i] for i in batch]) < length)
        def _():
            blocks = [(land_refs[pieces[i][0]][pieces[i][1], :rows, :], kr_buf[i]) for i in batch]
            fold(state, qa_ref[last], qr_ref[last], blocks, [firsts[i] for i in batch], length, scale)

    m_part, l_part, acc_part = part_ref[:, rank : rank + 1], part_ref[:, rank + LANES : rank + LANES + 1], part_ref[:, :rank]
    m_new = jnp.maximum(m_ref[...], m_part)
    here, there = jnp.exp(m_ref[...] - m_new), jnp.exp(m_part - m_new)
    total = l_ref[...] * here + l_part * there
    o_buf[...] = ((acc_ref[...] * here + acc_part * there) / total).astype(jnp.bfloat16)
    copy = pltpu.make_async_copy(o_buf, o_out.at[last], o_sem)
    copy.start()
    for c in stores + [copy]:
        c.wait()


def attend(lens, landed, rest, q_lat, q_rope, n, block):
    req_local, heads, rank = q_lat.shape
    width = q_rope.shape[1]
    rows = block // PIECES
    total = rest[0].shape[1]
    late = len(late_pieces())
    scale = (rank + width) ** -0.5
    caches = [jax.ShapeDtypeStruct((req_local, n * block, rank), jnp.bfloat16),
              jax.ShapeDtypeStruct((req_local, width, n * block), jnp.bfloat16),
              jax.ShapeDtypeStruct((req_local, heads, rank), jnp.bfloat16)]
    part = jax.ShapeDtypeStruct((heads, rank + 2 * LANES), jnp.float32)
    state = [pltpu.VMEM((heads, 1), jnp.float32), pltpu.VMEM((heads, 1), jnp.float32), pltpu.VMEM((heads, rank), jnp.float32)]

    def stores(depth, pieces):
        return [pltpu.VMEM((depth, width, pieces * rows), jnp.bfloat16), pltpu.SemaphoreType.DMA((depth, pieces)), pltpu.SemaphoreType.DMA((depth,))]

    def ring(depth, pieces):
        return [pltpu.VMEM((depth, pieces, total, rank), jnp.bfloat16), pltpu.SemaphoreType.DMA((depth,))] + stores(depth, pieces)

    params = pltpu.CompilerParams(vmem_limit_bytes=ATTEND_BYTES)
    flops = 2 * req_local * n * block * heads * rank
    *outs, first_part = pl.pallas_call(
        functools.partial(first_kernel, n, req_local, scale),
        in_specs=[SMEM, HBM, VMEM, VMEM],
        out_specs=[HBM] * 4,
        out_shape=caches + [part],
        scratch_shapes=state + [pltpu.VMEM(part.shape, part.dtype), pltpu.SemaphoreType.DMA,
                                pltpu.VMEM((rows, rank), jnp.bfloat16), pltpu.VMEM((width, block), jnp.bfloat16),
                                pltpu.VMEM((req_local - 1, heads, rank), jnp.bfloat16),
                                pltpu.SemaphoreType.DMA((req_local - 1,)), pltpu.SemaphoreType.DMA((req_local - 1,))]
        + ring(RING, PIECES) + ring(1, PIECES - LATE[-1]) + ring(n - len(LATE), PIECES),
        compiler_params=params,
        cost_estimate=pl.CostEstimate(flops=flops, bytes_accessed=req_local * n * block * rank * 4, transcendentals=0),
        name="attend_first",
    )(lens, landed, q_lat, q_rope)
    return pl.pallas_call(
        functools.partial(last_kernel, n, req_local, scale),
        in_specs=[SMEM] + [VMEM] * (len(LATE) + 3) + [HBM] * 3,
        out_specs=[HBM] * 3,
        out_shape=caches,
        scratch_shapes=state + [pltpu.VMEM((heads, rank), jnp.bfloat16), pltpu.SemaphoreType.DMA] + stores(late, 1),
        input_output_aliases={len(LATE) + 4 + k: k for k in range(3)},
        compiler_params=params,
        cost_estimate=pl.CostEstimate(flops=flops // req_local // PIECES, bytes_accessed=n * block * rank * 2, transcendentals=0),
        name="attend_last",
    )(lens, *rest, q_lat, q_rope, first_part, *outs)


def solution(mesh):
    seq_spec = P("dp", "x", None)
    req_spec = P(("dp", "x"), None, None)
    n = mesh.shape["x"]

    def local_step(c_raw, k_raw, norm_gain, rope_cos, rope_sin, seq_lens, q_lat, q_rope):
        q_rope = jnp.swapaxes(q_rope, 1, 2)
        landed, *rest = send(seq_lens, c_raw, jnp.swapaxes(k_raw, 1, 2), norm_gain, rope_cos.T, rope_sin.T, q_lat, q_rope, n)
        rest = [lax.ppermute(pieces, "x", [(i, move(i, j, n, 1)) for i in range(n)]) for j, pieces in enumerate(rest)]
        c_cache, kr_cache, o_lat = attend(seq_lens, landed, rest, q_lat, q_rope, n, c_raw.shape[1])
        return c_cache, jnp.swapaxes(kr_cache, 1, 2), o_lat

    return jax.shard_map(local_step, mesh=mesh, in_specs=(seq_spec, seq_spec, P(None), P("x", None), P("x", None), P("dp"), req_spec, req_spec), out_specs=(req_spec, req_spec, req_spec), check_vma=False)
```

```python
import functools

import jax
import jax.numpy as jnp
from jax import lax
from jax.experimental import pallas as pl
from jax.experimental.pallas import tpu as pltpu
from jax.sharding import PartitionSpec as P

NORM_EPS = 1e-6
PIECES = 3
ROUNDS = 6
LOADS = 4
RING = 12
LATE = (3, 3, 1)
BATCH = 7
AHEAD = 3
STRIPE = 128
LANES, SUBLANES = 128, 16
VMEM_BYTES = 60 * 1024 * 1024
ATTEND_BYTES = 44 * 1024 * 1024
MESH = pl.DeviceIdType.MESH
HBM = pl.BlockSpec(memory_space=pltpu.HBM)
VMEM = pl.BlockSpec(memory_space=pltpu.VMEM)
SMEM = pl.BlockSpec(memory_space=pltpu.SMEM)


def move(me, j, n, way):
    chip, core = me // 2, me % 2
    far = j % 3
    last = j // (n - 2)
    other = (j // 3) % 2 * (1 - last) + last * (1 - j % (n - 2))
    there = (core + other) % 2
    sender = core if way == 1 else there
    hop = (1 - last) * (1 + 2 * far - 3 * (far // 2)) * (1 - 2 * sender)
    return (chip + n // 2 + way * hop) % (n // 2) * 2 + there


def peer(j, n):
    return move(lax.axis_index("x"), j, n, 1)


def late_pieces():
    return [(j, h) for j, count in enumerate(LATE) for h in range(PIECES - count, PIECES)]


def result_place(land_ref, m, n):
    return land_ref.at[land_ref.shape[0] - 1, move(lax.axis_index("x"), m // PIECES, n, -1), m % PIECES]


def rope_tiles(width, rows):
    for r in range(width // SUBLANES):
        for c in range(rows // LANES):
            yield (slice(r * SUBLANES, (r + 1) * SUBLANES), slice(c * LANES, (c + 1) * LANES),
                   slice(rows + c * SUBLANES, rows + (c + 1) * SUBLANES), slice(r * LANES, (r + 1) * LANES))


def clear(state):
    m_ref, l_ref, acc_ref = state
    m_ref[...] = jnp.full_like(m_ref, -1e30)
    l_ref[...] = jnp.zeros_like(l_ref)
    acc_ref[...] = jnp.zeros_like(acc_ref)


def fold(state, qa, qr, pieces, firsts, length, scale):
    m_ref, l_ref, acc_ref = state
    scores = []
    for first, (lat, kr) in zip(firsts, pieces):
        s = lax.dot_general(qa, lat, (((1,), (1,)), ((), ())), preferred_element_type=jnp.float32)
        s = s + lax.dot_general(qr, kr, (((0,), (0,)), ((), ())), preferred_element_type=jnp.float32)
        rows = lat.shape[0]
        pos = first + lax.broadcasted_iota(jnp.int32, (1, rows), 1)
        scores.append(jnp.where(pos < length, s * scale, -1e30))
    m_old = m_ref[...]
    m_new = m_old
    for s in scores:
        m_new = jnp.maximum(m_new, jnp.max(s, axis=-1, keepdims=True))
    alpha = jnp.exp(m_old - m_new)
    total, acc = l_ref[...] * alpha, acc_ref[...] * alpha
    for s, (lat, _) in zip(scores, pieces):
        p = jnp.exp(s - m_new)
        total = total + jnp.sum(p, axis=-1, keepdims=True)
        acc = acc + jnp.dot(p.astype(jnp.bfloat16), lat, preferred_element_type=jnp.float32)
    m_ref[...], l_ref[...], acc_ref[...] = m_new, total, acc


def send_kernel(n, req_local, scale, lens_ref, c_hbm, k_hbm, gain_ref, cos_ref, sin_ref, qa_ref, qr_ref, land_ref, *scratch):
    rest_refs, scratch = scratch[: len(LATE)], scratch[len(LATE) :]
    c_buf, k_buf, out_buf, c_sem, k_sem, send_sem, recv_sem, m_ref, l_ref, acc_ref, fold_buf, kr_buf, fold_sem, o_buf, o_sem = scratch
    me = lax.axis_index("x")
    rounds = req_local * PIECES
    steps = rounds * n
    early = (rounds - PIECES) * n
    depth = out_buf.shape[0]
    rows, rank = c_buf.shape[1:]
    width = k_buf.shape[1]

    def step(t):
        q = t % n
        last = q // (n - 2)
        return (1 - last) * ((q + 2 * (me % 2)) % (n - 2)) + last * q

    def load(t):
        req = peer(step(t), n) * req_local + t // n // PIECES
        first = pl.multiple_of(t // n % PIECES * rows, rows)
        slot = t % LOADS
        return (pltpu.make_async_copy(c_hbm.at[req, pl.ds(first, rows), :], c_buf.at[slot], c_sem.at[slot]),
                pltpu.make_async_copy(k_hbm.at[req, :, pl.ds(first, rows)], k_buf.at[slot], k_sem.at[slot]))

    def landing(t):
        return land_ref.at[t // n // PIECES, me, t // n % PIECES]

    def remote(t):
        slot = t % depth
        return pltpu.make_async_remote_copy(
            src_ref=out_buf.at[slot], dst_ref=landing(t), send_sem=send_sem.at[slot],
            recv_sem=recv_sem.at[t // n * n + me], device_id={"x": peer(step(t), n)}, device_id_type=MESH)

    def own(t):
        return pltpu.make_async_copy(out_buf.at[t % depth], landing(t), send_sem.at[t % depth])

    def keep(t, j, h):
        return pltpu.make_async_copy(out_buf.at[t % depth], rest_refs[j].at[h - PIECES + LATE[j]], send_sem.at[t % depth])

    def at_late(t, way, j, h):
        return jnp.logical_and(t // n == early // n + h, way == j)

    def is_kept(t, way):
        return functools.reduce(jnp.logical_or, [at_late(t, way, j, h) for j, h in late_pieces()])

    def on_kind(t, act_remote, act_local):
        is_own = t % n == n - 1

        for j, h in late_pieces():
            @pl.when(at_late(t, step(t), j, h))
            def _():
                act_local(keep(t, j, h))

        @pl.when(is_own)
        def _():
            act_local(own(t))

        @pl.when(jnp.logical_not(jnp.logical_or(is_own, is_kept(t, step(t)))))
        def _():
            act_remote(remote(t))

    def start(t):
        on_kind(t, lambda c: c.start(), lambda c: c.start())

    def sent(t):
        on_kind(t, lambda c: c.wait_send(), lambda c: c.wait())

    def pack(t):
        for c in load(t):
            c.wait()
        slot, out = t % LOADS, t % depth
        first = t // n % PIECES * rows
        left = lens_ref[peer(step(t), n) * req_local + t // n // PIECES] - me * (rows * PIECES) - first
        gain = gain_ref[...].astype(jnp.float32)

        @pl.loop(0, rows, step=STRIPE)
        def _(r):
            r = pl.multiple_of(r, STRIPE)
            lat = c_buf[slot, pl.ds(r, STRIPE), :].astype(jnp.float32)
            inv = lax.rsqrt(jnp.mean(lat * lat, axis=-1, keepdims=True) + NORM_EPS)
            valid = r + lax.broadcasted_iota(jnp.int32, (STRIPE, 1), 0) < left
            out_buf[out, pl.ds(r, STRIPE), :] = jnp.where(valid, lat * inv * gain, 0.0).astype(jnp.bfloat16)

        key = k_buf[slot].astype(jnp.float32)
        half = width // 2
        lo, hi = key[:half], key[half:]
        first = pl.multiple_of(first, LANES)
        cos, sin = cos_ref[:, pl.ds(first, rows)], sin_ref[:, pl.ds(first, rows)]
        valid = lax.broadcasted_iota(jnp.int32, (1, rows), 1) < left
        rotated = (jnp.where(valid, lo * cos - hi * sin, 0.0).astype(jnp.bfloat16),
                   jnp.where(valid, hi * cos + lo * sin, 0.0).astype(jnp.bfloat16))
        for kr_rows, kr_cols, to_rows, to_cols in rope_tiles(width, rows):
            part, at = kr_rows.start // half, kr_rows.start % half
            out_buf[out, to_rows, to_cols] = rotated[part][at : at + SUBLANES, kr_cols]

    barrier = pltpu.get_barrier_semaphore()
    for j in range(n - 1):
        pl.semaphore_signal(barrier, inc=1, device_id={"x": peer(j, n)}, device_id_type=MESH)
    for t in range(LOADS):
        for c in load(t):
            c.start()
    pack(0)
    for c in load(LOADS):
        c.start()
    pl.semaphore_wait(barrier, n - 1)

    state = (m_ref, l_ref, acc_ref)
    per_req = PIECES * n
    folds = (req_local - 1) * per_req
    lag = depth + n

    def received(a):
        src = peer(a % n, n)
        piece = land_ref.at[a // per_req, src, a // n % PIECES]
        pltpu.make_async_remote_copy(
            src_ref=piece, dst_ref=piece, send_sem=send_sem.at[0], recv_sem=recv_sem.at[a // n * n + src],
            device_id={"x": src}, device_id_type=MESH).wait_recv()

    def result(m):
        return pltpu.make_async_copy(o_buf.at[m], result_place(land_ref, m, n).at[pl.ds(0, o_buf.shape[1]), :], o_sem.at[m])

    def fetch(a):
        return pltpu.make_async_copy(land_ref.at[a // per_req, peer(a % n, n), a // n % PIECES], fold_buf.at[a % (AHEAD + 1)], fold_sem.at[a % (AHEAD + 1)])

    @pl.loop(1, folds + lag)
    def _(t):
        @pl.when(t >= depth)
        def _():
            sent(t - depth)

        @pl.when(t < steps)
        def _():
            pack(t)

            @pl.when(t + LOADS < steps)
            def _():
                for c in load(t + LOADS):
                    c.start()

        @pl.when(t <= steps)
        def _():
            start(t - 1)

        arriving = t - lag + AHEAD

        @pl.when(jnp.logical_and(arriving >= 0, arriving < folds))
        def _():
            @pl.when(arriving % n < n - 1)
            def _():
                received(arriving)

            fetch(arriving).start()

        a = t - lag

        @pl.when(a >= 0)
        def _():
            m, src, slot = a // per_req, peer(a % n, n), a % (AHEAD + 1)

            @pl.when(a % per_req == 0)
            def _():
                clear(state)

            fetch(a).wait()
            for kr_rows, kr_cols, from_rows, from_cols in rope_tiles(width, rows):
                kr_buf[kr_rows, kr_cols] = fold_buf[slot, from_rows, from_cols]
            first = (src * PIECES + a // n % PIECES) * rows
            fold(state, qa_ref[m], qr_ref[m], [(fold_buf[slot, :rows, :], kr_buf[...])], [first], lens_ref[me * req_local + m], scale)

            @pl.when(a % per_req == per_req - 1)
            def _():
                o_buf[m] = (acc_ref[...] / l_ref[...]).astype(jnp.bfloat16)
                result(m).start()

    @pl.loop(folds + lag - depth, steps)
    def _(t):
        sent(t)

    @pl.loop(folds, steps)
    def _(a):
        @pl.when(jnp.logical_and(a % n < n - 1, jnp.logical_not(is_kept(a, a % n))))
        def _():
            received(a)

    for m in range(req_local - 1):
        result(m).wait()


def send(lens, c_raw, k_raw, gain, cos, sin, q_lat, q_rope, n):
    req_local, heads, _ = q_lat.shape
    requests, block, rank = c_raw.shape
    width = k_raw.shape[1]
    rows = block // PIECES
    total = rows + rows * width // rank
    depth = ROUNDS * n
    return pl.pallas_call(
        functools.partial(send_kernel, n, req_local, (rank + width) ** -0.5),
        in_specs=[SMEM, HBM, HBM] + [VMEM] * 5,
        out_specs=[HBM] * (1 + len(LATE)),
        out_shape=[jax.ShapeDtypeStruct((req_local, n, PIECES, total, rank), jnp.bfloat16)]
        + [jax.ShapeDtypeStruct((count, total, rank), jnp.bfloat16) for count in LATE],
        scratch_shapes=[
            pltpu.VMEM((LOADS, rows, rank), jnp.bfloat16),
            pltpu.VMEM((LOADS, width, rows), jnp.bfloat16),
            pltpu.VMEM((depth, total, rank), jnp.bfloat16),
            pltpu.SemaphoreType.DMA((LOADS,)),
            pltpu.SemaphoreType.DMA((LOADS,)),
            pltpu.SemaphoreType.DMA((depth,)),
            pltpu.SemaphoreType.DMA((req_local * PIECES * n,)),
            pltpu.VMEM((heads, 1), jnp.float32),
            pltpu.VMEM((heads, 1), jnp.float32),
            pltpu.VMEM((heads, rank), jnp.float32),
            pltpu.VMEM((AHEAD + 1, total, rank), jnp.bfloat16),
            pltpu.VMEM((width, rows), jnp.bfloat16),
            pltpu.SemaphoreType.DMA((AHEAD + 1,)),
            pltpu.VMEM((req_local - 1, heads, rank), jnp.bfloat16),
            pltpu.SemaphoreType.DMA((req_local - 1,)),
        ],
        compiler_params=pltpu.CompilerParams(vmem_limit_bytes=VMEM_BYTES, collective_id=0, has_side_effects=True),
        cost_estimate=pl.CostEstimate(flops=requests * block * rank * 100, bytes_accessed=requests * block * rank * 4, transcendentals=0),
        name="send",
    )(lens, c_raw, k_raw, gain, cos, sin, q_lat, q_rope)


def stream(steps, place, first_piece, pieces, scale, length, land_ref, queries, c_out, kr_out, state, zero_c, zero_k, ring, ahead):
    buf, in_sem, kr_buf, c_sem, k_sem = ring
    depth = buf.shape[0]
    rank = buf.shape[3]
    width = kr_buf.shape[1]
    rows = kr_buf.shape[2] // pieces

    def first(t):
        return pl.multiple_of((place(t)[1] * PIECES + first_piece) * rows, rows)

    def used(t):
        return first(t) < length(place(t)[0])

    def load(t):
        req, src = place(t)
        return pltpu.make_async_copy(land_ref.at[req, src, pl.ds(first_piece, pieces)], buf.at[t % depth], in_sem.at[t % depth])

    def writes(t, c_of, kr):
        slot, req, at = t % depth, place(t)[0], first(t)
        return [pltpu.make_async_copy(c_of(h), c_out.at[req, pl.ds(at + h * rows, rows), :], c_sem.at[slot, h]) for h in range(pieces)] + [
            pltpu.make_async_copy(kr, kr_out.at[req, :, pl.ds(at, pieces * rows)], k_sem.at[slot])]

    def stores(t):
        return writes(t, lambda h: buf.at[t % depth, h, pl.ds(0, rows), :], kr_buf.at[t % depth])

    def blanks(t):
        return writes(t, lambda h: zero_c, zero_k.at[:, pl.ds(0, pieces * rows)])

    def fetch(t):
        @pl.when(used(t))
        def _():
            load(t).start()

    def work(t):
        slot = t % depth
        load(t).wait()
        for h in range(pieces):
            for kr_rows, kr_cols, from_rows, from_cols in rope_tiles(width, rows):
                cols = slice(h * rows + kr_cols.start, h * rows + kr_cols.stop)
                kr_buf[slot, kr_rows, cols] = buf[slot, h, from_rows, from_cols]
        for c in stores(t):
            c.start()
        if queries is not None:
            qa, qr = queries()
            blocks = [(buf[slot, h, :rows, :], kr_buf[slot, :, h * rows : (h + 1) * rows]) for h in range(pieces)]
            fold(state, qa, qr, blocks, [first(t) + h * rows for h in range(pieces)], length(place(t)[0]), scale)

    def body(t):
        @pl.when(used(t))
        def _():
            work(t)

        @pl.when(jnp.logical_not(used(t)))
        def _():
            for c in blanks(t):
                c.start()

        @pl.when(t + ahead < steps)
        def _():
            @pl.when(t + ahead >= depth)
            def _():
                for c in stores(t + ahead - depth):
                    c.wait()

            fetch(t + ahead)

    def prologue():
        for t in range(min(ahead, steps)):
            fetch(t)

    def drain():
        @pl.loop(max(steps - depth, 0), steps)
        def _(t):
            for c in stores(t):
                c.wait()

    return steps, prologue, body, drain


def first_kernel(n, req_local, scale, lens_ref, land_ref, qa_ref, qr_ref, c_out, kr_out, o_out, part_out,
                 m_ref, l_ref, acc_ref, part_ref, part_sem, zero_c, zero_k, o_buf, o_in_sem, o_out_sem, *rings):
    length = lambda m: lens_ref[lax.axis_index("x") * req_local + m]
    state = (m_ref, l_ref, acc_ref)
    last = req_local - 1
    rank = acc_ref.shape[1]
    me = lax.axis_index("x")
    across = len(LATE) - 1
    queries = lambda: (qa_ref[last], qr_ref[last])
    common = (scale, length, land_ref)
    outs = (c_out, kr_out, state, zero_c, zero_k)
    main = stream(last * n, lambda t: (t // n, t % n), 0, PIECES, *common, None, *outs, rings[:5], RING // 2)
    front = stream(1, lambda t: (last, move(me, across, n, -1)), 0, PIECES - LATE[across], *common, queries, *outs, rings[5:10], 1)
    back = stream(n - len(LATE), lambda t: (last, move(me, len(LATE) + t, n, -1)), 0, PIECES, *common, queries, *outs, rings[10:], n - len(LATE))
    results = [(pltpu.make_async_copy(result_place(land_ref, m, n).at[pl.ds(0, o_buf.shape[1]), :], o_buf.at[m], o_in_sem.at[m]),
                pltpu.make_async_copy(o_buf.at[m], o_out.at[m], o_out_sem.at[m])) for m in range(last)]

    for part in (front, back, main):
        part[1]()
    for take, _ in results:
        take.start()
    zero_c[...] = jnp.zeros_like(zero_c)
    zero_k[...] = jnp.zeros_like(zero_k)
    clear(state)
    steps = main[0]

    @pl.loop(0, steps)
    def _(t):
        main[2](t)

        every = steps // back[0]

        @pl.when(t % every == 0)
        def _():
            back[2](t // every)

        @pl.when(t == every // 2)
        def _():
            front[2](0)

    for take, give in results:
        take.wait()
        give.start()
    part_ref[:, :rank] = acc_ref[...]
    part_ref[:, rank : rank + LANES] = jnp.broadcast_to(m_ref[...], (part_ref.shape[0], LANES))
    part_ref[:, rank + LANES :] = jnp.broadcast_to(l_ref[...], (part_ref.shape[0], LANES))
    copy = pltpu.make_async_copy(part_ref, part_out, part_sem)
    copy.start()
    copy.wait()
    for part in (main, front, back):
        part[3]()
    for _, give in results:
        give.wait()


def last_kernel(n, req_local, scale, lens_ref, *refs):
    land_refs, refs = refs[: len(LATE)], refs[len(LATE) :]
    qa_ref, qr_ref, part_ref, c_old, kr_old, o_old, c_out, kr_out, o_out, *refs = refs
    m_ref, l_ref, acc_ref, o_buf, o_sem, kr_buf, c_sem, k_sem = refs
    last = req_local - 1
    length = lens_ref[lax.axis_index("x") * req_local + last]
    state = (m_ref, l_ref, acc_ref)
    rank = acc_ref.shape[1]
    width = kr_buf.shape[1]
    rows = kr_buf.shape[2]
    pieces = late_pieces()
    firsts = [pl.multiple_of((move(lax.axis_index("x"), j, n, -1) * PIECES + h) * rows, rows) for j, h in pieces]
    pieces = [(j, h - PIECES + LATE[j]) for j, h in pieces]
    clear(state)
    stores = []
    for at in range(0, len(pieces), BATCH):
        batch = range(at, min(at + BATCH, len(pieces)))
        for i in batch:
            (k, h), first = pieces[i], firsts[i]
            stores.append(pltpu.make_async_copy(land_refs[k].at[h, pl.ds(0, rows), :], c_out.at[last, pl.ds(first, rows), :], c_sem.at[i, 0]))
            stores[-1].start()
            for kr_rows, kr_cols, from_rows, from_cols in rope_tiles(width, rows):
                kr_buf[i, kr_rows, kr_cols] = land_refs[k][h, from_rows, from_cols]
            stores.append(pltpu.make_async_copy(kr_buf.at[i], kr_out.at[last, :, pl.ds(first, rows)], k_sem.at[i]))
            stores[-1].start()

        @pl.when(functools.reduce(jnp.minimum, [firsts[i] for i in batch]) < length)
        def _():
            blocks = [(land_refs[pieces[i][0]][pieces[i][1], :rows, :], kr_buf[i]) for i in batch]
            fold(state, qa_ref[last], qr_ref[last], blocks, [firsts[i] for i in batch], length, scale)

    m_part, l_part, acc_part = part_ref[:, rank : rank + 1], part_ref[:, rank + LANES : rank + LANES + 1], part_ref[:, :rank]
    m_new = jnp.maximum(m_ref[...], m_part)
    here, there = jnp.exp(m_ref[...] - m_new), jnp.exp(m_part - m_new)
    total = l_ref[...] * here + l_part * there
    o_buf[...] = ((acc_ref[...] * here + acc_part * there) / total).astype(jnp.bfloat16)
    copy = pltpu.make_async_copy(o_buf, o_out.at[last], o_sem)
    copy.start()
    for c in stores + [copy]:
        c.wait()


def attend(lens, landed, rest, q_lat, q_rope, n, block):
    req_local, heads, rank = q_lat.shape
    width = q_rope.shape[1]
    rows = block // PIECES
    total = rest[0].shape[1]
    late = len(late_pieces())
    scale = (rank + width) ** -0.5
    caches = [jax.ShapeDtypeStruct((req_local, n * block, rank), jnp.bfloat16),
              jax.ShapeDtypeStruct((req_local, width, n * block), jnp.bfloat16),
              jax.ShapeDtypeStruct((req_local, heads, rank), jnp.bfloat16)]
    part = jax.ShapeDtypeStruct((heads, rank + 2 * LANES), jnp.float32)
    state = [pltpu.VMEM((heads, 1), jnp.float32), pltpu.VMEM((heads, 1), jnp.float32), pltpu.VMEM((heads, rank), jnp.float32)]

    def stores(depth, pieces):
        return [pltpu.VMEM((depth, width, pieces * rows), jnp.bfloat16), pltpu.SemaphoreType.DMA((depth, pieces)), pltpu.SemaphoreType.DMA((depth,))]

    def ring(depth, pieces):
        return [pltpu.VMEM((depth, pieces, total, rank), jnp.bfloat16), pltpu.SemaphoreType.DMA((depth,))] + stores(depth, pieces)

    params = pltpu.CompilerParams(vmem_limit_bytes=ATTEND_BYTES)
    flops = 2 * req_local * n * block * heads * rank
    *outs, first_part = pl.pallas_call(
        functools.partial(first_kernel, n, req_local, scale),
        in_specs=[SMEM, HBM, VMEM, VMEM],
        out_specs=[HBM] * 4,
        out_shape=caches + [part],
        scratch_shapes=state + [pltpu.VMEM(part.shape, part.dtype), pltpu.SemaphoreType.DMA,
                                pltpu.VMEM((rows, rank), jnp.bfloat16), pltpu.VMEM((width, block), jnp.bfloat16),
                                pltpu.VMEM((req_local - 1, heads, rank), jnp.bfloat16),
                                pltpu.SemaphoreType.DMA((req_local - 1,)), pltpu.SemaphoreType.DMA((req_local - 1,))]
        + ring(RING, PIECES) + ring(1, PIECES - LATE[-1]) + ring(n - len(LATE), PIECES),
        compiler_params=params,
        cost_estimate=pl.CostEstimate(flops=flops, bytes_accessed=req_local * n * block * rank * 4, transcendentals=0),
        name="attend_first",
    )(lens, landed, q_lat, q_rope)
    return pl.pallas_call(
        functools.partial(last_kernel, n, req_local, scale),
        in_specs=[SMEM] + [VMEM] * (len(LATE) + 3) + [HBM] * 3,
        out_specs=[HBM] * 3,
        out_shape=caches,
        scratch_shapes=state + [pltpu.VMEM((heads, rank), jnp.bfloat16), pltpu.SemaphoreType.DMA] + stores(late, 1),
        input_output_aliases={len(LATE) + 4 + k: k for k in range(3)},
        compiler_params=params,
        cost_estimate=pl.CostEstimate(flops=flops // req_local // PIECES, bytes_accessed=n * block * rank * 2, transcendentals=0),
        name="attend_last",
    )(lens, *rest, q_lat, q_rope, first_part, *outs)


def solution(mesh):
    seq_spec = P("dp", "x", None)
    req_spec = P(("dp", "x"), None, None)
    n = mesh.shape["x"]

    def local_step(c_raw, k_raw, norm_gain, rope_cos, rope_sin, seq_lens, q_lat, q_rope):
        q_rope = jnp.swapaxes(q_rope, 1, 2)
        landed, *rest = send(seq_lens, c_raw, jnp.swapaxes(k_raw, 1, 2), norm_gain, rope_cos.T, rope_sin.T, q_lat, q_rope, n)
        rest = [lax.ppermute(pieces, "x", [(i, move(i, j, n, 1)) for i in range(n)]) for j, pieces in enumerate(rest)]
        c_cache, kr_cache, o_lat = attend(seq_lens, landed, rest, q_lat, q_rope, n, c_raw.shape[1])
        return c_cache, jnp.swapaxes(kr_cache, 1, 2), o_lat

    return jax.shard_map(local_step, mesh=mesh, in_specs=(seq_spec, seq_spec, P(None), P("x", None), P("x", None), P("dp"), req_spec, req_spec), out_specs=(req_spec, req_spec, req_spec), check_vma=False)
```

```python
import functools

import jax
import jax.numpy as jnp
from jax import lax
from jax.experimental import pallas as pl
from jax.experimental.pallas import tpu as pltpu
from jax.sharding import PartitionSpec as P

NORM_EPS = 1e-6
PIECES = 3
ROUNDS = 6
LOADS = 4
RING = 20
LATE = (3, 3, 1)
BATCH = 7
AHEAD = 3
STRIPE = 128
LANES, SUBLANES = 128, 16
VMEM_BYTES = 60 * 1024 * 1024
ATTEND_BYTES = 44 * 1024 * 1024
MESH = pl.DeviceIdType.MESH
HBM = pl.BlockSpec(memory_space=pltpu.HBM)
VMEM = pl.BlockSpec(memory_space=pltpu.VMEM)
SMEM = pl.BlockSpec(memory_space=pltpu.SMEM)


def move(me, j, n, way):
    chip, core = me // 2, me % 2
    far = j % 3
    last = j // (n - 2)
    other = (j // 3) % 2 * (1 - last) + last * (1 - j % (n - 2))
    there = (core + other) % 2
    sender = core if way == 1 else there
    hop = (1 - last) * (1 + 2 * far - 3 * (far // 2)) * (1 - 2 * sender)
    return (chip + n // 2 + way * hop) % (n // 2) * 2 + there


def peer(j, n):
    return move(lax.axis_index("x"), j, n, 1)


def late_pieces():
    return [(j, h) for j, count in enumerate(LATE) for h in range(PIECES - count, PIECES)]


def result_place(land_ref, m, n):
    return land_ref.at[land_ref.shape[0] - 1, move(lax.axis_index("x"), m // PIECES, n, -1), m % PIECES]


def rope_tiles(width, rows):
    for r in range(width // SUBLANES):
        for c in range(rows // LANES):
            yield (slice(r * SUBLANES, (r + 1) * SUBLANES), slice(c * LANES, (c + 1) * LANES),
                   slice(rows + c * SUBLANES, rows + (c + 1) * SUBLANES), slice(r * LANES, (r + 1) * LANES))


def clear(state):
    m_ref, l_ref, acc_ref = state
    m_ref[...] = jnp.full_like(m_ref, -1e30)
    l_ref[...] = jnp.zeros_like(l_ref)
    acc_ref[...] = jnp.zeros_like(acc_ref)


def fold(state, qa, qr, pieces, firsts, length, scale):
    m_ref, l_ref, acc_ref = state
    scores = []
    for first, (lat, kr) in zip(firsts, pieces):
        s = lax.dot_general(qa, lat, (((1,), (1,)), ((), ())), preferred_element_type=jnp.float32)
        s = s + lax.dot_general(qr, kr, (((0,), (0,)), ((), ())), preferred_element_type=jnp.float32)
        rows = lat.shape[0]
        pos = first + lax.broadcasted_iota(jnp.int32, (1, rows), 1)
        scores.append(jnp.where(pos < length, s * scale, -1e30))
    m_old = m_ref[...]
    m_new = m_old
    for s in scores:
        m_new = jnp.maximum(m_new, jnp.max(s, axis=-1, keepdims=True))
    alpha = jnp.exp(m_old - m_new)
    total, acc = l_ref[...] * alpha, acc_ref[...] * alpha
    for s, (lat, _) in zip(scores, pieces):
        p = jnp.exp(s - m_new)
        total = total + jnp.sum(p, axis=-1, keepdims=True)
        acc = acc + jnp.dot(p.astype(jnp.bfloat16), lat, preferred_element_type=jnp.float32)
    m_ref[...], l_ref[...], acc_ref[...] = m_new, total, acc


def send_kernel(n, req_local, scale, lens_hbm, c_hbm, k_hbm, gain_ref, cos_hbm, sin_hbm, qa_hbm, qr_hbm, land_ref, *scratch):
    rest_refs, scratch = scratch[: len(LATE)], scratch[len(LATE) :]
    c_buf, k_buf, out_buf, c_sem, k_sem, send_sem, recv_sem, m_ref, l_ref, acc_ref, fold_buf, kr_buf, fold_sem, o_buf, o_sem, *tables = scratch
    lens_ref, cos_ref, sin_ref, qa_ref, qr_ref, table_sem = tables
    me = lax.axis_index("x")
    rounds = req_local * PIECES
    steps = rounds * n
    early = (rounds - PIECES) * n
    depth = out_buf.shape[0]
    rows, rank = c_buf.shape[1:]
    width = k_buf.shape[1]

    def step(t):
        q = t % n
        last = q // (n - 2)
        return (1 - last) * ((q + 2 * (me % 2)) % (n - 2)) + last * q

    def load(t):
        req = peer(step(t), n) * req_local + t // n // PIECES
        first = pl.multiple_of(t // n % PIECES * rows, rows)
        slot = t % LOADS
        return (pltpu.make_async_copy(c_hbm.at[req, pl.ds(first, rows), :], c_buf.at[slot], c_sem.at[slot]),
                pltpu.make_async_copy(k_hbm.at[req, :, pl.ds(first, rows)], k_buf.at[slot], k_sem.at[slot]))

    def landing(t):
        return land_ref.at[t // n // PIECES, me, t // n % PIECES]

    def remote(t):
        slot = t % depth
        return pltpu.make_async_remote_copy(
            src_ref=out_buf.at[slot], dst_ref=landing(t), send_sem=send_sem.at[slot],
            recv_sem=recv_sem.at[t // n * n + me], device_id={"x": peer(step(t), n)}, device_id_type=MESH)

    def own(t):
        return pltpu.make_async_copy(out_buf.at[t % depth], landing(t), send_sem.at[t % depth])

    def keep(t, j, h):
        return pltpu.make_async_copy(out_buf.at[t % depth], rest_refs[j].at[h - PIECES + LATE[j]], send_sem.at[t % depth])

    def at_late(t, way, j, h):
        return jnp.logical_and(t // n == early // n + h, way == j)

    def is_kept(t, way):
        return functools.reduce(jnp.logical_or, [at_late(t, way, j, h) for j, h in late_pieces()])

    def on_kind(t, act_remote, act_local):
        is_own = t % n == n - 1

        for j, h in late_pieces():
            @pl.when(at_late(t, step(t), j, h))
            def _():
                act_local(keep(t, j, h))

        @pl.when(is_own)
        def _():
            act_local(own(t))

        @pl.when(jnp.logical_not(jnp.logical_or(is_own, is_kept(t, step(t)))))
        def _():
            act_remote(remote(t))

    def start(t):
        on_kind(t, lambda c: c.start(), lambda c: c.start())

    def sent(t):
        on_kind(t, lambda c: c.wait_send(), lambda c: c.wait())

    def pack(t):
        for c in load(t):
            c.wait()
        slot, out = t % LOADS, t % depth
        first = t // n % PIECES * rows
        left = lens_ref[peer(step(t), n) * req_local + t // n // PIECES] - me * (rows * PIECES) - first
        gain = gain_ref[...].astype(jnp.float32)

        @pl.loop(0, rows, step=STRIPE)
        def _(r):
            r = pl.multiple_of(r, STRIPE)
            lat = c_buf[slot, pl.ds(r, STRIPE), :].astype(jnp.float32)
            inv = lax.rsqrt(jnp.mean(lat * lat, axis=-1, keepdims=True) + NORM_EPS)
            valid = r + lax.broadcasted_iota(jnp.int32, (STRIPE, 1), 0) < left
            out_buf[out, pl.ds(r, STRIPE), :] = jnp.where(valid, lat * inv * gain, 0.0).astype(jnp.bfloat16)

        key = k_buf[slot].astype(jnp.float32)
        half = width // 2
        lo, hi = key[:half], key[half:]
        first = pl.multiple_of(first, LANES)
        cos, sin = cos_ref[:, pl.ds(first, rows)], sin_ref[:, pl.ds(first, rows)]
        valid = lax.broadcasted_iota(jnp.int32, (1, rows), 1) < left
        rotated = (jnp.where(valid, lo * cos - hi * sin, 0.0).astype(jnp.bfloat16),
                   jnp.where(valid, hi * cos + lo * sin, 0.0).astype(jnp.bfloat16))
        for kr_rows, kr_cols, to_rows, to_cols in rope_tiles(width, rows):
            part, at = kr_rows.start // half, kr_rows.start % half
            out_buf[out, to_rows, to_cols] = rotated[part][at : at + SUBLANES, kr_cols]

    barrier = pltpu.get_barrier_semaphore()
    for j in range(n - 1):
        pl.semaphore_signal(barrier, inc=1, device_id={"x": peer(j, n)}, device_id_type=MESH)
    fills = [pltpu.make_async_copy(src, dst, table_sem.at[i]) for i, (src, dst) in enumerate(
        zip((lens_hbm, cos_hbm, sin_hbm, qa_hbm, qr_hbm), (lens_ref, cos_ref, sin_ref, qa_ref, qr_ref)))]
    for c in fills[:3]:
        c.start()
    for t in range(LOADS):
        for c in load(t):
            c.start()
    for c in fills[3:]:
        c.start()
    for c in fills[:3]:
        c.wait()
    pack(0)
    for c in load(LOADS):
        c.start()
    for c in fills[3:]:
        c.wait()
    pl.semaphore_wait(barrier, n - 1)

    state = (m_ref, l_ref, acc_ref)
    per_req = PIECES * n
    folds = (req_local - 1) * per_req
    lag = depth + n

    def received(a):
        src = peer(a % n, n)
        piece = land_ref.at[a // per_req, src, a // n % PIECES]
        pltpu.make_async_remote_copy(
            src_ref=piece, dst_ref=piece, send_sem=send_sem.at[0], recv_sem=recv_sem.at[a // n * n + src],
            device_id={"x": src}, device_id_type=MESH).wait_recv()

    def result(m):
        return pltpu.make_async_copy(o_buf.at[m], result_place(land_ref, m, n).at[pl.ds(0, o_buf.shape[1]), :], o_sem.at[m])

    def fetch(a):
        return pltpu.make_async_copy(land_ref.at[a // per_req, peer(a % n, n), a // n % PIECES], fold_buf.at[a % (AHEAD + 1)], fold_sem.at[a % (AHEAD + 1)])

    @pl.loop(1, folds + lag)
    def _(t):
        @pl.when(t >= depth)
        def _():
            sent(t - depth)

        @pl.when(t < steps)
        def _():
            pack(t)

            @pl.when(t + LOADS < steps)
            def _():
                for c in load(t + LOADS):
                    c.start()

        @pl.when(t <= steps)
        def _():
            start(t - 1)

        arriving = t - lag + AHEAD

        @pl.when(jnp.logical_and(arriving >= 0, arriving < folds))
        def _():
            @pl.when(arriving % n < n - 1)
            def _():
                received(arriving)

            fetch(arriving).start()

        a = t - lag

        @pl.when(a >= 0)
        def _():
            m, src, slot = a // per_req, peer(a % n, n), a % (AHEAD + 1)

            @pl.when(a % per_req == 0)
            def _():
                clear(state)

            fetch(a).wait()
            for kr_rows, kr_cols, from_rows, from_cols in rope_tiles(width, rows):
                kr_buf[kr_rows, kr_cols] = fold_buf[slot, from_rows, from_cols]
            first = (src * PIECES + a // n % PIECES) * rows
            fold(state, qa_ref[m], qr_ref[m], [(fold_buf[slot, :rows, :], kr_buf[...])], [first], lens_ref[me * req_local + m], scale)

            @pl.when(a % per_req == per_req - 1)
            def _():
                o_buf[m] = (acc_ref[...] / l_ref[...]).astype(jnp.bfloat16)
                result(m).start()

    @pl.loop(folds + lag - depth, steps)
    def _(t):
        sent(t)

    @pl.loop(folds, steps)
    def _(a):
        @pl.when(jnp.logical_and(a % n < n - 1, jnp.logical_not(is_kept(a, a % n))))
        def _():
            received(a)

    for m in range(req_local - 1):
        result(m).wait()


def send(lens, c_raw, k_raw, gain, cos, sin, q_lat, q_rope, n):
    req_local, heads, _ = q_lat.shape
    requests, block, rank = c_raw.shape
    width = k_raw.shape[1]
    rows = block // PIECES
    total = rows + rows * width // rank
    depth = ROUNDS * n
    return pl.pallas_call(
        functools.partial(send_kernel, n, req_local, (rank + width) ** -0.5),
        in_specs=[HBM, HBM, HBM, VMEM] + [HBM] * 4,
        out_specs=[HBM] * (1 + len(LATE)),
        out_shape=[jax.ShapeDtypeStruct((req_local, n, PIECES, total, rank), jnp.bfloat16)]
        + [jax.ShapeDtypeStruct((count, total, rank), jnp.bfloat16) for count in LATE],
        scratch_shapes=[
            pltpu.VMEM((LOADS, rows, rank), jnp.bfloat16),
            pltpu.VMEM((LOADS, width, rows), jnp.bfloat16),
            pltpu.VMEM((depth, total, rank), jnp.bfloat16),
            pltpu.SemaphoreType.DMA((LOADS,)),
            pltpu.SemaphoreType.DMA((LOADS,)),
            pltpu.SemaphoreType.DMA((depth,)),
            pltpu.SemaphoreType.DMA((req_local * PIECES * n,)),
            pltpu.VMEM((heads, 1), jnp.float32),
            pltpu.VMEM((heads, 1), jnp.float32),
            pltpu.VMEM((heads, rank), jnp.float32),
            pltpu.VMEM((AHEAD + 1, total, rank), jnp.bfloat16),
            pltpu.VMEM((width, rows), jnp.bfloat16),
            pltpu.SemaphoreType.DMA((AHEAD + 1,)),
            pltpu.VMEM((req_local - 1, heads, rank), jnp.bfloat16),
            pltpu.SemaphoreType.DMA((req_local - 1,)),
            pltpu.SMEM(lens.shape, lens.dtype),
            pltpu.VMEM(cos.shape, cos.dtype),
            pltpu.VMEM(sin.shape, sin.dtype),
            pltpu.VMEM(q_lat.shape, q_lat.dtype),
            pltpu.VMEM(q_rope.shape, q_rope.dtype),
            pltpu.SemaphoreType.DMA((5,)),
        ],
        compiler_params=pltpu.CompilerParams(vmem_limit_bytes=VMEM_BYTES, collective_id=0, has_side_effects=True),
        cost_estimate=pl.CostEstimate(flops=requests * block * rank * 100, bytes_accessed=requests * block * rank * 4, transcendentals=0),
        name="send",
    )(lens, c_raw, k_raw, gain, cos, sin, q_lat, q_rope)


def stream(steps, place, first_piece, pieces, scale, length, land_ref, queries, c_out, kr_out, state, zero_c, zero_k, ring, ahead):
    buf, in_sem, kr_buf, c_sem, k_sem = ring
    depth = buf.shape[0]
    rank = buf.shape[3]
    width = kr_buf.shape[1]
    rows = kr_buf.shape[2] // pieces

    def first(t):
        return pl.multiple_of((place(t)[1] * PIECES + first_piece) * rows, rows)

    def used(t):
        return first(t) < length(place(t)[0])

    def load(t):
        req, src = place(t)
        return pltpu.make_async_copy(land_ref.at[req, src, pl.ds(first_piece, pieces)], buf.at[t % depth], in_sem.at[t % depth])

    def writes(t, c_of, kr):
        slot, req, at = t % depth, place(t)[0], first(t)
        return [pltpu.make_async_copy(c_of(h), c_out.at[req, pl.ds(at + h * rows, rows), :], c_sem.at[slot, h]) for h in range(pieces)] + [
            pltpu.make_async_copy(kr, kr_out.at[req, :, pl.ds(at, pieces * rows)], k_sem.at[slot])]

    def stores(t):
        return writes(t, lambda h: buf.at[t % depth, h, pl.ds(0, rows), :], kr_buf.at[t % depth])

    def blanks(t):
        return writes(t, lambda h: zero_c, zero_k.at[:, pl.ds(0, pieces * rows)])

    def fetch(t):
        @pl.when(used(t))
        def _():
            load(t).start()

    def work(t):
        slot = t % depth
        load(t).wait()
        for h in range(pieces):
            for kr_rows, kr_cols, from_rows, from_cols in rope_tiles(width, rows):
                cols = slice(h * rows + kr_cols.start, h * rows + kr_cols.stop)
                kr_buf[slot, kr_rows, cols] = buf[slot, h, from_rows, from_cols]
        for c in stores(t):
            c.start()
        if queries is not None:
            qa, qr = queries()
            blocks = [(buf[slot, h, :rows, :], kr_buf[slot, :, h * rows : (h + 1) * rows]) for h in range(pieces)]
            fold(state, qa, qr, blocks, [first(t) + h * rows for h in range(pieces)], length(place(t)[0]), scale)

    def body(t):
        @pl.when(used(t))
        def _():
            work(t)

        @pl.when(jnp.logical_not(used(t)))
        def _():
            for c in blanks(t):
                c.start()

        @pl.when(t + ahead < steps)
        def _():
            @pl.when(t + ahead >= depth)
            def _():
                for c in stores(t + ahead - depth):
                    c.wait()

            fetch(t + ahead)

    def prologue():
        for t in range(min(ahead, steps)):
            fetch(t)

    def drain():
        @pl.loop(max(steps - depth, 0), steps)
        def _(t):
            for c in stores(t):
                c.wait()

    return steps, prologue, body, drain


def first_kernel(n, req_local, scale, lens_ref, land_ref, qa_ref, qr_ref, c_out, kr_out, o_out, part_out,
                 m_ref, l_ref, acc_ref, part_ref, part_sem, zero_c, zero_k, o_buf, o_in_sem, o_out_sem, *rings):
    length = lambda m: lens_ref[lax.axis_index("x") * req_local + m]
    state = (m_ref, l_ref, acc_ref)
    last = req_local - 1
    rank = acc_ref.shape[1]
    me = lax.axis_index("x")
    across = len(LATE) - 1
    queries = lambda: (qa_ref[last], qr_ref[last])
    common = (scale, length, land_ref)
    outs = (c_out, kr_out, state, zero_c, zero_k)
    main = stream(last * n, lambda t: (t // n, t % n), 0, PIECES, *common, None, *outs, rings[:5], RING // 2)
    front = stream(1, lambda t: (last, move(me, across, n, -1)), 0, PIECES - LATE[across], *common, queries, *outs, rings[5:10], 1)
    back = stream(n - len(LATE), lambda t: (last, move(me, len(LATE) + t, n, -1)), 0, PIECES, *common, queries, *outs, rings[10:], n - len(LATE))
    results = [(pltpu.make_async_copy(result_place(land_ref, m, n).at[pl.ds(0, o_buf.shape[1]), :], o_buf.at[m], o_in_sem.at[m]),
                pltpu.make_async_copy(o_buf.at[m], o_out.at[m], o_out_sem.at[m])) for m in range(last)]

    for part in (front, back, main):
        part[1]()
    for take, _ in results:
        take.start()
    zero_c[...] = jnp.zeros_like(zero_c)
    zero_k[...] = jnp.zeros_like(zero_k)
    clear(state)
    steps = main[0]

    @pl.loop(0, steps)
    def _(t):
        main[2](t)

        every = steps // back[0]

        @pl.when(t % every == 0)
        def _():
            back[2](t // every)

        @pl.when(t == every // 2)
        def _():
            front[2](0)

    for take, give in results:
        take.wait()
        give.start()
    part_ref[:, :rank] = acc_ref[...]
    part_ref[:, rank : rank + LANES] = jnp.broadcast_to(m_ref[...], (part_ref.shape[0], LANES))
    part_ref[:, rank + LANES :] = jnp.broadcast_to(l_ref[...], (part_ref.shape[0], LANES))
    copy = pltpu.make_async_copy(part_ref, part_out, part_sem)
    copy.start()
    copy.wait()
    for part in (main, front, back):
        part[3]()
    for _, give in results:
        give.wait()


def last_kernel(n, req_local, scale, lens_ref, *refs):
    land_refs, refs = refs[: len(LATE)], refs[len(LATE) :]
    qa_ref, qr_ref, part_ref, c_old, kr_old, o_old, c_out, kr_out, o_out, *refs = refs
    m_ref, l_ref, acc_ref, o_buf, o_sem, kr_buf, c_sem, k_sem = refs
    last = req_local - 1
    length = lens_ref[lax.axis_index("x") * req_local + last]
    state = (m_ref, l_ref, acc_ref)
    rank = acc_ref.shape[1]
    width = kr_buf.shape[1]
    rows = kr_buf.shape[2]
    pieces = late_pieces()
    firsts = [pl.multiple_of((move(lax.axis_index("x"), j, n, -1) * PIECES + h) * rows, rows) for j, h in pieces]
    pieces = [(j, h - PIECES + LATE[j]) for j, h in pieces]
    clear(state)
    stores = []
    for at in range(0, len(pieces), BATCH):
        batch = range(at, min(at + BATCH, len(pieces)))
        for i in batch:
            (k, h), first = pieces[i], firsts[i]
            stores.append(pltpu.make_async_copy(land_refs[k].at[h, pl.ds(0, rows), :], c_out.at[last, pl.ds(first, rows), :], c_sem.at[i, 0]))
            stores[-1].start()
            for kr_rows, kr_cols, from_rows, from_cols in rope_tiles(width, rows):
                kr_buf[i, kr_rows, kr_cols] = land_refs[k][h, from_rows, from_cols]
            stores.append(pltpu.make_async_copy(kr_buf.at[i], kr_out.at[last, :, pl.ds(first, rows)], k_sem.at[i]))
            stores[-1].start()

        @pl.when(functools.reduce(jnp.minimum, [firsts[i] for i in batch]) < length)
        def _():
            blocks = [(land_refs[pieces[i][0]][pieces[i][1], :rows, :], kr_buf[i]) for i in batch]
            fold(state, qa_ref[last], qr_ref[last], blocks, [firsts[i] for i in batch], length, scale)

    m_part, l_part, acc_part = part_ref[:, rank : rank + 1], part_ref[:, rank + LANES : rank + LANES + 1], part_ref[:, :rank]
    m_new = jnp.maximum(m_ref[...], m_part)
    here, there = jnp.exp(m_ref[...] - m_new), jnp.exp(m_part - m_new)
    total = l_ref[...] * here + l_part * there
    o_buf[...] = ((acc_ref[...] * here + acc_part * there) / total).astype(jnp.bfloat16)
    copy = pltpu.make_async_copy(o_buf, o_out.at[last], o_sem)
    copy.start()
    for c in stores + [copy]:
        c.wait()


def attend(lens, landed, rest, q_lat, q_rope, n, block):
    req_local, heads, rank = q_lat.shape
    width = q_rope.shape[1]
    rows = block // PIECES
    total = rest[0].shape[1]
    late = len(late_pieces())
    scale = (rank + width) ** -0.5
    caches = [jax.ShapeDtypeStruct((req_local, n * block, rank), jnp.bfloat16),
              jax.ShapeDtypeStruct((req_local, width, n * block), jnp.bfloat16),
              jax.ShapeDtypeStruct((req_local, heads, rank), jnp.bfloat16)]
    part = jax.ShapeDtypeStruct((heads, rank + 2 * LANES), jnp.float32)
    state = [pltpu.VMEM((heads, 1), jnp.float32), pltpu.VMEM((heads, 1), jnp.float32), pltpu.VMEM((heads, rank), jnp.float32)]

    def stores(depth, pieces):
        return [pltpu.VMEM((depth, width, pieces * rows), jnp.bfloat16), pltpu.SemaphoreType.DMA((depth, pieces)), pltpu.SemaphoreType.DMA((depth,))]

    def ring(depth, pieces):
        return [pltpu.VMEM((depth, pieces, total, rank), jnp.bfloat16), pltpu.SemaphoreType.DMA((depth,))] + stores(depth, pieces)

    params = pltpu.CompilerParams(vmem_limit_bytes=ATTEND_BYTES)
    flops = 2 * req_local * n * block * heads * rank
    *outs, first_part = pl.pallas_call(
        functools.partial(first_kernel, n, req_local, scale),
        in_specs=[SMEM, HBM, VMEM, VMEM],
        out_specs=[HBM] * 4,
        out_shape=caches + [part],
        scratch_shapes=state + [pltpu.VMEM(part.shape, part.dtype), pltpu.SemaphoreType.DMA,
                                pltpu.VMEM((rows, rank), jnp.bfloat16), pltpu.VMEM((width, block), jnp.bfloat16),
                                pltpu.VMEM((req_local - 1, heads, rank), jnp.bfloat16),
                                pltpu.SemaphoreType.DMA((req_local - 1,)), pltpu.SemaphoreType.DMA((req_local - 1,))]
        + ring(RING, PIECES) + ring(1, PIECES - LATE[-1]) + ring(n - len(LATE), PIECES),
        compiler_params=params,
        cost_estimate=pl.CostEstimate(flops=flops, bytes_accessed=req_local * n * block * rank * 4, transcendentals=0),
        name="attend_first",
    )(lens, landed, q_lat, q_rope)
    return pl.pallas_call(
        functools.partial(last_kernel, n, req_local, scale),
        in_specs=[SMEM] + [VMEM] * (len(LATE) + 3) + [HBM] * 3,
        out_specs=[HBM] * 3,
        out_shape=caches,
        scratch_shapes=state + [pltpu.VMEM((heads, rank), jnp.bfloat16), pltpu.SemaphoreType.DMA] + stores(late, 1),
        input_output_aliases={len(LATE) + 4 + k: k for k in range(3)},
        compiler_params=params,
        cost_estimate=pl.CostEstimate(flops=flops // req_local // PIECES, bytes_accessed=n * block * rank * 2, transcendentals=0),
        name="attend_last",
    )(lens, *rest, q_lat, q_rope, first_part, *outs)


def solution(mesh):
    seq_spec = P("dp", "x", None)
    req_spec = P(("dp", "x"), None, None)
    n = mesh.shape["x"]

    def local_step(c_raw, k_raw, norm_gain, rope_cos, rope_sin, seq_lens, q_lat, q_rope):
        q_rope = jnp.swapaxes(q_rope, 1, 2)
        landed, *rest = send(seq_lens, c_raw, jnp.swapaxes(k_raw, 1, 2), norm_gain, rope_cos.T, rope_sin.T, q_lat, q_rope, n)
        rest = [lax.ppermute(pieces, "x", [(i, move(i, j, n, 1)) for i in range(n)]) for j, pieces in enumerate(rest)]
        c_cache, kr_cache, o_lat = attend(seq_lens, landed, rest, q_lat, q_rope, n, c_raw.shape[1])
        return c_cache, jnp.swapaxes(kr_cache, 1, 2), o_lat

    return jax.shard_map(local_step, mesh=mesh, in_specs=(seq_spec, seq_spec, P(None), P("x", None), P("x", None), P("dp"), req_spec, req_spec), out_specs=(req_spec, req_spec, req_spec), check_vma=False)
```

```python
import functools

import jax
import jax.numpy as jnp
from jax import lax
from jax.experimental import pallas as pl
from jax.experimental.pallas import tpu as pltpu
from jax.sharding import PartitionSpec as P

NORM_EPS = 1e-6
PIECES = 3
ROUNDS = 6
LOADS = 4
RING = 20
LATE_STEPS = 2
LATE = 4
AHEAD = 3
STRIPE = 128
LANES, SUBLANES = 128, 16
VMEM_BYTES = 60 * 1024 * 1024
ATTEND_BYTES = 44 * 1024 * 1024
MESH = pl.DeviceIdType.MESH
HBM = pl.BlockSpec(memory_space=pltpu.HBM)
VMEM = pl.BlockSpec(memory_space=pltpu.VMEM)
SMEM = pl.BlockSpec(memory_space=pltpu.SMEM)


def move(me, j, n, way):
    chip, core = me // 2, me % 2
    far = j % 3
    last = j // (n - 2)
    other = (j // 3) % 2 * (1 - last) + last * (1 - j % (n - 2))
    there = (core + other) % 2
    sender = core if way == 1 else there
    hop = (1 - last) * (1 + 2 * far - 3 * (far // 2)) * (1 - 2 * sender)
    return (chip + n // 2 + way * hop) % (n // 2) * 2 + there


def peer(j, n):
    return move(lax.axis_index("x"), j, n, 1)


def result_place(land_ref, m, n):
    return land_ref.at[land_ref.shape[0] - 1, move(lax.axis_index("x"), m // PIECES, n, -1), m % PIECES]


def rope_tiles(width, rows):
    for r in range(width // SUBLANES):
        for c in range(rows // LANES):
            yield (slice(r * SUBLANES, (r + 1) * SUBLANES), slice(c * LANES, (c + 1) * LANES),
                   slice(rows + c * SUBLANES, rows + (c + 1) * SUBLANES), slice(r * LANES, (r + 1) * LANES))


def clear(state):
    m_ref, l_ref, acc_ref = state
    m_ref[...] = jnp.full_like(m_ref, -1e30)
    l_ref[...] = jnp.zeros_like(l_ref)
    acc_ref[...] = jnp.zeros_like(acc_ref)


def fold(state, qa, qr, pieces, firsts, length, scale):
    m_ref, l_ref, acc_ref = state
    scores = []
    for first, (lat, kr) in zip(firsts, pieces):
        s = lax.dot_general(qa, lat, (((1,), (1,)), ((), ())), preferred_element_type=jnp.float32)
        s = s + lax.dot_general(qr, kr, (((0,), (0,)), ((), ())), preferred_element_type=jnp.float32)
        rows = lat.shape[0]
        pos = first + lax.broadcasted_iota(jnp.int32, (1, rows), 1)
        scores.append(jnp.where(pos < length, s * scale, -1e30))
    m_old = m_ref[...]
    m_new = m_old
    for s in scores:
        m_new = jnp.maximum(m_new, jnp.max(s, axis=-1, keepdims=True))
    alpha = jnp.exp(m_old - m_new)
    total, acc = l_ref[...] * alpha, acc_ref[...] * alpha
    for s, (lat, _) in zip(scores, pieces):
        p = jnp.exp(s - m_new)
        total = total + jnp.sum(p, axis=-1, keepdims=True)
        acc = acc + jnp.dot(p.astype(jnp.bfloat16), lat, preferred_element_type=jnp.float32)
    m_ref[...], l_ref[...], acc_ref[...] = m_new, total, acc


def hand_over(state, part_ref):
    m_ref, l_ref, acc_ref = state
    heads, rank = acc_ref.shape
    part_ref[:, :rank] = acc_ref[...]
    part_ref[:, rank : rank + LANES] = jnp.broadcast_to(m_ref[...], (heads, LANES))
    part_ref[:, rank + LANES :] = jnp.broadcast_to(l_ref[...], (heads, LANES))


def finish(state, part_ref):
    m_ref, l_ref, acc_ref = state
    rank = acc_ref.shape[1]
    m_part, l_part, acc_part = part_ref[:, rank : rank + 1], part_ref[:, rank + LANES : rank + LANES + 1], part_ref[:, :rank]
    m_new = jnp.maximum(m_ref[...], m_part)
    here, there = jnp.exp(m_ref[...] - m_new), jnp.exp(m_part - m_new)
    total = l_ref[...] * here + l_part * there
    return ((acc_ref[...] * here + acc_part * there) / total).astype(jnp.bfloat16)


def send_kernel(n, req_local, scale, lens_hbm, c_hbm, k_hbm, gain_ref, cos_hbm, sin_hbm, qa_hbm, qr_hbm, land_ref, *scratch):
    part_out, rest_refs, scratch = scratch[0], scratch[1 : 1 + LATE_STEPS], scratch[1 + LATE_STEPS :]
    c_buf, k_buf, out_buf, c_sem, k_sem, send_sem, recv_sem, m_ref, l_ref, acc_ref, fold_buf, kr_buf, fold_sem, o_buf, o_sem, part_ref, part_sem, *tables = scratch
    lens_ref, cos_ref, sin_ref, qa_ref, qr_ref, table_sem = tables
    me = lax.axis_index("x")
    rounds = req_local * PIECES
    steps = rounds * n
    early = (rounds - LATE) * n
    depth = out_buf.shape[0]
    rows, rank = c_buf.shape[1:]
    width = k_buf.shape[1]

    def step(t):
        q = t % n
        last = q // (n - 2)
        return (1 - last) * ((q + 2 * (me % 2)) % (n - 2)) + last * q

    def load(t):
        req = peer(step(t), n) * req_local + t // n // PIECES
        first = pl.multiple_of(t // n % PIECES * rows, rows)
        slot = t % LOADS
        return (pltpu.make_async_copy(c_hbm.at[req, pl.ds(first, rows), :], c_buf.at[slot], c_sem.at[slot]),
                pltpu.make_async_copy(k_hbm.at[req, :, pl.ds(first, rows)], k_buf.at[slot], k_sem.at[slot]))

    def landing(t):
        return land_ref.at[t // n // PIECES, me, t // n % PIECES]

    def remote(t):
        slot = t % depth
        return pltpu.make_async_remote_copy(
            src_ref=out_buf.at[slot], dst_ref=landing(t), send_sem=send_sem.at[slot],
            recv_sem=recv_sem.at[t // n * n + me], device_id={"x": peer(step(t), n)}, device_id_type=MESH)

    def own(t):
        return pltpu.make_async_copy(out_buf.at[t % depth], landing(t), send_sem.at[t % depth])

    def keep(t, j):
        return pltpu.make_async_copy(out_buf.at[t % depth], rest_refs[j].at[(t - early) // n], send_sem.at[t % depth])

    def is_kept(t, way):
        return jnp.logical_and(t >= early, way < LATE_STEPS)

    def on_kind(t, act_remote, act_local):
        is_own = t % n == n - 1

        for j in range(LATE_STEPS):
            @pl.when(jnp.logical_and(t >= early, step(t) == j))
            def _():
                act_local(keep(t, j))

        @pl.when(is_own)
        def _():
            act_local(own(t))

        @pl.when(jnp.logical_not(jnp.logical_or(is_own, is_kept(t, step(t)))))
        def _():
            act_remote(remote(t))

    def start(t):
        on_kind(t, lambda c: c.start(), lambda c: c.start())

    def sent(t):
        on_kind(t, lambda c: c.wait_send(), lambda c: c.wait())

    def pack(t):
        for c in load(t):
            c.wait()
        slot, out = t % LOADS, t % depth
        first = t // n % PIECES * rows
        left = lens_ref[peer(step(t), n) * req_local + t // n // PIECES] - me * (rows * PIECES) - first
        gain = gain_ref[...].astype(jnp.float32)

        @pl.loop(0, rows, step=STRIPE)
        def _(r):
            r = pl.multiple_of(r, STRIPE)
            lat = c_buf[slot, pl.ds(r, STRIPE), :].astype(jnp.float32)
            inv = lax.rsqrt(jnp.mean(lat * lat, axis=-1, keepdims=True) + NORM_EPS)
            valid = r + lax.broadcasted_iota(jnp.int32, (STRIPE, 1), 0) < left
            out_buf[out, pl.ds(r, STRIPE), :] = jnp.where(valid, lat * inv * gain, 0.0).astype(jnp.bfloat16)

        key = k_buf[slot].astype(jnp.float32)
        half = width // 2
        lo, hi = key[:half], key[half:]
        first = pl.multiple_of(first, LANES)
        cos, sin = cos_ref[:, pl.ds(first, rows)], sin_ref[:, pl.ds(first, rows)]
        valid = lax.broadcasted_iota(jnp.int32, (1, rows), 1) < left
        rotated = (jnp.where(valid, lo * cos - hi * sin, 0.0).astype(jnp.bfloat16),
                   jnp.where(valid, hi * cos + lo * sin, 0.0).astype(jnp.bfloat16))
        for kr_rows, kr_cols, to_rows, to_cols in rope_tiles(width, rows):
            part, at = kr_rows.start // half, kr_rows.start % half
            out_buf[out, to_rows, to_cols] = rotated[part][at : at + SUBLANES, kr_cols]

    barrier = pltpu.get_barrier_semaphore()
    for j in range(n - 1):
        pl.semaphore_signal(barrier, inc=1, device_id={"x": peer(j, n)}, device_id_type=MESH)
    fills = [pltpu.make_async_copy(src, dst, table_sem.at[i]) for i, (src, dst) in enumerate(
        zip((lens_hbm, cos_hbm, sin_hbm, qa_hbm, qr_hbm), (lens_ref, cos_ref, sin_ref, qa_ref, qr_ref)))]
    for c in fills[:3]:
        c.start()
    for t in range(LOADS):
        for c in load(t):
            c.start()
    for c in fills[3:]:
        c.start()
    for c in fills[:3]:
        c.wait()
    pack(0)
    for c in load(LOADS):
        c.start()
    for c in fills[3:]:
        c.wait()
    pl.semaphore_wait(barrier, n - 1)

    state = (m_ref, l_ref, acc_ref)
    per_req = PIECES * n
    folds = (req_local - 1) * per_req
    lag = depth + n

    def received(a):
        src = peer(a % n, n)
        piece = land_ref.at[a // per_req, src, a // n % PIECES]
        pltpu.make_async_remote_copy(
            src_ref=piece, dst_ref=piece, send_sem=send_sem.at[0], recv_sem=recv_sem.at[a // n * n + src],
            device_id={"x": src}, device_id_type=MESH).wait_recv()

    def result(m):
        return pltpu.make_async_copy(o_buf.at[m], result_place(land_ref, m, n).at[pl.ds(0, o_buf.shape[1]), :], o_sem.at[m])

    def fetch(a):
        return pltpu.make_async_copy(land_ref.at[a // per_req, peer(a % n, n), a // n % PIECES], fold_buf.at[a % (AHEAD + 1)], fold_sem.at[a % (AHEAD + 1)])

    @pl.loop(1, folds + lag)
    def _(t):
        @pl.when(t >= depth)
        def _():
            sent(t - depth)

        @pl.when(t < steps)
        def _():
            pack(t)

            @pl.when(t + LOADS < steps)
            def _():
                for c in load(t + LOADS):
                    c.start()

        @pl.when(t <= steps)
        def _():
            start(t - 1)

        arriving = t - lag + AHEAD

        @pl.when(jnp.logical_and(arriving >= 0, arriving < folds))
        def _():
            @pl.when(jnp.logical_and(arriving % n < n - 1, jnp.logical_not(is_kept(arriving, arriving % n))))
            def _():
                received(arriving)

            @pl.when(jnp.logical_not(is_kept(arriving, arriving % n)))
            def _():
                fetch(arriving).start()

        a = t - lag

        @pl.when(a >= 0)
        def _():
            m, src, slot = a // per_req, peer(a % n, n), a % (AHEAD + 1)

            @pl.when(a % per_req == 0)
            def _():
                clear(state)

            @pl.when(jnp.logical_not(is_kept(a, a % n)))
            def _():
                fetch(a).wait()
                for kr_rows, kr_cols, from_rows, from_cols in rope_tiles(width, rows):
                    kr_buf[kr_rows, kr_cols] = fold_buf[slot, from_rows, from_cols]
                first = (src * PIECES + a // n % PIECES) * rows
                fold(state, qa_ref[m], qr_ref[m], [(fold_buf[slot, :rows, :], kr_buf[...])], [first], lens_ref[me * req_local + m], scale)

            @pl.when(jnp.logical_and(a % per_req == per_req - 1, m < req_local - 2))
            def _():
                o_buf[m] = (acc_ref[...] / l_ref[...]).astype(jnp.bfloat16)
                result(m).start()

    @pl.loop(folds + lag - depth, steps)
    def _(t):
        sent(t)

    @pl.loop(folds, steps)
    def _(a):
        @pl.when(jnp.logical_and(a % n < n - 1, jnp.logical_not(is_kept(a, a % n))))
        def _():
            received(a)

    hand_over(state, part_ref)
    copy = pltpu.make_async_copy(part_ref, part_out, part_sem)
    copy.start()
    for m in range(req_local - 2):
        result(m).wait()
    copy.wait()


def send(lens, c_raw, k_raw, gain, cos, sin, q_lat, q_rope, n):
    req_local, heads, _ = q_lat.shape
    requests, block, rank = c_raw.shape
    width = k_raw.shape[1]
    rows = block // PIECES
    total = rows + rows * width // rank
    depth = ROUNDS * n
    return pl.pallas_call(
        functools.partial(send_kernel, n, req_local, (rank + width) ** -0.5),
        in_specs=[HBM, HBM, HBM, VMEM] + [HBM] * 4,
        out_specs=[HBM] * (2 + LATE_STEPS),
        out_shape=[jax.ShapeDtypeStruct((req_local, n, PIECES, total, rank), jnp.bfloat16)]
        + [jax.ShapeDtypeStruct((heads, rank + 2 * LANES), jnp.float32)]
        + [jax.ShapeDtypeStruct((LATE, total, rank), jnp.bfloat16)] * LATE_STEPS,
        scratch_shapes=[
            pltpu.VMEM((LOADS, rows, rank), jnp.bfloat16),
            pltpu.VMEM((LOADS, width, rows), jnp.bfloat16),
            pltpu.VMEM((depth, total, rank), jnp.bfloat16),
            pltpu.SemaphoreType.DMA((LOADS,)),
            pltpu.SemaphoreType.DMA((LOADS,)),
            pltpu.SemaphoreType.DMA((depth,)),
            pltpu.SemaphoreType.DMA((req_local * PIECES * n,)),
            pltpu.VMEM((heads, 1), jnp.float32),
            pltpu.VMEM((heads, 1), jnp.float32),
            pltpu.VMEM((heads, rank), jnp.float32),
            pltpu.VMEM((AHEAD + 1, total, rank), jnp.bfloat16),
            pltpu.VMEM((width, rows), jnp.bfloat16),
            pltpu.SemaphoreType.DMA((AHEAD + 1,)),
            pltpu.VMEM((req_local - 2, heads, rank), jnp.bfloat16),
            pltpu.SemaphoreType.DMA((req_local - 2,)),
            pltpu.VMEM((heads, rank + 2 * LANES), jnp.float32),
            pltpu.SemaphoreType.DMA,
            pltpu.SMEM(lens.shape, lens.dtype),
            pltpu.VMEM(cos.shape, cos.dtype),
            pltpu.VMEM(sin.shape, sin.dtype),
            pltpu.VMEM(q_lat.shape, q_lat.dtype),
            pltpu.VMEM(q_rope.shape, q_rope.dtype),
            pltpu.SemaphoreType.DMA((5,)),
        ],
        compiler_params=pltpu.CompilerParams(vmem_limit_bytes=VMEM_BYTES, collective_id=0, has_side_effects=True),
        cost_estimate=pl.CostEstimate(flops=requests * block * rank * 100, bytes_accessed=requests * block * rank * 4, transcendentals=0),
        name="send",
    )(lens, c_raw, k_raw, gain, cos, sin, q_lat, q_rope)


def stream(steps, place, first_piece, pieces, scale, length, land_ref, queries, c_out, kr_out, state, zero_c, zero_k, ring, ahead):
    buf, in_sem, kr_buf, c_sem, k_sem = ring
    depth = buf.shape[0]
    rank = buf.shape[3]
    width = kr_buf.shape[1]
    rows = kr_buf.shape[2] // pieces

    def first(t):
        return pl.multiple_of((place(t)[1] * PIECES + first_piece) * rows, rows)

    def used(t):
        return first(t) < length(place(t)[0])

    def load(t):
        req, src = place(t)
        return pltpu.make_async_copy(land_ref.at[req, src, pl.ds(first_piece, pieces)], buf.at[t % depth], in_sem.at[t % depth])

    def writes(t, c_of, kr):
        slot, req, at = t % depth, place(t)[0], first(t)
        return [pltpu.make_async_copy(c_of(h), c_out.at[req, pl.ds(at + h * rows, rows), :], c_sem.at[slot, h]) for h in range(pieces)] + [
            pltpu.make_async_copy(kr, kr_out.at[req, :, pl.ds(at, pieces * rows)], k_sem.at[slot])]

    def stores(t):
        return writes(t, lambda h: buf.at[t % depth, h, pl.ds(0, rows), :], kr_buf.at[t % depth])

    def blanks(t):
        return writes(t, lambda h: zero_c, zero_k.at[:, pl.ds(0, pieces * rows)])

    def fetch(t):
        @pl.when(used(t))
        def _():
            load(t).start()

    def work(t):
        slot = t % depth
        load(t).wait()
        for h in range(pieces):
            for kr_rows, kr_cols, from_rows, from_cols in rope_tiles(width, rows):
                cols = slice(h * rows + kr_cols.start, h * rows + kr_cols.stop)
                kr_buf[slot, kr_rows, cols] = buf[slot, h, from_rows, from_cols]
        for c in stores(t):
            c.start()
        if queries is not None:
            qa, qr = queries()
            blocks = [(buf[slot, h, :rows, :], kr_buf[slot, :, h * rows : (h + 1) * rows]) for h in range(pieces)]
            fold(state, qa, qr, blocks, [first(t) + h * rows for h in range(pieces)], length(place(t)[0]), scale)

    def body(t):
        @pl.when(used(t))
        def _():
            work(t)

        @pl.when(jnp.logical_not(used(t)))
        def _():
            for c in blanks(t):
                c.start()

        @pl.when(t + ahead < steps)
        def _():
            @pl.when(t + ahead >= depth)
            def _():
                for c in stores(t + ahead - depth):
                    c.wait()

            fetch(t + ahead)

    def prologue():
        for t in range(min(ahead, steps)):
            fetch(t)

    def drain():
        @pl.loop(max(steps - depth, 0), steps)
        def _(t):
            for c in stores(t):
                c.wait()

    return steps, prologue, body, drain


def first_kernel(n, req_local, scale, lens_ref, land_ref, qa_ref, qr_ref, c_out, kr_out, o_out, part_out,
                 m_ref, l_ref, acc_ref, part_ref, part_sem, zero_c, zero_k, o_buf, o_in_sem, o_out_sem, *rings):
    length = lambda m: lens_ref[lax.axis_index("x") * req_local + m]
    state = (m_ref, l_ref, acc_ref)
    last = req_local - 1
    rank = acc_ref.shape[1]
    me = lax.axis_index("x")
    queries = lambda: (qa_ref[last], qr_ref[last])
    common = (scale, length, land_ref)
    outs = (c_out, kr_out, state, zero_c, zero_k)
    whole = (last - 1) * n
    after = lambda t: move(me, LATE_STEPS + t, n, -1)

    def place(t):
        tail = t // whole
        return t // n * (1 - tail) + (last - 1) * tail, t % n * (1 - tail) + after(t - whole * tail) * tail

    main = stream(whole + n - LATE_STEPS, place, 0, PIECES, *common, None, *outs, rings[:5], RING // 2)
    front = stream(LATE_STEPS, lambda t: (last - 1, move(me, t, n, -1)), 0, 2 * PIECES - LATE, *common, None, *outs, rings[5:10], LATE_STEPS)
    back = stream(n - LATE_STEPS, lambda t: (last, after(t)), 0, PIECES, *common, queries, *outs, rings[10:], n - LATE_STEPS)
    results = [(pltpu.make_async_copy(result_place(land_ref, m, n).at[pl.ds(0, o_buf.shape[1]), :], o_buf.at[m], o_in_sem.at[m]),
                pltpu.make_async_copy(o_buf.at[m], o_out.at[m], o_out_sem.at[m])) for m in range(last - 1)]

    for part in (front, back, main):
        part[1]()
    for take, _ in results:
        take.start()
    zero_c[...] = jnp.zeros_like(zero_c)
    zero_k[...] = jnp.zeros_like(zero_k)
    clear(state)
    steps = main[0]

    @pl.loop(0, steps)
    def _(t):
        main[2](t)

        every = steps // back[0]

        @pl.when(jnp.logical_and(t % every == 0, t // every < back[0]))
        def _():
            back[2](t // every)

        @pl.when(jnp.logical_and(t % every == every // 2, t // every < front[0]))
        def _():
            front[2](t // every)

    for take, give in results:
        take.wait()
        give.start()
    hand_over(state, part_ref)
    copy = pltpu.make_async_copy(part_ref, part_out, part_sem)
    copy.start()
    copy.wait()
    for part in (main, front, back):
        part[3]()
    for _, give in results:
        give.wait()


def last_kernel(n, req_local, scale, lens_ref, *refs):
    land_refs, refs = refs[:LATE_STEPS], refs[LATE_STEPS:]
    qa_ref, qr_ref, part_ref, before_ref, c_old, kr_old, o_old, c_out, kr_out, o_out, *refs = refs
    m_ref, l_ref, acc_ref, o_buf, o_sem, kr_buf, c_sem, k_sem = refs
    state = (m_ref, l_ref, acc_ref)
    width = kr_buf.shape[1]
    rows = kr_buf.shape[2]
    waits = []
    for req, rounds, part in ((req_local - 1, range(LATE - PIECES, LATE), part_ref), (req_local - 2, range(LATE - PIECES), before_ref)):
        length = lens_ref[lax.axis_index("x") * req_local + req]
        pieces = [(j, r) for j in range(LATE_STEPS) for r in rounds]
        firsts = [pl.multiple_of((move(lax.axis_index("x"), j, n, -1) * PIECES + (r - LATE) % PIECES) * rows, rows) for j, r in pieces]
        clear(state)
        for (j, r), first in zip(pieces, firsts):
            i = j * LATE + r
            waits.append(pltpu.make_async_copy(land_refs[j].at[r, pl.ds(0, rows), :], c_out.at[req, pl.ds(first, rows), :], c_sem.at[i, 0]))
            waits[-1].start()
            for kr_rows, kr_cols, from_rows, from_cols in rope_tiles(width, rows):
                kr_buf[i, kr_rows, kr_cols] = land_refs[j][r, from_rows, from_cols]
            waits.append(pltpu.make_async_copy(kr_buf.at[i], kr_out.at[req, :, pl.ds(first, rows)], k_sem.at[i]))
            waits[-1].start()

        @pl.when(functools.reduce(jnp.minimum, firsts) < length)
        def _():
            blocks = [(land_refs[j][r, :rows, :], kr_buf[j * LATE + r]) for j, r in pieces]
            fold(state, qa_ref[req], qr_ref[req], blocks, firsts, length, scale)

        at = req_local - 1 - req
        o_buf[at] = finish(state, part)
        waits.append(pltpu.make_async_copy(o_buf.at[at], o_out.at[req], o_sem.at[at]))
        waits[-1].start()
    for c in waits:
        c.wait()


def attend(lens, landed, before, rest, q_lat, q_rope, n, block):
    req_local, heads, rank = q_lat.shape
    width = q_rope.shape[1]
    rows = block // PIECES
    total = rest[0].shape[1]
    late = LATE_STEPS * LATE
    scale = (rank + width) ** -0.5
    caches = [jax.ShapeDtypeStruct((req_local, n * block, rank), jnp.bfloat16),
              jax.ShapeDtypeStruct((req_local, width, n * block), jnp.bfloat16),
              jax.ShapeDtypeStruct((req_local, heads, rank), jnp.bfloat16)]
    part = jax.ShapeDtypeStruct((heads, rank + 2 * LANES), jnp.float32)
    state = [pltpu.VMEM((heads, 1), jnp.float32), pltpu.VMEM((heads, 1), jnp.float32), pltpu.VMEM((heads, rank), jnp.float32)]

    def stores(depth, pieces):
        return [pltpu.VMEM((depth, width, pieces * rows), jnp.bfloat16), pltpu.SemaphoreType.DMA((depth, pieces)), pltpu.SemaphoreType.DMA((depth,))]

    def ring(depth, pieces):
        return [pltpu.VMEM((depth, pieces, total, rank), jnp.bfloat16), pltpu.SemaphoreType.DMA((depth,))] + stores(depth, pieces)

    params = pltpu.CompilerParams(vmem_limit_bytes=ATTEND_BYTES)
    flops = 2 * req_local * n * block * heads * rank
    *outs, first_part = pl.pallas_call(
        functools.partial(first_kernel, n, req_local, scale),
        in_specs=[SMEM, HBM, VMEM, VMEM],
        out_specs=[HBM] * 4,
        out_shape=caches + [part],
        scratch_shapes=state + [pltpu.VMEM(part.shape, part.dtype), pltpu.SemaphoreType.DMA,
                                pltpu.VMEM((rows, rank), jnp.bfloat16), pltpu.VMEM((width, block), jnp.bfloat16),
                                pltpu.VMEM((req_local - 2, heads, rank), jnp.bfloat16),
                                pltpu.SemaphoreType.DMA((req_local - 2,)), pltpu.SemaphoreType.DMA((req_local - 2,))]
        + ring(RING, PIECES) + ring(LATE_STEPS, 2 * PIECES - LATE) + ring(n - LATE_STEPS, PIECES),
        compiler_params=params,
        cost_estimate=pl.CostEstimate(flops=flops, bytes_accessed=req_local * n * block * rank * 4, transcendentals=0),
        name="attend_first",
    )(lens, landed, q_lat, q_rope)
    return pl.pallas_call(
        functools.partial(last_kernel, n, req_local, scale),
        in_specs=[SMEM] + [VMEM] * (LATE_STEPS + 4) + [HBM] * 3,
        out_specs=[HBM] * 3,
        out_shape=caches,
        scratch_shapes=state + [pltpu.VMEM((2, heads, rank), jnp.bfloat16), pltpu.SemaphoreType.DMA((2,))] + stores(late, 1),
        input_output_aliases={LATE_STEPS + 5 + k: k for k in range(3)},
        compiler_params=params,
        cost_estimate=pl.CostEstimate(flops=flops // req_local // PIECES, bytes_accessed=n * block * rank * 2, transcendentals=0),
        name="attend_last",
    )(lens, *rest, q_lat, q_rope, first_part, before, *outs)


def solution(mesh):
    seq_spec = P("dp", "x", None)
    req_spec = P(("dp", "x"), None, None)
    n = mesh.shape["x"]

    def local_step(c_raw, k_raw, norm_gain, rope_cos, rope_sin, seq_lens, q_lat, q_rope):
        q_rope = jnp.swapaxes(q_rope, 1, 2)
        landed, before, *rest = send(seq_lens, c_raw, jnp.swapaxes(k_raw, 1, 2), norm_gain, rope_cos.T, rope_sin.T, q_lat, q_rope, n)
        rest = [lax.ppermute(pieces, "x", [(i, move(i, j, n, 1)) for i in range(n)]) for j, pieces in enumerate(rest)]
        c_cache, kr_cache, o_lat = attend(seq_lens, landed, before, rest, q_lat, q_rope, n, c_raw.shape[1])
        return c_cache, jnp.swapaxes(kr_cache, 1, 2), o_lat

    return jax.shard_map(local_step, mesh=mesh, in_specs=(seq_spec, seq_spec, P(None), P("x", None), P("x", None), P("dp"), req_spec, req_spec), out_specs=(req_spec, req_spec, req_spec), check_vma=False)
```

```python
import functools

import jax
import jax.numpy as jnp
from jax import lax
from jax.experimental import pallas as pl
from jax.experimental.pallas import tpu as pltpu
from jax.sharding import PartitionSpec as P

NORM_EPS = 1e-6
PIECES = 3
ROUNDS = 6
LOADS = 4
RING = 20
LATE_STEPS = 2
LATE = 4
AHEAD = 3
STRIPE = 128
LANES, SUBLANES = 128, 16
VMEM_BYTES = 60 * 1024 * 1024
ATTEND_BYTES = 44 * 1024 * 1024
MESH = pl.DeviceIdType.MESH
HBM = pl.BlockSpec(memory_space=pltpu.HBM)
VMEM = pl.BlockSpec(memory_space=pltpu.VMEM)
SMEM = pl.BlockSpec(memory_space=pltpu.SMEM)


def move(me, j, n, way):
    chip, core = me // 2, me % 2
    far = j % 3
    last = j // (n - 2)
    other = (j // 3) % 2 * (1 - last) + last * (1 - j % (n - 2))
    there = (core + other) % 2
    sender = core if way == 1 else there
    hop = (1 - last) * (1 + 2 * far - 3 * (far // 2)) * (1 - 2 * sender)
    return (chip + n // 2 + way * hop) % (n // 2) * 2 + there


def peer(j, n):
    return move(lax.axis_index("x"), j, n, 1)


def result_place(land_ref, m, n):
    return land_ref.at[land_ref.shape[0] - 1, move(lax.axis_index("x"), m // PIECES, n, -1), m % PIECES]


def rope_tiles(width, rows):
    for r in range(width // SUBLANES):
        for c in range(rows // LANES):
            yield (slice(r * SUBLANES, (r + 1) * SUBLANES), slice(c * LANES, (c + 1) * LANES),
                   slice(rows + c * SUBLANES, rows + (c + 1) * SUBLANES), slice(r * LANES, (r + 1) * LANES))


def clear(state):
    m_ref, l_ref, acc_ref = state
    m_ref[...] = jnp.full_like(m_ref, -1e30)
    l_ref[...] = jnp.zeros_like(l_ref)
    acc_ref[...] = jnp.zeros_like(acc_ref)


def fold(state, qa, qr, pieces, firsts, length, scale):
    values = folded(*(ref[...] for ref in state), qa, qr, pieces, firsts, length, scale)
    for ref, value in zip(state, values):
        ref[...] = value


def folded(m_old, l_old, acc_old, qa, qr, pieces, firsts, length, scale):
    scores = []
    for first, (lat, kr) in zip(firsts, pieces):
        s = lax.dot_general(qa, lat, (((1,), (1,)), ((), ())), preferred_element_type=jnp.float32)
        s = s + lax.dot_general(qr, kr, (((0,), (0,)), ((), ())), preferred_element_type=jnp.float32)
        rows = lat.shape[0]
        pos = first + lax.broadcasted_iota(jnp.int32, (1, rows), 1)
        scores.append(jnp.where(pos < length, s * scale, -1e30))
    m_new = m_old
    for s in scores:
        m_new = jnp.maximum(m_new, jnp.max(s, axis=-1, keepdims=True))
    alpha = jnp.exp(m_old - m_new)
    total, acc = l_old * alpha, acc_old * alpha
    for s, (lat, _) in zip(scores, pieces):
        p = jnp.exp(s - m_new)
        total = total + jnp.sum(p, axis=-1, keepdims=True)
        acc = acc + jnp.dot(p.astype(jnp.bfloat16), lat, preferred_element_type=jnp.float32)
    return m_new, total, acc


def hand_over(state, part_ref):
    m_ref, l_ref, acc_ref = state
    heads, rank = acc_ref.shape
    part_ref[:, :rank] = acc_ref[...]
    part_ref[:, rank : rank + LANES] = jnp.broadcast_to(m_ref[...], (heads, LANES))
    part_ref[:, rank + LANES :] = jnp.broadcast_to(l_ref[...], (heads, LANES))


def send_kernel(n, req_local, scale, lens_hbm, c_hbm, k_hbm, gain_ref, cos_hbm, sin_hbm, qa_hbm, qr_hbm, land_ref, *scratch):
    part_out, rest_refs, scratch = scratch[0], scratch[1 : 1 + LATE_STEPS], scratch[1 + LATE_STEPS :]
    c_buf, k_buf, out_buf, c_sem, k_sem, send_sem, recv_sem, m_ref, l_ref, acc_ref, fold_buf, kr_buf, fold_sem, o_buf, o_sem, part_ref, part_sem, *tables = scratch
    lens_ref, cos_ref, sin_ref, qa_ref, qr_ref, table_sem = tables
    me = lax.axis_index("x")
    rounds = req_local * PIECES
    steps = rounds * n
    early = (rounds - LATE) * n
    depth = out_buf.shape[0]
    rows, rank = c_buf.shape[1:]
    width = k_buf.shape[1]

    def step(t):
        q = t % n
        last = q // (n - 2)
        return (1 - last) * ((q + 2 * (me % 2)) % (n - 2)) + last * q

    def load(t):
        req = peer(step(t), n) * req_local + t // n // PIECES
        first = pl.multiple_of(t // n % PIECES * rows, rows)
        slot = t % LOADS
        return (pltpu.make_async_copy(c_hbm.at[req, pl.ds(first, rows), :], c_buf.at[slot], c_sem.at[slot]),
                pltpu.make_async_copy(k_hbm.at[req, :, pl.ds(first, rows)], k_buf.at[slot], k_sem.at[slot]))

    def landing(t):
        return land_ref.at[t // n // PIECES, me, t // n % PIECES]

    def remote(t):
        slot = t % depth
        return pltpu.make_async_remote_copy(
            src_ref=out_buf.at[slot], dst_ref=landing(t), send_sem=send_sem.at[slot],
            recv_sem=recv_sem.at[t // n * n + me], device_id={"x": peer(step(t), n)}, device_id_type=MESH)

    def own(t):
        return pltpu.make_async_copy(out_buf.at[t % depth], landing(t), send_sem.at[t % depth])

    def keep(t, j):
        return pltpu.make_async_copy(out_buf.at[t % depth], rest_refs[j].at[(t - early) // n], send_sem.at[t % depth])

    def is_kept(t, way):
        return jnp.logical_and(t >= early, way < LATE_STEPS)

    def on_kind(t, act_remote, act_local):
        is_own = t % n == n - 1

        for j in range(LATE_STEPS):
            @pl.when(jnp.logical_and(t >= early, step(t) == j))
            def _():
                act_local(keep(t, j))

        @pl.when(is_own)
        def _():
            act_local(own(t))

        @pl.when(jnp.logical_not(jnp.logical_or(is_own, is_kept(t, step(t)))))
        def _():
            act_remote(remote(t))

    def start(t):
        on_kind(t, lambda c: c.start(), lambda c: c.start())

    def sent(t):
        on_kind(t, lambda c: c.wait_send(), lambda c: c.wait())

    def pack(t):
        for c in load(t):
            c.wait()
        slot, out = t % LOADS, t % depth
        first = t // n % PIECES * rows
        left = lens_ref[peer(step(t), n) * req_local + t // n // PIECES] - me * (rows * PIECES) - first
        gain = gain_ref[...].astype(jnp.float32)

        @pl.loop(0, rows, step=STRIPE)
        def _(r):
            r = pl.multiple_of(r, STRIPE)
            lat = c_buf[slot, pl.ds(r, STRIPE), :].astype(jnp.float32)
            inv = lax.rsqrt(jnp.mean(lat * lat, axis=-1, keepdims=True) + NORM_EPS)
            valid = r + lax.broadcasted_iota(jnp.int32, (STRIPE, 1), 0) < left
            out_buf[out, pl.ds(r, STRIPE), :] = jnp.where(valid, lat * inv * gain, 0.0).astype(jnp.bfloat16)

        key = k_buf[slot].astype(jnp.float32)
        half = width // 2
        lo, hi = key[:half], key[half:]
        first = pl.multiple_of(first, LANES)
        cos, sin = cos_ref[:, pl.ds(first, rows)], sin_ref[:, pl.ds(first, rows)]
        valid = lax.broadcasted_iota(jnp.int32, (1, rows), 1) < left
        rotated = (jnp.where(valid, lo * cos - hi * sin, 0.0).astype(jnp.bfloat16),
                   jnp.where(valid, hi * cos + lo * sin, 0.0).astype(jnp.bfloat16))
        for kr_rows, kr_cols, to_rows, to_cols in rope_tiles(width, rows):
            part, at = kr_rows.start // half, kr_rows.start % half
            out_buf[out, to_rows, to_cols] = rotated[part][at : at + SUBLANES, kr_cols]

    barrier = pltpu.get_barrier_semaphore()
    for j in range(n - 1):
        pl.semaphore_signal(barrier, inc=1, device_id={"x": peer(j, n)}, device_id_type=MESH)
    fills = [pltpu.make_async_copy(src, dst, table_sem.at[i]) for i, (src, dst) in enumerate(
        zip((lens_hbm, cos_hbm, sin_hbm, qa_hbm, qr_hbm), (lens_ref, cos_ref, sin_ref, qa_ref, qr_ref)))]
    for c in fills[:3]:
        c.start()
    for t in range(LOADS):
        for c in load(t):
            c.start()
    for c in fills[3:]:
        c.start()
    for c in fills[:3]:
        c.wait()
    pack(0)
    for c in load(LOADS):
        c.start()
    for c in fills[3:]:
        c.wait()
    pl.semaphore_wait(barrier, n - 1)

    state = (m_ref, l_ref, acc_ref)
    per_req = PIECES * n
    folds = (req_local - 1) * per_req
    lag = depth + n

    def received(a):
        src = peer(a % n, n)
        piece = land_ref.at[a // per_req, src, a // n % PIECES]
        pltpu.make_async_remote_copy(
            src_ref=piece, dst_ref=piece, send_sem=send_sem.at[0], recv_sem=recv_sem.at[a // n * n + src],
            device_id={"x": src}, device_id_type=MESH).wait_recv()

    def result(m):
        return pltpu.make_async_copy(o_buf.at[m], result_place(land_ref, m, n).at[pl.ds(0, o_buf.shape[1]), :], o_sem.at[m])

    def fetch(a):
        return pltpu.make_async_copy(land_ref.at[a // per_req, peer(a % n, n), a // n % PIECES], fold_buf.at[a % (AHEAD + 1)], fold_sem.at[a % (AHEAD + 1)])

    @pl.loop(1, folds + lag)
    def _(t):
        @pl.when(t >= depth)
        def _():
            sent(t - depth)

        @pl.when(t < steps)
        def _():
            pack(t)

            @pl.when(t + LOADS < steps)
            def _():
                for c in load(t + LOADS):
                    c.start()

        @pl.when(t <= steps)
        def _():
            start(t - 1)

        arriving = t - lag + AHEAD

        @pl.when(jnp.logical_and(arriving >= 0, arriving < folds))
        def _():
            @pl.when(jnp.logical_and(arriving % n < n - 1, jnp.logical_not(is_kept(arriving, arriving % n))))
            def _():
                received(arriving)

            @pl.when(jnp.logical_not(is_kept(arriving, arriving % n)))
            def _():
                fetch(arriving).start()

        a = t - lag

        @pl.when(a >= 0)
        def _():
            m, src, slot = a // per_req, peer(a % n, n), a % (AHEAD + 1)

            @pl.when(a % per_req == 0)
            def _():
                clear(state)

            @pl.when(jnp.logical_not(is_kept(a, a % n)))
            def _():
                fetch(a).wait()
                for kr_rows, kr_cols, from_rows, from_cols in rope_tiles(width, rows):
                    kr_buf[kr_rows, kr_cols] = fold_buf[slot, from_rows, from_cols]
                first = (src * PIECES + a // n % PIECES) * rows
                fold(state, qa_ref[m], qr_ref[m], [(fold_buf[slot, :rows, :], kr_buf[...])], [first], lens_ref[me * req_local + m], scale)

            @pl.when(jnp.logical_and(a % per_req == per_req - 1, m < req_local - 2))
            def _():
                o_buf[m] = (acc_ref[...] / l_ref[...]).astype(jnp.bfloat16)
                result(m).start()

    hand_over(state, part_ref)
    copy = pltpu.make_async_copy(part_ref, part_out, part_sem)
    copy.start()

    @pl.loop(folds + lag - depth, steps)
    def _(t):
        sent(t)

    @pl.loop(folds, steps)
    def _(a):
        @pl.when(jnp.logical_and(a % n < n - 1, jnp.logical_not(is_kept(a, a % n))))
        def _():
            received(a)

    for m in range(req_local - 2):
        result(m).wait()
    copy.wait()


def send(lens, c_raw, k_raw, gain, cos, sin, q_lat, q_rope, n):
    req_local, heads, _ = q_lat.shape
    requests, block, rank = c_raw.shape
    width = k_raw.shape[1]
    rows = block // PIECES
    total = rows + rows * width // rank
    depth = ROUNDS * n
    return pl.pallas_call(
        functools.partial(send_kernel, n, req_local, (rank + width) ** -0.5),
        in_specs=[HBM, HBM, HBM, VMEM] + [HBM] * 4,
        out_specs=[HBM] * (2 + LATE_STEPS),
        out_shape=[jax.ShapeDtypeStruct((req_local, n, PIECES, total, rank), jnp.bfloat16)]
        + [jax.ShapeDtypeStruct((heads, rank + 2 * LANES), jnp.float32)]
        + [jax.ShapeDtypeStruct((LATE, total, rank), jnp.bfloat16)] * LATE_STEPS,
        scratch_shapes=[
            pltpu.VMEM((LOADS, rows, rank), jnp.bfloat16),
            pltpu.VMEM((LOADS, width, rows), jnp.bfloat16),
            pltpu.VMEM((depth, total, rank), jnp.bfloat16),
            pltpu.SemaphoreType.DMA((LOADS,)),
            pltpu.SemaphoreType.DMA((LOADS,)),
            pltpu.SemaphoreType.DMA((depth,)),
            pltpu.SemaphoreType.DMA((req_local * PIECES * n,)),
            pltpu.VMEM((heads, 1), jnp.float32),
            pltpu.VMEM((heads, 1), jnp.float32),
            pltpu.VMEM((heads, rank), jnp.float32),
            pltpu.VMEM((AHEAD + 1, total, rank), jnp.bfloat16),
            pltpu.VMEM((width, rows), jnp.bfloat16),
            pltpu.SemaphoreType.DMA((AHEAD + 1,)),
            pltpu.VMEM((req_local - 2, heads, rank), jnp.bfloat16),
            pltpu.SemaphoreType.DMA((req_local - 2,)),
            pltpu.VMEM((heads, rank + 2 * LANES), jnp.float32),
            pltpu.SemaphoreType.DMA,
            pltpu.SMEM(lens.shape, lens.dtype),
            pltpu.VMEM(cos.shape, cos.dtype),
            pltpu.VMEM(sin.shape, sin.dtype),
            pltpu.VMEM(q_lat.shape, q_lat.dtype),
            pltpu.VMEM(q_rope.shape, q_rope.dtype),
            pltpu.SemaphoreType.DMA((5,)),
        ],
        compiler_params=pltpu.CompilerParams(vmem_limit_bytes=VMEM_BYTES, collective_id=0, has_side_effects=True),
        cost_estimate=pl.CostEstimate(flops=requests * block * rank * 100, bytes_accessed=requests * block * rank * 4, transcendentals=0),
        name="send",
    )(lens, c_raw, k_raw, gain, cos, sin, q_lat, q_rope)


def stream(steps, place, first_piece, pieces, scale, length, land_ref, queries, c_out, kr_out, state, zero_c, zero_k, ring, ahead):
    buf, in_sem, kr_buf, c_sem, k_sem = ring
    depth = buf.shape[0]
    rank = buf.shape[3]
    width = kr_buf.shape[1]
    rows = kr_buf.shape[2] // pieces

    def first(t):
        return pl.multiple_of((place(t)[1] * PIECES + first_piece) * rows, rows)

    def used(t):
        return first(t) < length(place(t)[0])

    def load(t):
        req, src = place(t)
        return pltpu.make_async_copy(land_ref.at[req, src, pl.ds(first_piece, pieces)], buf.at[t % depth], in_sem.at[t % depth])

    def writes(t, c_of, kr):
        slot, req, at = t % depth, place(t)[0], first(t)
        return [pltpu.make_async_copy(c_of(h), c_out.at[req, pl.ds(at + h * rows, rows), :], c_sem.at[slot, h]) for h in range(pieces)] + [
            pltpu.make_async_copy(kr, kr_out.at[req, :, pl.ds(at, pieces * rows)], k_sem.at[slot])]

    def stores(t):
        return writes(t, lambda h: buf.at[t % depth, h, pl.ds(0, rows), :], kr_buf.at[t % depth])

    def blanks(t):
        return writes(t, lambda h: zero_c, zero_k.at[:, pl.ds(0, pieces * rows)])

    def fetch(t):
        @pl.when(used(t))
        def _():
            load(t).start()

    def work(t):
        slot = t % depth
        load(t).wait()
        for h in range(pieces):
            for kr_rows, kr_cols, from_rows, from_cols in rope_tiles(width, rows):
                cols = slice(h * rows + kr_cols.start, h * rows + kr_cols.stop)
                kr_buf[slot, kr_rows, cols] = buf[slot, h, from_rows, from_cols]
        for c in stores(t):
            c.start()
        if queries is not None:
            qa, qr = queries()
            blocks = [(buf[slot, h, :rows, :], kr_buf[slot, :, h * rows : (h + 1) * rows]) for h in range(pieces)]
            fold(state, qa, qr, blocks, [first(t) + h * rows for h in range(pieces)], length(place(t)[0]), scale)

    def body(t):
        @pl.when(used(t))
        def _():
            work(t)

        @pl.when(jnp.logical_not(used(t)))
        def _():
            for c in blanks(t):
                c.start()

        @pl.when(t + ahead < steps)
        def _():
            @pl.when(t + ahead >= depth)
            def _():
                for c in stores(t + ahead - depth):
                    c.wait()

            fetch(t + ahead)

    def prologue():
        for t in range(min(ahead, steps)):
            fetch(t)

    def drain():
        @pl.loop(max(steps - depth, 0), steps)
        def _(t):
            for c in stores(t):
                c.wait()

    return steps, prologue, body, drain


def first_kernel(n, req_local, scale, lens_ref, land_ref, qa_ref, qr_ref, c_out, kr_out, o_out, part_out,
                 m_ref, l_ref, acc_ref, part_ref, part_sem, zero_c, zero_k, o_buf, o_in_sem, o_out_sem, *rings):
    length = lambda m: lens_ref[lax.axis_index("x") * req_local + m]
    state = (m_ref, l_ref, acc_ref)
    last = req_local - 1
    rank = acc_ref.shape[1]
    me = lax.axis_index("x")
    queries = lambda: (qa_ref[last], qr_ref[last])
    common = (scale, length, land_ref)
    outs = (c_out, kr_out, state, zero_c, zero_k)
    whole = (last - 1) * n
    after = lambda t: move(me, LATE_STEPS + t, n, -1)

    def place(t):
        tail = t // whole
        return t // n * (1 - tail) + (last - 1) * tail, t % n * (1 - tail) + after(t - whole * tail) * tail

    main = stream(whole + n - LATE_STEPS, place, 0, PIECES, *common, None, *outs, rings[:5], RING // 2)
    front = stream(LATE_STEPS, lambda t: (last - 1, move(me, t, n, -1)), 0, 2 * PIECES - LATE, *common, None, *outs, rings[5:10], LATE_STEPS)
    back = stream(n - LATE_STEPS, lambda t: (last, after(t)), 0, PIECES, *common, queries, *outs, rings[10:], n - LATE_STEPS)
    results = [(pltpu.make_async_copy(result_place(land_ref, m, n).at[pl.ds(0, o_buf.shape[1]), :], o_buf.at[m], o_in_sem.at[m]),
                pltpu.make_async_copy(o_buf.at[m], o_out.at[m], o_out_sem.at[m])) for m in range(last - 1)]

    for part in (front, back, main):
        part[1]()
    for take, _ in results:
        take.start()
    zero_c[...] = jnp.zeros_like(zero_c)
    zero_k[...] = jnp.zeros_like(zero_k)
    clear(state)
    steps = main[0]

    @pl.loop(0, steps)
    def _(t):
        main[2](t)

        every = steps // back[0]

        @pl.when(jnp.logical_and(t % every == 0, t // every < back[0]))
        def _():
            back[2](t // every)

        @pl.when(jnp.logical_and(t % every == every // 2, t // every < front[0]))
        def _():
            front[2](t // every)

    for take, give in results:
        take.wait()
        give.start()
    hand_over(state, part_ref)
    copy = pltpu.make_async_copy(part_ref, part_out, part_sem)
    copy.start()
    copy.wait()
    for part in (main, front, back):
        part[3]()
    for _, give in results:
        give.wait()


def last_kernel(n, req_local, scale, lens_ref, *refs):
    land_refs, refs = refs[:LATE_STEPS], refs[LATE_STEPS:]
    qa_ref, qr_ref, part_ref, before_ref, c_old, kr_old, o_old, c_out, kr_out, o_out, *refs = refs
    o_buf, o_sem, kr_buf, c_sem, k_sem = refs
    rank = qa_ref.shape[2]
    width = kr_buf.shape[1]
    rows = kr_buf.shape[2]
    waits = []
    groups = []
    for req, rounds, part in ((req_local - 1, range(LATE - PIECES, LATE), part_ref), (req_local - 2, range(LATE - PIECES), before_ref)):
        pieces = [(j, r) for j in range(LATE_STEPS) for r in rounds]
        firsts = [pl.multiple_of((move(lax.axis_index("x"), j, n, -1) * PIECES + (r - LATE) % PIECES) * rows, rows) for j, r in pieces]
        groups.append((req, part, pieces, firsts))
        for (j, r), first in zip(pieces, firsts):
            i = j * LATE + r
            waits.append(pltpu.make_async_copy(land_refs[j].at[r, pl.ds(0, rows), :], c_out.at[req, pl.ds(first, rows), :], c_sem.at[i, 0]))
            waits[-1].start()
            for kr_rows, kr_cols, from_rows, from_cols in rope_tiles(width, rows):
                kr_buf[i, kr_rows, kr_cols] = land_refs[j][r, from_rows, from_cols]
            waits.append(pltpu.make_async_copy(kr_buf.at[i], kr_out.at[req, :, pl.ds(first, rows)], k_sem.at[i]))
            waits[-1].start()
    for at, (req, part, pieces, firsts) in enumerate(groups):
        length = lens_ref[lax.axis_index("x") * req_local + req]
        blocks = [(land_refs[j][r, :rows, :], kr_buf[j * LATE + r]) for j, r in pieces]
        state = part[:, rank : rank + 1], part[:, rank + LANES : rank + LANES + 1], part[:, :rank]
        _, total, acc = folded(*state, qa_ref[req], qr_ref[req], blocks, firsts, length, scale)
        o_buf[at] = (acc / total).astype(jnp.bfloat16)
    for at, (req, *_) in enumerate(groups):
        waits.append(pltpu.make_async_copy(o_buf.at[at], o_out.at[req], o_sem.at[at]))
        waits[-1].start()
    for c in waits:
        c.wait()


def attend(lens, landed, before, rest, q_lat, q_rope, n, block):
    req_local, heads, rank = q_lat.shape
    width = q_rope.shape[1]
    rows = block // PIECES
    total = rest[0].shape[1]
    late = LATE_STEPS * LATE
    scale = (rank + width) ** -0.5
    caches = [jax.ShapeDtypeStruct((req_local, n * block, rank), jnp.bfloat16),
              jax.ShapeDtypeStruct((req_local, width, n * block), jnp.bfloat16),
              jax.ShapeDtypeStruct((req_local, heads, rank), jnp.bfloat16)]
    part = jax.ShapeDtypeStruct((heads, rank + 2 * LANES), jnp.float32)
    state = [pltpu.VMEM((heads, 1), jnp.float32), pltpu.VMEM((heads, 1), jnp.float32), pltpu.VMEM((heads, rank), jnp.float32)]

    def stores(depth, pieces):
        return [pltpu.VMEM((depth, width, pieces * rows), jnp.bfloat16), pltpu.SemaphoreType.DMA((depth, pieces)), pltpu.SemaphoreType.DMA((depth,))]

    def ring(depth, pieces):
        return [pltpu.VMEM((depth, pieces, total, rank), jnp.bfloat16), pltpu.SemaphoreType.DMA((depth,))] + stores(depth, pieces)

    params = pltpu.CompilerParams(vmem_limit_bytes=ATTEND_BYTES)
    flops = 2 * req_local * n * block * heads * rank
    *outs, first_part = pl.pallas_call(
        functools.partial(first_kernel, n, req_local, scale),
        in_specs=[SMEM, HBM, VMEM, VMEM],
        out_specs=[HBM] * 4,
        out_shape=caches + [part],
        scratch_shapes=state + [pltpu.VMEM(part.shape, part.dtype), pltpu.SemaphoreType.DMA,
                                pltpu.VMEM((rows, rank), jnp.bfloat16), pltpu.VMEM((width, block), jnp.bfloat16),
                                pltpu.VMEM((req_local - 2, heads, rank), jnp.bfloat16),
                                pltpu.SemaphoreType.DMA((req_local - 2,)), pltpu.SemaphoreType.DMA((req_local - 2,))]
        + ring(RING, PIECES) + ring(LATE_STEPS, 2 * PIECES - LATE) + ring(n - LATE_STEPS, PIECES),
        compiler_params=params,
        cost_estimate=pl.CostEstimate(flops=flops, bytes_accessed=req_local * n * block * rank * 4, transcendentals=0),
        name="attend_first",
    )(lens, landed, q_lat, q_rope)
    return pl.pallas_call(
        functools.partial(last_kernel, n, req_local, scale),
        in_specs=[SMEM] + [VMEM] * (LATE_STEPS + 4) + [HBM] * 3,
        out_specs=[HBM] * 3,
        out_shape=caches,
        scratch_shapes=[pltpu.VMEM((2, heads, rank), jnp.bfloat16), pltpu.SemaphoreType.DMA((2,))] + stores(late, 1),
        input_output_aliases={LATE_STEPS + 5 + k: k for k in range(3)},
        compiler_params=params,
        cost_estimate=pl.CostEstimate(flops=flops // req_local // PIECES, bytes_accessed=n * block * rank * 2, transcendentals=0),
        name="attend_last",
    )(lens, *rest, q_lat, q_rope, first_part, before, *outs)


def solution(mesh):
    seq_spec = P("dp", "x", None)
    req_spec = P(("dp", "x"), None, None)
    n = mesh.shape["x"]

    def local_step(c_raw, k_raw, norm_gain, rope_cos, rope_sin, seq_lens, q_lat, q_rope):
        q_rope = jnp.swapaxes(q_rope, 1, 2)
        landed, before, *rest = send(seq_lens, c_raw, jnp.swapaxes(k_raw, 1, 2), norm_gain, rope_cos.T, rope_sin.T, q_lat, q_rope, n)
        rest = [lax.ppermute(pieces, "x", [(i, move(i, j, n, 1)) for i in range(n)]) for j, pieces in enumerate(rest)]
        c_cache, kr_cache, o_lat = attend(seq_lens, landed, before, rest, q_lat, q_rope, n, c_raw.shape[1])
        return c_cache, jnp.swapaxes(kr_cache, 1, 2), o_lat

    return jax.shard_map(local_step, mesh=mesh, in_specs=(seq_spec, seq_spec, P(None), P("x", None), P("x", None), P("dp"), req_spec, req_spec), out_specs=(req_spec, req_spec, req_spec), check_vma=False)
```

```python
import functools

import jax
import jax.numpy as jnp
from jax import lax
from jax.experimental import pallas as pl
from jax.experimental.pallas import tpu as pltpu
from jax.sharding import PartitionSpec as P

NORM_EPS = 1e-6
PIECES = 3
ROUNDS = 6
LOADS = 4
RING = 20
LATE_STEPS = 2
LATE = 4
AHEAD = 3
STRIPE = 128
LANES, SUBLANES = 128, 16
VMEM_BYTES = 60 * 1024 * 1024
ATTEND_BYTES = 44 * 1024 * 1024
MESH = pl.DeviceIdType.MESH
HBM = pl.BlockSpec(memory_space=pltpu.HBM)
VMEM = pl.BlockSpec(memory_space=pltpu.VMEM)
SMEM = pl.BlockSpec(memory_space=pltpu.SMEM)


def move(me, j, n, way):
    chip, core = me // 2, me % 2
    far = j % 3
    last = j // (n - 2)
    other = (j // 3) % 2 * (1 - last) + last * (1 - j % (n - 2))
    there = (core + other) % 2
    sender = core if way == 1 else there
    hop = (1 - last) * (1 + 2 * far - 3 * (far // 2)) * (1 - 2 * sender)
    return (chip + n // 2 + way * hop) % (n // 2) * 2 + there


def peer(j, n):
    return move(lax.axis_index("x"), j, n, 1)


def result_place(land_ref, m, n):
    return land_ref.at[land_ref.shape[0] - 1, move(lax.axis_index("x"), m // PIECES, n, -1), m % PIECES]


def rope_tiles(width, rows):
    for r in range(width // SUBLANES):
        for c in range(rows // LANES):
            yield (slice(r * SUBLANES, (r + 1) * SUBLANES), slice(c * LANES, (c + 1) * LANES),
                   slice(rows + c * SUBLANES, rows + (c + 1) * SUBLANES), slice(r * LANES, (r + 1) * LANES))


def clear(state):
    m_ref, l_ref, acc_ref = state
    m_ref[...] = jnp.full_like(m_ref, -1e30)
    l_ref[...] = jnp.zeros_like(l_ref)
    acc_ref[...] = jnp.zeros_like(acc_ref)


def fold(state, qa, qr, pieces, firsts, length, scale):
    values = folded(*(ref[...] for ref in state), qa, qr, pieces, firsts, length, scale)
    for ref, value in zip(state, values):
        ref[...] = value


def folded(m_old, l_old, acc_old, qa, qr, pieces, firsts, length, scale):
    scores = []
    for first, (lat, kr) in zip(firsts, pieces):
        s = lax.dot_general(qa, lat, (((1,), (1,)), ((), ())), preferred_element_type=jnp.float32)
        s = s + lax.dot_general(qr, kr, (((0,), (0,)), ((), ())), preferred_element_type=jnp.float32)
        rows = lat.shape[0]
        pos = first + lax.broadcasted_iota(jnp.int32, (1, rows), 1)
        scores.append(jnp.where(pos < length, s * scale, -1e30))
    m_new = m_old
    for s in scores:
        m_new = jnp.maximum(m_new, jnp.max(s, axis=-1, keepdims=True))
    alpha = jnp.exp(m_old - m_new)
    total, acc = l_old * alpha, acc_old * alpha
    for s, (lat, _) in zip(scores, pieces):
        p = jnp.exp(s - m_new)
        total = total + jnp.sum(p, axis=-1, keepdims=True)
        acc = acc + jnp.dot(p.astype(jnp.bfloat16), lat, preferred_element_type=jnp.float32)
    return m_new, total, acc


def hand_over(state, length, part_ref):
    m_ref, l_ref, acc_ref = state
    heads, rank = acc_ref.shape
    part_ref[:, :rank] = acc_ref[...]
    part_ref[:, rank : rank + LANES] = jnp.broadcast_to(m_ref[...], (heads, LANES))
    part_ref[:, rank + LANES : rank + 2 * LANES] = jnp.broadcast_to(l_ref[...], (heads, LANES))
    part_ref[:, rank + 2 * LANES :] = jnp.full((heads, LANES), length, jnp.int32).astype(jnp.float32)


def send_kernel(n, req_local, scale, lens_hbm, c_hbm, k_hbm, gain_ref, cos_hbm, sin_hbm, qa_hbm, qr_hbm, land_ref, *scratch):
    part_out, rest_refs, scratch = scratch[0], scratch[1 : 1 + LATE_STEPS], scratch[1 + LATE_STEPS :]
    c_buf, k_buf, out_buf, c_sem, k_sem, send_sem, recv_sem, m_ref, l_ref, acc_ref, fold_buf, kr_buf, fold_sem, o_buf, o_sem, part_ref, part_sem, *tables = scratch
    lens_ref, cos_ref, sin_ref, qa_ref, qr_ref, table_sem = tables
    me = lax.axis_index("x")
    rounds = req_local * PIECES
    steps = rounds * n
    early = (rounds - LATE) * n
    depth = out_buf.shape[0]
    rows, rank = c_buf.shape[1:]
    width = k_buf.shape[1]

    def step(t):
        q = t % n
        last = q // (n - 2)
        return (1 - last) * ((q + 2 * (me % 2)) % (n - 2)) + last * q

    def load(t):
        req = peer(step(t), n) * req_local + t // n // PIECES
        first = pl.multiple_of(t // n % PIECES * rows, rows)
        slot = t % LOADS
        return (pltpu.make_async_copy(c_hbm.at[req, pl.ds(first, rows), :], c_buf.at[slot], c_sem.at[slot]),
                pltpu.make_async_copy(k_hbm.at[req, :, pl.ds(first, rows)], k_buf.at[slot], k_sem.at[slot]))

    def landing(t):
        return land_ref.at[t // n // PIECES, me, t // n % PIECES]

    def remote(t):
        slot = t % depth
        return pltpu.make_async_remote_copy(
            src_ref=out_buf.at[slot], dst_ref=landing(t), send_sem=send_sem.at[slot],
            recv_sem=recv_sem.at[t // n * n + me], device_id={"x": peer(step(t), n)}, device_id_type=MESH)

    def own(t):
        return pltpu.make_async_copy(out_buf.at[t % depth], landing(t), send_sem.at[t % depth])

    def keep(t, j):
        return pltpu.make_async_copy(out_buf.at[t % depth], rest_refs[j].at[(t - early) // n], send_sem.at[t % depth])

    def is_kept(t, way):
        return jnp.logical_and(t >= early, way < LATE_STEPS)

    def on_kind(t, act_remote, act_local):
        is_own = t % n == n - 1

        for j in range(LATE_STEPS):
            @pl.when(jnp.logical_and(t >= early, step(t) == j))
            def _():
                act_local(keep(t, j))

        @pl.when(is_own)
        def _():
            act_local(own(t))

        @pl.when(jnp.logical_not(jnp.logical_or(is_own, is_kept(t, step(t)))))
        def _():
            act_remote(remote(t))

    def start(t):
        on_kind(t, lambda c: c.start(), lambda c: c.start())

    def sent(t):
        on_kind(t, lambda c: c.wait_send(), lambda c: c.wait())

    def pack(t):
        for c in load(t):
            c.wait()
        slot, out = t % LOADS, t % depth
        first = t // n % PIECES * rows
        left = lens_ref[peer(step(t), n) * req_local + t // n // PIECES] - me * (rows * PIECES) - first
        gain = gain_ref[...].astype(jnp.float32)

        @pl.loop(0, rows, step=STRIPE)
        def _(r):
            r = pl.multiple_of(r, STRIPE)
            lat = c_buf[slot, pl.ds(r, STRIPE), :].astype(jnp.float32)
            inv = lax.rsqrt(jnp.mean(lat * lat, axis=-1, keepdims=True) + NORM_EPS)
            valid = r + lax.broadcasted_iota(jnp.int32, (STRIPE, 1), 0) < left
            out_buf[out, pl.ds(r, STRIPE), :] = jnp.where(valid, lat * inv * gain, 0.0).astype(jnp.bfloat16)

        key = k_buf[slot].astype(jnp.float32)
        half = width // 2
        lo, hi = key[:half], key[half:]
        first = pl.multiple_of(first, LANES)
        cos, sin = cos_ref[:, pl.ds(first, rows)], sin_ref[:, pl.ds(first, rows)]
        valid = lax.broadcasted_iota(jnp.int32, (1, rows), 1) < left
        rotated = (jnp.where(valid, lo * cos - hi * sin, 0.0).astype(jnp.bfloat16),
                   jnp.where(valid, hi * cos + lo * sin, 0.0).astype(jnp.bfloat16))
        for kr_rows, kr_cols, to_rows, to_cols in rope_tiles(width, rows):
            part, at = kr_rows.start // half, kr_rows.start % half
            out_buf[out, to_rows, to_cols] = rotated[part][at : at + SUBLANES, kr_cols]

    barrier = pltpu.get_barrier_semaphore()
    for j in range(n - 1):
        pl.semaphore_signal(barrier, inc=1, device_id={"x": peer(j, n)}, device_id_type=MESH)
    fills = [pltpu.make_async_copy(src, dst, table_sem.at[i]) for i, (src, dst) in enumerate(
        zip((lens_hbm, cos_hbm, sin_hbm, qa_hbm, qr_hbm), (lens_ref, cos_ref, sin_ref, qa_ref, qr_ref)))]
    for c in fills[:3]:
        c.start()
    for t in range(LOADS):
        for c in load(t):
            c.start()
    for c in fills[3:]:
        c.start()
    for c in fills[:3]:
        c.wait()
    pack(0)
    for c in load(LOADS):
        c.start()
    for c in fills[3:]:
        c.wait()
    pl.semaphore_wait(barrier, n - 1)

    state = (m_ref, l_ref, acc_ref)
    per_req = PIECES * n
    folds = (req_local - 1) * per_req
    lag = depth + n

    def received(a):
        src = peer(a % n, n)
        piece = land_ref.at[a // per_req, src, a // n % PIECES]
        pltpu.make_async_remote_copy(
            src_ref=piece, dst_ref=piece, send_sem=send_sem.at[0], recv_sem=recv_sem.at[a // n * n + src],
            device_id={"x": src}, device_id_type=MESH).wait_recv()

    def result(m):
        return pltpu.make_async_copy(o_buf.at[m], result_place(land_ref, m, n).at[pl.ds(0, o_buf.shape[1]), :], o_sem.at[m])

    def fetch(a):
        return pltpu.make_async_copy(land_ref.at[a // per_req, peer(a % n, n), a // n % PIECES], fold_buf.at[a % (AHEAD + 1)], fold_sem.at[a % (AHEAD + 1)])

    @pl.loop(1, folds + lag)
    def _(t):
        @pl.when(t >= depth)
        def _():
            sent(t - depth)

        @pl.when(t < steps)
        def _():
            pack(t)

            @pl.when(t + LOADS < steps)
            def _():
                for c in load(t + LOADS):
                    c.start()

        @pl.when(t <= steps)
        def _():
            start(t - 1)

        arriving = t - lag + AHEAD

        @pl.when(jnp.logical_and(arriving >= 0, arriving < folds))
        def _():
            @pl.when(jnp.logical_and(arriving % n < n - 1, jnp.logical_not(is_kept(arriving, arriving % n))))
            def _():
                received(arriving)

            @pl.when(jnp.logical_not(is_kept(arriving, arriving % n)))
            def _():
                fetch(arriving).start()

        a = t - lag

        @pl.when(a >= 0)
        def _():
            m, src, slot = a // per_req, peer(a % n, n), a % (AHEAD + 1)

            @pl.when(a % per_req == 0)
            def _():
                clear(state)

            @pl.when(jnp.logical_not(is_kept(a, a % n)))
            def _():
                fetch(a).wait()
                for kr_rows, kr_cols, from_rows, from_cols in rope_tiles(width, rows):
                    kr_buf[kr_rows, kr_cols] = fold_buf[slot, from_rows, from_cols]
                first = (src * PIECES + a // n % PIECES) * rows
                fold(state, qa_ref[m], qr_ref[m], [(fold_buf[slot, :rows, :], kr_buf[...])], [first], lens_ref[me * req_local + m], scale)

            @pl.when(jnp.logical_and(a % per_req == per_req - 1, m < req_local - 2))
            def _():
                o_buf[m] = (acc_ref[...] / l_ref[...]).astype(jnp.bfloat16)
                result(m).start()

    hand_over(state, lens_ref[me * req_local + req_local - 2], part_ref)
    copy = pltpu.make_async_copy(part_ref, part_out, part_sem)
    copy.start()

    @pl.loop(folds + lag - depth, steps)
    def _(t):
        sent(t)

    @pl.loop(folds, steps)
    def _(a):
        @pl.when(jnp.logical_and(a % n < n - 1, jnp.logical_not(is_kept(a, a % n))))
        def _():
            received(a)

    for m in range(req_local - 2):
        result(m).wait()
    copy.wait()


def send(lens, c_raw, k_raw, gain, cos, sin, q_lat, q_rope, n):
    req_local, heads, _ = q_lat.shape
    requests, block, rank = c_raw.shape
    width = k_raw.shape[1]
    rows = block // PIECES
    total = rows + rows * width // rank
    depth = ROUNDS * n
    return pl.pallas_call(
        functools.partial(send_kernel, n, req_local, (rank + width) ** -0.5),
        in_specs=[HBM, HBM, HBM, VMEM] + [HBM] * 4,
        out_specs=[HBM] * (2 + LATE_STEPS),
        out_shape=[jax.ShapeDtypeStruct((req_local, n, PIECES, total, rank), jnp.bfloat16)]
        + [jax.ShapeDtypeStruct((heads, rank + 3 * LANES), jnp.float32)]
        + [jax.ShapeDtypeStruct((LATE, total, rank), jnp.bfloat16)] * LATE_STEPS,
        scratch_shapes=[
            pltpu.VMEM((LOADS, rows, rank), jnp.bfloat16),
            pltpu.VMEM((LOADS, width, rows), jnp.bfloat16),
            pltpu.VMEM((depth, total, rank), jnp.bfloat16),
            pltpu.SemaphoreType.DMA((LOADS,)),
            pltpu.SemaphoreType.DMA((LOADS,)),
            pltpu.SemaphoreType.DMA((depth,)),
            pltpu.SemaphoreType.DMA((req_local * PIECES * n,)),
            pltpu.VMEM((heads, 1), jnp.float32),
            pltpu.VMEM((heads, 1), jnp.float32),
            pltpu.VMEM((heads, rank), jnp.float32),
            pltpu.VMEM((AHEAD + 1, total, rank), jnp.bfloat16),
            pltpu.VMEM((width, rows), jnp.bfloat16),
            pltpu.SemaphoreType.DMA((AHEAD + 1,)),
            pltpu.VMEM((req_local - 2, heads, rank), jnp.bfloat16),
            pltpu.SemaphoreType.DMA((req_local - 2,)),
            pltpu.VMEM((heads, rank + 3 * LANES), jnp.float32),
            pltpu.SemaphoreType.DMA,
            pltpu.SMEM(lens.shape, lens.dtype),
            pltpu.VMEM(cos.shape, cos.dtype),
            pltpu.VMEM(sin.shape, sin.dtype),
            pltpu.VMEM(q_lat.shape, q_lat.dtype),
            pltpu.VMEM(q_rope.shape, q_rope.dtype),
            pltpu.SemaphoreType.DMA((5,)),
        ],
        compiler_params=pltpu.CompilerParams(vmem_limit_bytes=VMEM_BYTES, collective_id=0, has_side_effects=True),
        cost_estimate=pl.CostEstimate(flops=requests * block * rank * 100, bytes_accessed=requests * block * rank * 4, transcendentals=0),
        name="send",
    )(lens, c_raw, k_raw, gain, cos, sin, q_lat, q_rope)


def stream(steps, place, first_piece, pieces, scale, length, land_ref, queries, c_out, kr_out, state, zero_c, zero_k, ring, ahead):
    buf, in_sem, kr_buf, c_sem, k_sem = ring
    depth = buf.shape[0]
    rank = buf.shape[3]
    width = kr_buf.shape[1]
    rows = kr_buf.shape[2] // pieces

    def first(t):
        return pl.multiple_of((place(t)[1] * PIECES + first_piece) * rows, rows)

    def used(t):
        return first(t) < length(place(t)[0])

    def load(t):
        req, src = place(t)
        return pltpu.make_async_copy(land_ref.at[req, src, pl.ds(first_piece, pieces)], buf.at[t % depth], in_sem.at[t % depth])

    def writes(t, c_of, kr):
        slot, req, at = t % depth, place(t)[0], first(t)
        return [pltpu.make_async_copy(c_of(h), c_out.at[req, pl.ds(at + h * rows, rows), :], c_sem.at[slot, h]) for h in range(pieces)] + [
            pltpu.make_async_copy(kr, kr_out.at[req, :, pl.ds(at, pieces * rows)], k_sem.at[slot])]

    def stores(t):
        return writes(t, lambda h: buf.at[t % depth, h, pl.ds(0, rows), :], kr_buf.at[t % depth])

    def blanks(t):
        return writes(t, lambda h: zero_c, zero_k.at[:, pl.ds(0, pieces * rows)])

    def fetch(t):
        @pl.when(used(t))
        def _():
            load(t).start()

    def work(t):
        slot = t % depth
        load(t).wait()
        for h in range(pieces):
            for kr_rows, kr_cols, from_rows, from_cols in rope_tiles(width, rows):
                cols = slice(h * rows + kr_cols.start, h * rows + kr_cols.stop)
                kr_buf[slot, kr_rows, cols] = buf[slot, h, from_rows, from_cols]
        for c in stores(t):
            c.start()
        if queries is not None:
            qa, qr = queries()
            blocks = [(buf[slot, h, :rows, :], kr_buf[slot, :, h * rows : (h + 1) * rows]) for h in range(pieces)]
            fold(state, qa, qr, blocks, [first(t) + h * rows for h in range(pieces)], length(place(t)[0]), scale)

    def body(t):
        @pl.when(used(t))
        def _():
            work(t)

        @pl.when(jnp.logical_not(used(t)))
        def _():
            for c in blanks(t):
                c.start()

        @pl.when(t + ahead < steps)
        def _():
            @pl.when(t + ahead >= depth)
            def _():
                for c in stores(t + ahead - depth):
                    c.wait()

            fetch(t + ahead)

    def prologue():
        for t in range(min(ahead, steps)):
            fetch(t)

    def drain():
        @pl.loop(max(steps - depth, 0), steps)
        def _(t):
            for c in stores(t):
                c.wait()

    return steps, prologue, body, drain


def first_kernel(n, req_local, scale, lens_ref, land_ref, qa_ref, qr_ref, c_out, kr_out, o_out, part_out,
                 m_ref, l_ref, acc_ref, part_ref, part_sem, zero_c, zero_k, o_buf, o_in_sem, o_out_sem, *rings):
    length = lambda m: lens_ref[lax.axis_index("x") * req_local + m]
    state = (m_ref, l_ref, acc_ref)
    last = req_local - 1
    rank = acc_ref.shape[1]
    me = lax.axis_index("x")
    queries = lambda: (qa_ref[last], qr_ref[last])
    common = (scale, length, land_ref)
    outs = (c_out, kr_out, state, zero_c, zero_k)
    whole = (last - 1) * n
    after = lambda t: move(me, LATE_STEPS + t, n, -1)

    def place(t):
        tail = t // whole
        return t // n * (1 - tail) + (last - 1) * tail, t % n * (1 - tail) + after(t - whole * tail) * tail

    main = stream(whole + n - LATE_STEPS, place, 0, PIECES, *common, None, *outs, rings[:5], RING // 2)
    front = stream(LATE_STEPS, lambda t: (last - 1, move(me, t, n, -1)), 0, 2 * PIECES - LATE, *common, None, *outs, rings[5:10], LATE_STEPS)
    back = stream(n - LATE_STEPS, lambda t: (last, after(t)), 0, PIECES, *common, queries, *outs, rings[10:], n - LATE_STEPS)
    results = [(pltpu.make_async_copy(result_place(land_ref, m, n).at[pl.ds(0, o_buf.shape[1]), :], o_buf.at[m], o_in_sem.at[m]),
                pltpu.make_async_copy(o_buf.at[m], o_out.at[m], o_out_sem.at[m])) for m in range(last - 1)]

    for part in (front, back, main):
        part[1]()
    for take, _ in results:
        take.start()
    zero_c[...] = jnp.zeros_like(zero_c)
    zero_k[...] = jnp.zeros_like(zero_k)
    clear(state)
    steps = main[0]

    @pl.loop(0, steps)
    def _(t):
        main[2](t)

        every = steps // back[0]

        @pl.when(jnp.logical_and(t % every == 0, t // every < back[0]))
        def _():
            back[2](t // every)

        @pl.when(jnp.logical_and(t % every == every // 2, t // every < front[0]))
        def _():
            front[2](t // every)

    for take, give in results:
        take.wait()
        give.start()
    hand_over(state, length(last), part_ref)
    copy = pltpu.make_async_copy(part_ref, part_out, part_sem)
    copy.start()
    copy.wait()
    for part in (main, front, back):
        part[3]()
    for _, give in results:
        give.wait()


def last_kernel(n, req_local, scale, *refs):
    land_refs, refs = refs[:LATE_STEPS], refs[LATE_STEPS:]
    qa_ref, qr_ref, part_ref, before_ref, c_old, kr_old, o_old, c_out, kr_out, o_out, *refs = refs
    o_buf, o_sem, kr_buf, c_sem, k_sem = refs
    rank = qa_ref.shape[2]
    width = kr_buf.shape[1]
    rows = kr_buf.shape[2]
    waits = []
    groups = []
    for req, rounds, part in ((req_local - 1, range(LATE - PIECES, LATE), part_ref), (req_local - 2, range(LATE - PIECES), before_ref)):
        pieces = [(j, r) for j in range(LATE_STEPS) for r in rounds]
        firsts = [pl.multiple_of((move(lax.axis_index("x"), j, n, -1) * PIECES + (r - LATE) % PIECES) * rows, rows) for j, r in pieces]
        groups.append((req, part, pieces, firsts))
        for (j, r), first in zip(pieces, firsts):
            i = j * LATE + r
            waits.append(pltpu.make_async_copy(land_refs[j].at[r, pl.ds(0, rows), :], c_out.at[req, pl.ds(first, rows), :], c_sem.at[i, 0]))
            waits[-1].start()
            for kr_rows, kr_cols, from_rows, from_cols in rope_tiles(width, rows):
                kr_buf[i, kr_rows, kr_cols] = land_refs[j][r, from_rows, from_cols]
            waits.append(pltpu.make_async_copy(kr_buf.at[i], kr_out.at[req, :, pl.ds(first, rows)], k_sem.at[i]))
            waits[-1].start()
    for at, (req, part, pieces, firsts) in enumerate(groups):
        length = part[:, rank + 2 * LANES : rank + 2 * LANES + 1]
        blocks = [(land_refs[j][r, :rows, :], kr_buf[j * LATE + r]) for j, r in pieces]
        state = part[:, rank : rank + 1], part[:, rank + LANES : rank + LANES + 1], part[:, :rank]
        _, total, acc = folded(*state, qa_ref[req], qr_ref[req], blocks, firsts, length, scale)
        o_buf[at] = (acc / total).astype(jnp.bfloat16)
    for at, (req, *_) in enumerate(groups):
        waits.append(pltpu.make_async_copy(o_buf.at[at], o_out.at[req], o_sem.at[at]))
        waits[-1].start()
    for c in waits:
        c.wait()


def attend(lens, landed, before, rest, q_lat, q_rope, n, block):
    req_local, heads, rank = q_lat.shape
    width = q_rope.shape[1]
    rows = block // PIECES
    total = rest[0].shape[1]
    late = LATE_STEPS * LATE
    scale = (rank + width) ** -0.5
    caches = [jax.ShapeDtypeStruct((req_local, n * block, rank), jnp.bfloat16),
              jax.ShapeDtypeStruct((req_local, width, n * block), jnp.bfloat16),
              jax.ShapeDtypeStruct((req_local, heads, rank), jnp.bfloat16)]
    part = jax.ShapeDtypeStruct((heads, rank + 3 * LANES), jnp.float32)
    state = [pltpu.VMEM((heads, 1), jnp.float32), pltpu.VMEM((heads, 1), jnp.float32), pltpu.VMEM((heads, rank), jnp.float32)]

    def stores(depth, pieces):
        return [pltpu.VMEM((depth, width, pieces * rows), jnp.bfloat16), pltpu.SemaphoreType.DMA((depth, pieces)), pltpu.SemaphoreType.DMA((depth,))]

    def ring(depth, pieces):
        return [pltpu.VMEM((depth, pieces, total, rank), jnp.bfloat16), pltpu.SemaphoreType.DMA((depth,))] + stores(depth, pieces)

    params = pltpu.CompilerParams(vmem_limit_bytes=ATTEND_BYTES)
    flops = 2 * req_local * n * block * heads * rank
    *outs, first_part = pl.pallas_call(
        functools.partial(first_kernel, n, req_local, scale),
        in_specs=[SMEM, HBM, VMEM, VMEM],
        out_specs=[HBM] * 4,
        out_shape=caches + [part],
        scratch_shapes=state + [pltpu.VMEM(part.shape, part.dtype), pltpu.SemaphoreType.DMA,
                                pltpu.VMEM((rows, rank), jnp.bfloat16), pltpu.VMEM((width, block), jnp.bfloat16),
                                pltpu.VMEM((req_local - 2, heads, rank), jnp.bfloat16),
                                pltpu.SemaphoreType.DMA((req_local - 2,)), pltpu.SemaphoreType.DMA((req_local - 2,))]
        + ring(RING, PIECES) + ring(LATE_STEPS, 2 * PIECES - LATE) + ring(n - LATE_STEPS, PIECES),
        compiler_params=params,
        cost_estimate=pl.CostEstimate(flops=flops, bytes_accessed=req_local * n * block * rank * 4, transcendentals=0),
        name="attend_first",
    )(lens, landed, q_lat, q_rope)
    return pl.pallas_call(
        functools.partial(last_kernel, n, req_local, scale),
        in_specs=[VMEM] * (LATE_STEPS + 4) + [HBM] * 3,
        out_specs=[HBM] * 3,
        out_shape=caches,
        scratch_shapes=[pltpu.VMEM((2, heads, rank), jnp.bfloat16), pltpu.SemaphoreType.DMA((2,))] + stores(late, 1),
        input_output_aliases={LATE_STEPS + 4 + k: k for k in range(3)},
        compiler_params=params,
        cost_estimate=pl.CostEstimate(flops=flops // req_local // PIECES, bytes_accessed=n * block * rank * 2, transcendentals=0),
        name="attend_last",
    )(*rest, q_lat, q_rope, first_part, before, *outs)


def solution(mesh):
    seq_spec = P("dp", "x", None)
    req_spec = P(("dp", "x"), None, None)
    n = mesh.shape["x"]

    def local_step(c_raw, k_raw, norm_gain, rope_cos, rope_sin, seq_lens, q_lat, q_rope):
        q_rope = jnp.swapaxes(q_rope, 1, 2)
        landed, before, *rest = send(seq_lens, c_raw, jnp.swapaxes(k_raw, 1, 2), norm_gain, rope_cos.T, rope_sin.T, q_lat, q_rope, n)
        rest = [lax.ppermute(pieces, "x", [(i, move(i, j, n, 1)) for i in range(n)]) for j, pieces in enumerate(rest)]
        c_cache, kr_cache, o_lat = attend(seq_lens, landed, before, rest, q_lat, q_rope, n, c_raw.shape[1])
        return c_cache, jnp.swapaxes(kr_cache, 1, 2), o_lat

    return jax.shard_map(local_step, mesh=mesh, in_specs=(seq_spec, seq_spec, P(None), P("x", None), P("x", None), P("dp"), req_spec, req_spec), out_specs=(req_spec, req_spec, req_spec), check_vma=False)
```

```python
import functools

import jax
import jax.numpy as jnp
from jax import lax
from jax.experimental import pallas as pl
from jax.experimental.pallas import tpu as pltpu
from jax.sharding import PartitionSpec as P

NORM_EPS = 1e-6
PIECES = 3
ROUNDS = 8
LOADS = 4
RING = 20
LATE_STEPS = 2
LATE = 4
AHEAD = 3
STRIPE = 128
LANES, SUBLANES = 128, 16
VMEM_BYTES = 60 * 1024 * 1024
ATTEND_BYTES = 44 * 1024 * 1024
MESH = pl.DeviceIdType.MESH
HBM = pl.BlockSpec(memory_space=pltpu.HBM)
VMEM = pl.BlockSpec(memory_space=pltpu.VMEM)
SMEM = pl.BlockSpec(memory_space=pltpu.SMEM)


def move(me, j, n, way):
    chip, core = me // 2, me % 2
    far = j % 3
    last = j // (n - 2)
    other = (j // 3) % 2 * (1 - last) + last * (1 - j % (n - 2))
    there = (core + other) % 2
    sender = core if way == 1 else there
    hop = (1 - last) * (1 + 2 * far - 3 * (far // 2)) * (1 - 2 * sender)
    return (chip + n // 2 + way * hop) % (n // 2) * 2 + there


def peer(j, n):
    return move(lax.axis_index("x"), j, n, 1)


def result_place(land_ref, m, n):
    return land_ref.at[land_ref.shape[0] - 1, move(lax.axis_index("x"), m // PIECES, n, -1), m % PIECES]


def rope_tiles(width, rows):
    for r in range(width // SUBLANES):
        for c in range(rows // LANES):
            yield (slice(r * SUBLANES, (r + 1) * SUBLANES), slice(c * LANES, (c + 1) * LANES),
                   slice(rows + c * SUBLANES, rows + (c + 1) * SUBLANES), slice(r * LANES, (r + 1) * LANES))


def clear(state):
    m_ref, l_ref, acc_ref = state
    m_ref[...] = jnp.full_like(m_ref, -1e30)
    l_ref[...] = jnp.zeros_like(l_ref)
    acc_ref[...] = jnp.zeros_like(acc_ref)


def fold(state, qa, qr, pieces, firsts, length, scale):
    values = folded(*(ref[...] for ref in state), qa, qr, pieces, firsts, length, scale)
    for ref, value in zip(state, values):
        ref[...] = value


def folded(m_old, l_old, acc_old, qa, qr, pieces, firsts, length, scale):
    scores = []
    for first, (lat, kr) in zip(firsts, pieces):
        s = lax.dot_general(qa, lat, (((1,), (1,)), ((), ())), preferred_element_type=jnp.float32)
        s = s + lax.dot_general(qr, kr, (((0,), (0,)), ((), ())), preferred_element_type=jnp.float32)
        rows = lat.shape[0]
        pos = first + lax.broadcasted_iota(jnp.int32, (1, rows), 1)
        scores.append(jnp.where(pos < length, s * scale, -1e30))
    m_new = m_old
    for s in scores:
        m_new = jnp.maximum(m_new, jnp.max(s, axis=-1, keepdims=True))
    alpha = jnp.exp(m_old - m_new)
    total, acc = l_old * alpha, acc_old * alpha
    for s, (lat, _) in zip(scores, pieces):
        p = jnp.exp(s - m_new)
        total = total + jnp.sum(p, axis=-1, keepdims=True)
        acc = acc + jnp.dot(p.astype(jnp.bfloat16), lat, preferred_element_type=jnp.float32)
    return m_new, total, acc


def hand_over(state, length, part_ref):
    m_ref, l_ref, acc_ref = state
    heads, rank = acc_ref.shape
    part_ref[:, :rank] = acc_ref[...]
    part_ref[:, rank : rank + LANES] = jnp.broadcast_to(m_ref[...], (heads, LANES))
    part_ref[:, rank + LANES : rank + 2 * LANES] = jnp.broadcast_to(l_ref[...], (heads, LANES))
    part_ref[:, rank + 2 * LANES :] = jnp.full((heads, LANES), length, jnp.int32).astype(jnp.float32)


def send_kernel(n, req_local, scale, lens_hbm, c_hbm, k_hbm, gain_ref, cos_hbm, sin_hbm, qa_hbm, qr_hbm, land_ref, *scratch):
    part_out, rest_refs, scratch = scratch[0], scratch[1 : 1 + LATE_STEPS], scratch[1 + LATE_STEPS :]
    c_buf, k_buf, out_buf, c_sem, k_sem, send_sem, recv_sem, m_ref, l_ref, acc_ref, fold_buf, kr_buf, fold_sem, o_buf, o_sem, part_ref, part_sem, *tables = scratch
    lens_ref, cos_ref, sin_ref, qa_ref, qr_ref, table_sem = tables
    me = lax.axis_index("x")
    rounds = req_local * PIECES
    steps = rounds * n
    early = (rounds - LATE) * n
    depth = out_buf.shape[0]
    rows, rank = c_buf.shape[1:]
    width = k_buf.shape[1]

    def step(t):
        q = t % n
        last = q // (n - 2)
        return (1 - last) * ((q + 2 * (me % 2)) % (n - 2)) + last * q

    def load(t):
        req = peer(step(t), n) * req_local + t // n // PIECES
        first = pl.multiple_of(t // n % PIECES * rows, rows)
        slot = t % LOADS
        return (pltpu.make_async_copy(c_hbm.at[req, pl.ds(first, rows), :], c_buf.at[slot], c_sem.at[slot]),
                pltpu.make_async_copy(k_hbm.at[req, :, pl.ds(first, rows)], k_buf.at[slot], k_sem.at[slot]))

    def landing(t):
        return land_ref.at[t // n // PIECES, me, t // n % PIECES]

    def remote(t):
        slot = t % depth
        return pltpu.make_async_remote_copy(
            src_ref=out_buf.at[slot], dst_ref=landing(t), send_sem=send_sem.at[slot],
            recv_sem=recv_sem.at[t // n * n + me], device_id={"x": peer(step(t), n)}, device_id_type=MESH)

    def own(t):
        return pltpu.make_async_copy(out_buf.at[t % depth], landing(t), send_sem.at[t % depth])

    def keep(t, j):
        return pltpu.make_async_copy(out_buf.at[t % depth], rest_refs[j].at[(t - early) // n], send_sem.at[t % depth])

    def is_kept(t, way):
        return jnp.logical_and(t >= early, way < LATE_STEPS)

    def on_kind(t, act_remote, act_local):
        is_own = t % n == n - 1

        for j in range(LATE_STEPS):
            @pl.when(jnp.logical_and(t >= early, step(t) == j))
            def _():
                act_local(keep(t, j))

        @pl.when(is_own)
        def _():
            act_local(own(t))

        @pl.when(jnp.logical_not(jnp.logical_or(is_own, is_kept(t, step(t)))))
        def _():
            act_remote(remote(t))

    def start(t):
        on_kind(t, lambda c: c.start(), lambda c: c.start())

    def sent(t):
        on_kind(t, lambda c: c.wait_send(), lambda c: c.wait())

    def pack(t):
        for c in load(t):
            c.wait()
        slot, out = t % LOADS, t % depth
        first = t // n % PIECES * rows
        left = lens_ref[peer(step(t), n) * req_local + t // n // PIECES] - me * (rows * PIECES) - first
        gain = gain_ref[...].astype(jnp.float32)

        @pl.loop(0, rows, step=STRIPE)
        def _(r):
            r = pl.multiple_of(r, STRIPE)
            lat = c_buf[slot, pl.ds(r, STRIPE), :].astype(jnp.float32)
            inv = lax.rsqrt(jnp.mean(lat * lat, axis=-1, keepdims=True) + NORM_EPS)
            valid = r + lax.broadcasted_iota(jnp.int32, (STRIPE, 1), 0) < left
            out_buf[out, pl.ds(r, STRIPE), :] = jnp.where(valid, lat * inv * gain, 0.0).astype(jnp.bfloat16)

        key = k_buf[slot].astype(jnp.float32)
        half = width // 2
        lo, hi = key[:half], key[half:]
        first = pl.multiple_of(first, LANES)
        cos, sin = cos_ref[:, pl.ds(first, rows)], sin_ref[:, pl.ds(first, rows)]
        valid = lax.broadcasted_iota(jnp.int32, (1, rows), 1) < left
        rotated = (jnp.where(valid, lo * cos - hi * sin, 0.0).astype(jnp.bfloat16),
                   jnp.where(valid, hi * cos + lo * sin, 0.0).astype(jnp.bfloat16))
        for kr_rows, kr_cols, to_rows, to_cols in rope_tiles(width, rows):
            part, at = kr_rows.start // half, kr_rows.start % half
            out_buf[out, to_rows, to_cols] = rotated[part][at : at + SUBLANES, kr_cols]

    barrier = pltpu.get_barrier_semaphore()
    for j in range(n - 1):
        pl.semaphore_signal(barrier, inc=1, device_id={"x": peer(j, n)}, device_id_type=MESH)
    fills = [pltpu.make_async_copy(src, dst, table_sem.at[i]) for i, (src, dst) in enumerate(
        zip((lens_hbm, cos_hbm, sin_hbm, qa_hbm, qr_hbm), (lens_ref, cos_ref, sin_ref, qa_ref, qr_ref)))]
    for c in fills[:3]:
        c.start()
    for t in range(LOADS):
        for c in load(t):
            c.start()
    for c in fills[3:]:
        c.start()
    for c in fills[:3]:
        c.wait()
    pack(0)
    for c in load(LOADS):
        c.start()
    for c in fills[3:]:
        c.wait()
    pl.semaphore_wait(barrier, n - 1)

    state = (m_ref, l_ref, acc_ref)
    per_req = PIECES * n
    folds = (req_local - 1) * per_req
    lag = depth + n

    def received(a):
        src = peer(a % n, n)
        piece = land_ref.at[a // per_req, src, a // n % PIECES]
        pltpu.make_async_remote_copy(
            src_ref=piece, dst_ref=piece, send_sem=send_sem.at[0], recv_sem=recv_sem.at[a // n * n + src],
            device_id={"x": src}, device_id_type=MESH).wait_recv()

    def result(m):
        return pltpu.make_async_copy(o_buf.at[m], result_place(land_ref, m, n).at[pl.ds(0, o_buf.shape[1]), :], o_sem.at[m])

    def fetch(a):
        return pltpu.make_async_copy(land_ref.at[a // per_req, peer(a % n, n), a // n % PIECES], fold_buf.at[a % (AHEAD + 1)], fold_sem.at[a % (AHEAD + 1)])

    @pl.loop(1, folds + lag)
    def _(t):
        @pl.when(t >= depth)
        def _():
            sent(t - depth)

        @pl.when(t < steps)
        def _():
            pack(t)

            @pl.when(t + LOADS < steps)
            def _():
                for c in load(t + LOADS):
                    c.start()

        @pl.when(t <= steps)
        def _():
            start(t - 1)

        arriving = t - lag + AHEAD

        @pl.when(jnp.logical_and(arriving >= 0, arriving < folds))
        def _():
            @pl.when(jnp.logical_and(arriving % n < n - 1, jnp.logical_not(is_kept(arriving, arriving % n))))
            def _():
                received(arriving)

            @pl.when(jnp.logical_not(is_kept(arriving, arriving % n)))
            def _():
                fetch(arriving).start()

        a = t - lag

        @pl.when(a >= 0)
        def _():
            m, src, slot = a // per_req, peer(a % n, n), a % (AHEAD + 1)

            @pl.when(a % per_req == 0)
            def _():
                clear(state)

            @pl.when(jnp.logical_not(is_kept(a, a % n)))
            def _():
                fetch(a).wait()
                for kr_rows, kr_cols, from_rows, from_cols in rope_tiles(width, rows):
                    kr_buf[kr_rows, kr_cols] = fold_buf[slot, from_rows, from_cols]
                first = (src * PIECES + a // n % PIECES) * rows
                fold(state, qa_ref[m], qr_ref[m], [(fold_buf[slot, :rows, :], kr_buf[...])], [first], lens_ref[me * req_local + m], scale)

            @pl.when(jnp.logical_and(a % per_req == per_req - 1, m < req_local - 2))
            def _():
                o_buf[m] = (acc_ref[...] / l_ref[...]).astype(jnp.bfloat16)
                result(m).start()

    hand_over(state, lens_ref[me * req_local + req_local - 2], part_ref)
    copy = pltpu.make_async_copy(part_ref, part_out, part_sem)
    copy.start()

    @pl.loop(folds + lag - depth, steps)
    def _(t):
        sent(t)

    @pl.loop(folds, steps)
    def _(a):
        @pl.when(jnp.logical_and(a % n < n - 1, jnp.logical_not(is_kept(a, a % n))))
        def _():
            received(a)

    for m in range(req_local - 2):
        result(m).wait()
    copy.wait()


def send(lens, c_raw, k_raw, gain, cos, sin, q_lat, q_rope, n):
    req_local, heads, _ = q_lat.shape
    requests, block, rank = c_raw.shape
    width = k_raw.shape[1]
    rows = block // PIECES
    total = rows + rows * width // rank
    depth = ROUNDS * n
    return pl.pallas_call(
        functools.partial(send_kernel, n, req_local, (rank + width) ** -0.5),
        in_specs=[HBM, HBM, HBM, VMEM] + [HBM] * 4,
        out_specs=[HBM] * (2 + LATE_STEPS),
        out_shape=[jax.ShapeDtypeStruct((req_local, n, PIECES, total, rank), jnp.bfloat16)]
        + [jax.ShapeDtypeStruct((heads, rank + 3 * LANES), jnp.float32)]
        + [jax.ShapeDtypeStruct((LATE, total, rank), jnp.bfloat16)] * LATE_STEPS,
        scratch_shapes=[
            pltpu.VMEM((LOADS, rows, rank), jnp.bfloat16),
            pltpu.VMEM((LOADS, width, rows), jnp.bfloat16),
            pltpu.VMEM((depth, total, rank), jnp.bfloat16),
            pltpu.SemaphoreType.DMA((LOADS,)),
            pltpu.SemaphoreType.DMA((LOADS,)),
            pltpu.SemaphoreType.DMA((depth,)),
            pltpu.SemaphoreType.DMA((req_local * PIECES * n,)),
            pltpu.VMEM((heads, 1), jnp.float32),
            pltpu.VMEM((heads, 1), jnp.float32),
            pltpu.VMEM((heads, rank), jnp.float32),
            pltpu.VMEM((AHEAD + 1, total, rank), jnp.bfloat16),
            pltpu.VMEM((width, rows), jnp.bfloat16),
            pltpu.SemaphoreType.DMA((AHEAD + 1,)),
            pltpu.VMEM((req_local - 2, heads, rank), jnp.bfloat16),
            pltpu.SemaphoreType.DMA((req_local - 2,)),
            pltpu.VMEM((heads, rank + 3 * LANES), jnp.float32),
            pltpu.SemaphoreType.DMA,
            pltpu.SMEM(lens.shape, lens.dtype),
            pltpu.VMEM(cos.shape, cos.dtype),
            pltpu.VMEM(sin.shape, sin.dtype),
            pltpu.VMEM(q_lat.shape, q_lat.dtype),
            pltpu.VMEM(q_rope.shape, q_rope.dtype),
            pltpu.SemaphoreType.DMA((5,)),
        ],
        compiler_params=pltpu.CompilerParams(vmem_limit_bytes=VMEM_BYTES, collective_id=0, has_side_effects=True),
        cost_estimate=pl.CostEstimate(flops=requests * block * rank * 100, bytes_accessed=requests * block * rank * 4, transcendentals=0),
        name="send",
    )(lens, c_raw, k_raw, gain, cos, sin, q_lat, q_rope)


def stream(steps, place, first_piece, pieces, scale, length, land_ref, queries, c_out, kr_out, state, zero_c, zero_k, ring, ahead):
    buf, in_sem, kr_buf, c_sem, k_sem = ring
    depth = buf.shape[0]
    rank = buf.shape[3]
    width = kr_buf.shape[1]
    rows = kr_buf.shape[2] // pieces

    def first(t):
        return pl.multiple_of((place(t)[1] * PIECES + first_piece) * rows, rows)

    def used(t):
        return first(t) < length(place(t)[0])

    def load(t):
        req, src = place(t)
        return pltpu.make_async_copy(land_ref.at[req, src, pl.ds(first_piece, pieces)], buf.at[t % depth], in_sem.at[t % depth])

    def writes(t, c_of, kr):
        slot, req, at = t % depth, place(t)[0], first(t)
        return [pltpu.make_async_copy(c_of(h), c_out.at[req, pl.ds(at + h * rows, rows), :], c_sem.at[slot, h]) for h in range(pieces)] + [
            pltpu.make_async_copy(kr, kr_out.at[req, :, pl.ds(at, pieces * rows)], k_sem.at[slot])]

    def stores(t):
        return writes(t, lambda h: buf.at[t % depth, h, pl.ds(0, rows), :], kr_buf.at[t % depth])

    def blanks(t):
        return writes(t, lambda h: zero_c, zero_k.at[:, pl.ds(0, pieces * rows)])

    def fetch(t):
        @pl.when(used(t))
        def _():
            load(t).start()

    def work(t):
        slot = t % depth
        load(t).wait()
        for h in range(pieces):
            for kr_rows, kr_cols, from_rows, from_cols in rope_tiles(width, rows):
                cols = slice(h * rows + kr_cols.start, h * rows + kr_cols.stop)
                kr_buf[slot, kr_rows, cols] = buf[slot, h, from_rows, from_cols]
        for c in stores(t):
            c.start()
        if queries is not None:
            qa, qr = queries()
            blocks = [(buf[slot, h, :rows, :], kr_buf[slot, :, h * rows : (h + 1) * rows]) for h in range(pieces)]
            fold(state, qa, qr, blocks, [first(t) + h * rows for h in range(pieces)], length(place(t)[0]), scale)

    def body(t):
        @pl.when(used(t))
        def _():
            work(t)

        @pl.when(jnp.logical_not(used(t)))
        def _():
            for c in blanks(t):
                c.start()

        @pl.when(t + ahead < steps)
        def _():
            @pl.when(t + ahead >= depth)
            def _():
                for c in stores(t + ahead - depth):
                    c.wait()

            fetch(t + ahead)

    def prologue():
        for t in range(min(ahead, steps)):
            fetch(t)

    def drain():
        @pl.loop(max(steps - depth, 0), steps)
        def _(t):
            for c in stores(t):
                c.wait()

    return steps, prologue, body, drain


def first_kernel(n, req_local, scale, lens_ref, land_ref, qa_ref, qr_ref, c_out, kr_out, o_out, part_out,
                 m_ref, l_ref, acc_ref, part_ref, part_sem, zero_c, zero_k, o_buf, o_in_sem, o_out_sem, *rings):
    length = lambda m: lens_ref[lax.axis_index("x") * req_local + m]
    state = (m_ref, l_ref, acc_ref)
    last = req_local - 1
    rank = acc_ref.shape[1]
    me = lax.axis_index("x")
    queries = lambda: (qa_ref[last], qr_ref[last])
    common = (scale, length, land_ref)
    outs = (c_out, kr_out, state, zero_c, zero_k)
    whole = (last - 1) * n
    after = lambda t: move(me, LATE_STEPS + t, n, -1)

    def place(t):
        tail = t // whole
        return t // n * (1 - tail) + (last - 1) * tail, t % n * (1 - tail) + after(t - whole * tail) * tail

    main = stream(whole + n - LATE_STEPS, place, 0, PIECES, *common, None, *outs, rings[:5], RING // 2)
    front = stream(LATE_STEPS, lambda t: (last - 1, move(me, t, n, -1)), 0, 2 * PIECES - LATE, *common, None, *outs, rings[5:10], LATE_STEPS)
    back = stream(n - LATE_STEPS, lambda t: (last, after(t)), 0, PIECES, *common, queries, *outs, rings[10:], n - LATE_STEPS)
    results = [(pltpu.make_async_copy(result_place(land_ref, m, n).at[pl.ds(0, o_buf.shape[1]), :], o_buf.at[m], o_in_sem.at[m]),
                pltpu.make_async_copy(o_buf.at[m], o_out.at[m], o_out_sem.at[m])) for m in range(last - 1)]

    for part in (front, back, main):
        part[1]()
    for take, _ in results:
        take.start()
    zero_c[...] = jnp.zeros_like(zero_c)
    zero_k[...] = jnp.zeros_like(zero_k)
    clear(state)
    steps = main[0]

    @pl.loop(0, steps)
    def _(t):
        main[2](t)

        every = steps // back[0]

        @pl.when(jnp.logical_and(t % every == 0, t // every < back[0]))
        def _():
            back[2](t // every)

        @pl.when(jnp.logical_and(t % every == every // 2, t // every < front[0]))
        def _():
            front[2](t // every)

    for take, give in results:
        take.wait()
        give.start()
    hand_over(state, length(last), part_ref)
    copy = pltpu.make_async_copy(part_ref, part_out, part_sem)
    copy.start()
    copy.wait()
    for part in (main, front, back):
        part[3]()
    for _, give in results:
        give.wait()


def last_kernel(n, req_local, scale, *refs):
    land_refs, refs = refs[:LATE_STEPS], refs[LATE_STEPS:]
    qa_ref, qr_ref, part_ref, before_ref, c_old, kr_old, o_old, c_out, kr_out, o_out, *refs = refs
    o_buf, o_sem, kr_buf, c_sem, k_sem = refs
    rank = qa_ref.shape[2]
    width = kr_buf.shape[1]
    rows = kr_buf.shape[2]
    waits = []
    groups = []
    for req, rounds, part in ((req_local - 1, range(LATE - PIECES, LATE), part_ref), (req_local - 2, range(LATE - PIECES), before_ref)):
        pieces = [(j, r) for j in range(LATE_STEPS) for r in rounds]
        firsts = [pl.multiple_of((move(lax.axis_index("x"), j, n, -1) * PIECES + (r - LATE) % PIECES) * rows, rows) for j, r in pieces]
        groups.append((req, part, pieces, firsts))
        for (j, r), first in zip(pieces, firsts):
            i = j * LATE + r
            waits.append(pltpu.make_async_copy(land_refs[j].at[r, pl.ds(0, rows), :], c_out.at[req, pl.ds(first, rows), :], c_sem.at[i, 0]))
            waits[-1].start()
            for kr_rows, kr_cols, from_rows, from_cols in rope_tiles(width, rows):
                kr_buf[i, kr_rows, kr_cols] = land_refs[j][r, from_rows, from_cols]
            waits.append(pltpu.make_async_copy(kr_buf.at[i], kr_out.at[req, :, pl.ds(first, rows)], k_sem.at[i]))
            waits[-1].start()
    for at, (req, part, pieces, firsts) in enumerate(groups):
        length = part[:, rank + 2 * LANES : rank + 2 * LANES + 1]
        blocks = [(land_refs[j][r, :rows, :], kr_buf[j * LATE + r]) for j, r in pieces]
        state = part[:, rank : rank + 1], part[:, rank + LANES : rank + LANES + 1], part[:, :rank]
        _, total, acc = folded(*state, qa_ref[req], qr_ref[req], blocks, firsts, length, scale)
        o_buf[at] = (acc / total).astype(jnp.bfloat16)
    for at, (req, *_) in enumerate(groups):
        waits.append(pltpu.make_async_copy(o_buf.at[at], o_out.at[req], o_sem.at[at]))
        waits[-1].start()
    for c in waits:
        c.wait()


def attend(lens, landed, before, rest, q_lat, q_rope, n, block):
    req_local, heads, rank = q_lat.shape
    width = q_rope.shape[1]
    rows = block // PIECES
    total = rest[0].shape[1]
    late = LATE_STEPS * LATE
    scale = (rank + width) ** -0.5
    caches = [jax.ShapeDtypeStruct((req_local, n * block, rank), jnp.bfloat16),
              jax.ShapeDtypeStruct((req_local, width, n * block), jnp.bfloat16),
              jax.ShapeDtypeStruct((req_local, heads, rank), jnp.bfloat16)]
    part = jax.ShapeDtypeStruct((heads, rank + 3 * LANES), jnp.float32)
    state = [pltpu.VMEM((heads, 1), jnp.float32), pltpu.VMEM((heads, 1), jnp.float32), pltpu.VMEM((heads, rank), jnp.float32)]

    def stores(depth, pieces):
        return [pltpu.VMEM((depth, width, pieces * rows), jnp.bfloat16), pltpu.SemaphoreType.DMA((depth, pieces)), pltpu.SemaphoreType.DMA((depth,))]

    def ring(depth, pieces):
        return [pltpu.VMEM((depth, pieces, total, rank), jnp.bfloat16), pltpu.SemaphoreType.DMA((depth,))] + stores(depth, pieces)

    params = pltpu.CompilerParams(vmem_limit_bytes=ATTEND_BYTES)
    flops = 2 * req_local * n * block * heads * rank
    *outs, first_part = pl.pallas_call(
        functools.partial(first_kernel, n, req_local, scale),
        in_specs=[SMEM, HBM, VMEM, VMEM],
        out_specs=[HBM] * 4,
        out_shape=caches + [part],
        scratch_shapes=state + [pltpu.VMEM(part.shape, part.dtype), pltpu.SemaphoreType.DMA,
                                pltpu.VMEM((rows, rank), jnp.bfloat16), pltpu.VMEM((width, block), jnp.bfloat16),
                                pltpu.VMEM((req_local - 2, heads, rank), jnp.bfloat16),
                                pltpu.SemaphoreType.DMA((req_local - 2,)), pltpu.SemaphoreType.DMA((req_local - 2,))]
        + ring(RING, PIECES) + ring(LATE_STEPS, 2 * PIECES - LATE) + ring(n - LATE_STEPS, PIECES),
        compiler_params=params,
        cost_estimate=pl.CostEstimate(flops=flops, bytes_accessed=req_local * n * block * rank * 4, transcendentals=0),
        name="attend_first",
    )(lens, landed, q_lat, q_rope)
    return pl.pallas_call(
        functools.partial(last_kernel, n, req_local, scale),
        in_specs=[VMEM] * (LATE_STEPS + 4) + [HBM] * 3,
        out_specs=[HBM] * 3,
        out_shape=caches,
        scratch_shapes=[pltpu.VMEM((2, heads, rank), jnp.bfloat16), pltpu.SemaphoreType.DMA((2,))] + stores(late, 1),
        input_output_aliases={LATE_STEPS + 4 + k: k for k in range(3)},
        compiler_params=params,
        cost_estimate=pl.CostEstimate(flops=flops // req_local // PIECES, bytes_accessed=n * block * rank * 2, transcendentals=0),
        name="attend_last",
    )(*rest, q_lat, q_rope, first_part, before, *outs)


def solution(mesh):
    seq_spec = P("dp", "x", None)
    req_spec = P(("dp", "x"), None, None)
    n = mesh.shape["x"]

    def local_step(c_raw, k_raw, norm_gain, rope_cos, rope_sin, seq_lens, q_lat, q_rope):
        q_rope = jnp.swapaxes(q_rope, 1, 2)
        landed, before, *rest = send(seq_lens, c_raw, jnp.swapaxes(k_raw, 1, 2), norm_gain, rope_cos.T, rope_sin.T, q_lat, q_rope, n)
        rest = [lax.ppermute(pieces, "x", [(i, move(i, j, n, 1)) for i in range(n)]) for j, pieces in enumerate(rest)]
        c_cache, kr_cache, o_lat = attend(seq_lens, landed, before, rest, q_lat, q_rope, n, c_raw.shape[1])
        return c_cache, jnp.swapaxes(kr_cache, 1, 2), o_lat

    return jax.shard_map(local_step, mesh=mesh, in_specs=(seq_spec, seq_spec, P(None), P("x", None), P("x", None), P("dp"), req_spec, req_spec), out_specs=(req_spec, req_spec, req_spec), check_vma=False)
```
